32 devices in a mesh: dp: 8 (over z, x), head: 4 (over y, core).
Axes of the slice: x: 2, y: 2, z: 4, core: 2. Of those that a mesh axis runs over, the one named last changes fastest.
Arguments:
- inputs: bfloat16 [8192, 2048], P('dp'), may hold values from -6 to 6
- lengths: int32 [8], P('dp'), may hold values from 256 to 1024, as said below
- gain_attn: bfloat16 [2048], P('dp'), may hold values from 0.5 to 1.5
- w_query: bfloat16 [2048, 2048], P('dp', 'head'), may hold values from -0.25 to 0.25
- w_key: bfloat16 [2048, 2048], P('dp', 'head'), may hold values from -0.25 to 0.25
- w_value: bfloat16 [2048, 2048], P('dp', 'head'), may hold values from -0.125 to 0.125
- w_slot: bfloat16 [2048, 256], P('dp', 'head'), may hold values from -0.125 to 0.125
- gate_bias: float32 [256], P('head'), may hold values from 0 to 8
- w_out: bfloat16 [2048, 2048], P('head', 'dp'), may hold values from -0.5 to 0.5
- gain_ffn: bfloat16 [2048], P('dp'), may hold values from 0.5 to 1.5
- w_gate: bfloat16 [2048, 5632], P('dp', 'head'), may hold values from -0.125 to 0.125
- w_up: bfloat16 [2048, 5632], P('dp', 'head'), may hold values from -0.125 to 0.125
- w_down: bfloat16 [5632, 2048], P('head', 'dp'), may hold values from -0.078125 to 0.078125
- cotangent: bfloat16 [8192, 2048], P('dp'), may hold values from -6 to 6
Outputs:
- output: bfloat16 [8192, 2048], P('dp')
- grad_inputs: float32 [8192, 2048], P('dp')
- grad_gain_attn: float32 [2048], P('dp')
- grad_w_query: float32 [2048, 2048], P('dp', 'head')
- grad_w_key: float32 [2048, 2048], P('dp', 'head')
- grad_w_value: float32 [2048, 2048], P('dp', 'head')
- grad_w_slot: float32 [2048, 256], P('dp', 'head')
- grad_gate_bias: float32 [256], P('head')
- grad_w_out: float32 [2048, 2048], P('head', 'dp')
- grad_gain_ffn: float32 [2048], P('dp')
- grad_w_gate: float32 [2048, 5632], P('dp', 'head')
- grad_w_up: float32 [2048, 5632], P('dp', 'head')
- grad_w_down: float32 [5632, 2048], P('head', 'dp')
The draws below stay inside these ranges and needn't reach their ends.
Inputs may be any that keep to these rules, and one draw needn't show every extreme that they name: lengths[s] is the number of valid leading positions of sequence s; some sequence has all 1024 valid.
All inputs are finite; a program needn't handle non-finite values.
Results may differ from the reference program's by a relative error of at most 0.014.
Values may be sent and summed in bfloat16 or wider, within the bound.
A program may use at most 256 MiB of HBM per device.

```python
import jax
import jax.numpy as jnp
from jax import lax

D = 2048
HEADS = 4
KDIM = 512
SLOTS = 64
FF = 5632
LEN = 1024
SPAN = 64
SEQS = 8
TOKENS = 8192


def draw_lengths(key, part):
    counts = jax.random.randint(key, (SEQS,), LEN // 4, LEN + 1)
    chosen = jax.random.randint(jax.random.fold_in(key, 7), (), 0, SEQS)
    return jnp.where(jnp.arange(SEQS) == chosen, LEN, counts).astype(jnp.int32)


def block_scale(key, shape, shards, low, largest):
    def one(axis_at, parts):
        heights = jax.random.uniform(jax.random.fold_in(jax.random.fold_in(key, 6), axis_at), (parts,), jnp.float32, low / len(shards), largest / len(shards))
        return jnp.repeat(jnp.exp(heights), shape[axis_at] // parts).reshape((-1,) + (1,) * (len(shape) - axis_at - 1))

    level = one(*shards[0])
    for cut in shards[1:]:
        level = level * one(*cut)
    return level


def bell_draw(key, shape, scale, limit, split=(), dtype=jnp.bfloat16):
    loudness = block_scale(key, shape, split, -0.22, 0.18) if split else 1.0
    drawn = jax.random.normal(key, shape, jnp.float32) * scale * loudness
    return jnp.minimum(jnp.maximum(drawn, -limit), limit).astype(dtype)


def setup_inputs(seed: int = 0) -> dict:
    seeds = jax.random.split(jax.random.key(seed), 15)
    return {
        "inputs": bell_draw(seeds[0], (TOKENS, D), 1.0, 6.0, ((0, 8),)),
        "lengths": draw_lengths(jax.random.fold_in(seeds[14], 71), 0),
        "gain_attn": jnp.clip(1.0 + 0.1 * jax.random.normal(seeds[2], (D,), jnp.float32), 0.5, 1.5).astype(jnp.bfloat16),
        "w_query": bell_draw(seeds[3], (D, HEADS * KDIM), (D // 4) ** -0.5, 0.25, ((0, 8), (1, 4))),
        "w_key": bell_draw(seeds[4], (D, HEADS * KDIM), (D // 4) ** -0.5, 0.25, ((0, 8), (1, 4))),
        "w_value": bell_draw(seeds[5], (D, HEADS * KDIM), D ** -0.5, 0.125, ((0, 8), (1, 4))),
        "w_slot": bell_draw(seeds[6], (D, HEADS * SLOTS), D ** -0.5, 0.125, ((0, 8), (1, 4))),
        "gate_bias": jnp.clip(8.0 * jax.random.uniform(seeds[7], (HEADS * SLOTS,), jnp.float32) ** block_scale(seeds[7], (HEADS * SLOTS,), ((0, 4),), -0.2, 0.2), 0.0, 8.0),
        "w_out": bell_draw(seeds[8], (HEADS * KDIM, D), (HEADS * KDIM // 16) ** -0.5, 0.5, ((0, 4), (1, 8))),
        "gain_ffn": jnp.clip(1.0 + 0.1 * jax.random.normal(seeds[9], (D,), jnp.float32), 0.5, 1.5).astype(jnp.bfloat16),
        "w_gate": bell_draw(seeds[10], (D, FF), D ** -0.5, 0.125, ((0, 8), (1, 4))),
        "w_up": bell_draw(seeds[11], (D, FF), D ** -0.5, 0.125, ((0, 8), (1, 4))),
        "w_down": bell_draw(seeds[12], (FF, D), FF ** -0.5, 0.078125, ((0, 4), (1, 8))),
        "cotangent": bell_draw(seeds[13], (TOKENS, D), 1.0, 6.0, ((0, 8),)),
    }


epsilon = 1e-06
damping = 8.0
highest = lax.Precision.HIGHEST

@jax.custom_vjp
def low(v):
    return lax.optimization_barrier(v.astype(jnp.bfloat16)).astype(jnp.float32)

@jax.custom_vjp
def low_back(v):
    return v

def low_keep(v):
    return (low(v), None)

def low_pass(kept, grad):
    return (grad,)

def back_keep(v):
    return (v, None)

def back_low(kept, grad):
    return (low(grad),)
low.defvjp(low_keep, low_pass)
low_back.defvjp(back_keep, back_low)

def product(left, right):
    return jnp.dot(left, right, precision=highest)

def norm_rows(values, gain):
    factor = lax.rsqrt(lax.optimization_barrier(jnp.mean(values * values, axis=-1, keepdims=True)) + epsilon)
    return values * factor * gain

def swiglu(gate_act, up_act):
    return jax.nn.silu(gate_act) * up_act

def span_step(states, pieces):
    queries, key_rows, value_rows, logdecay, writes = pieces
    state_keys, state_values = states
    rows_count = queries.shape[0]
    cumul = jnp.cumsum(logdecay, axis=0)
    causal = (jnp.arange(rows_count)[:, None] >= jnp.arange(rows_count)[None, :])[:, :, None]
    spread = jnp.where(causal, cumul[:, None, :] - cumul[None, :, :], 0.0)
    weighted = jnp.where(causal, jnp.exp(spread), 0.0) * writes[None, :, :]
    scale_factor = queries.shape[1] ** (-0.5)
    inner_products = jnp.dot(queries, key_rows.T, precision=highest) * scale_factor
    carried = jnp.dot(queries, state_keys.T, precision=highest) * scale_factor
    scores = jnp.exp(cumul) * carried + jnp.einsum('tsj,ts->tj', weighted, inner_products, precision=highest)
    slot_probs = jax.nn.softmax(scores, axis=-1)
    mixing = jnp.einsum('tj,tsj->ts', slot_probs, weighted, precision=highest)
    result = jnp.dot(slot_probs * jnp.exp(cumul), state_values, precision=highest) + jnp.dot(mixing, value_rows, precision=highest)
    last_cumul = cumul[-1]
    tail_weight = jnp.exp(last_cumul[None, :] - cumul) * writes
    new_keys = jnp.exp(last_cumul)[:, None] * state_keys + jnp.dot(tail_weight.T, key_rows, precision=highest)
    new_values = jnp.exp(last_cumul)[:, None] * state_values + jnp.dot(tail_weight.T, value_rows, precision=highest)
    return ((new_keys, new_values), result)

def slot_mixer(queries, key_rows, value_rows, gate_logits, valid_mask):
    logdecay = valid_mask[:, None] * jax.nn.log_sigmoid(gate_logits) / damping
    writes = valid_mask[:, None] * (1.0 - jnp.exp(logdecay))
    length = queries.shape[0]
    blocks = length // SPAN

    def blocked(matrix):
        return matrix.reshape(blocks, SPAN, matrix.shape[1])
    start_state = (jnp.zeros((gate_logits.shape[1], key_rows.shape[1]), jnp.float32), jnp.zeros((gate_logits.shape[1], value_rows.shape[1]), jnp.float32))
    _, outputs = lax.scan(jax.checkpoint(span_step), start_state, (blocked(queries), blocked(key_rows), blocked(value_rows), blocked(logdecay), blocked(writes)))
    return outputs.reshape(length, value_rows.shape[1]) * valid_mask[:, None]

def block_layer(rows_in, group_lengths, gain_attn, w_query, w_key, w_value, w_slot, gate_bias, w_out, gain_ffn, w_gate, w_up, w_down):
    groups = group_lengths.shape[0]
    length = rows_in.shape[0] // groups
    normed = low(norm_rows(rows_in, gain_attn))
    queries = low(low_back(product(normed, w_query)))
    key_proj = low(low_back(product(normed, w_key)))
    value_proj = low(low_back(product(normed, w_value)))
    gate_logits = low_back(product(normed, w_slot)) + gate_bias
    positions = jnp.arange(length).astype(jnp.int32)
    valid_mask = (positions[None, :] < group_lengths[:, None].astype(jnp.int32)).astype(jnp.float32)

    def by_head(matrix, width):
        return matrix.reshape(groups, length, HEADS, width).transpose(0, 2, 1, 3)
    inner_map = jax.vmap(slot_mixer, (0, 0, 0, 0, None))
    outer_map = jax.vmap(inner_map, (0, 0, 0, 0, 0))
    mixed = outer_map(by_head(queries, KDIM), by_head(key_proj, KDIM), by_head(value_proj, KDIM), by_head(gate_logits, SLOTS), valid_mask)
    mixed = low(mixed.transpose(0, 2, 1, 3).reshape(groups * length, HEADS * KDIM))
    attn = low_back(product(mixed, w_out))
    resid = rows_in + attn
    normed2 = low(norm_rows(resid, gain_ffn))
    gate_act = low_back(product(normed2, w_gate))
    up_act = low_back(product(normed2, w_up))
    hidden = low(swiglu(gate_act, up_act))
    return resid + product(hidden, w_down)

def reference(inputs, lengths, gain_attn, w_query, w_key, w_value, w_slot, gate_bias, w_out, gain_ffn, w_gate, w_up, w_down, cotangent):
    weights = tuple((member.astype(jnp.float32) for member in (gain_attn, w_query, w_key, w_value, w_slot, gate_bias, w_out, gain_ffn, w_gate, w_up, w_down)))
    per_group = 4

    def forward(rows_in, params):
        grouped = rows_in.reshape(SEQS // per_group, per_group * LEN, D)
        group_lens = lengths.reshape(SEQS // per_group, per_group)

        def group_step(carry, inputs_pair):
            return (carry, jax.checkpoint(block_layer)(inputs_pair[0], inputs_pair[1], *params))
        _, outputs = lax.scan(group_step, 0.0, (grouped, group_lens))
        return outputs.reshape(TOKENS, D)
    result, pull_back = jax.vjp(forward, inputs.astype(jnp.float32), weights)
    grad_rows, grads = pull_back(cotangent.astype(jnp.float32))
    return (result.astype(jnp.bfloat16), grad_rows, grads[0], grads[1], grads[2], grads[3], grads[4], grads[5], grads[6], grads[7], grads[8], grads[9], grads[10])
```

```python
import jax
import jax.numpy as jnp
from jax import lax
from jax.experimental import pallas as pl
from jax.experimental.pallas import tpu as pltpu
from jax.sharding import PartitionSpec as P

BLOCK = 64
TILE = 128
epsilon = 1e-06


def split_low(values):
    high = values.astype(jnp.bfloat16)
    return high, (values - high.astype(jnp.float32)).astype(jnp.bfloat16)


def dot_nn(left, right):
    return lax.dot_general(left, right, (((1,), (0,)), ((), ())), preferred_element_type=jnp.float32)


def dot_nt(left, right):
    return lax.dot_general(left, right, (((1,), (1,)), ((), ())), preferred_element_type=jnp.float32)


def lane_place():
    lanes = lax.broadcasted_iota(jnp.int32, (BLOCK, TILE), 1)
    return lanes, jnp.bitwise_and(lanes, BLOCK - 1)


def prefix_sum(values, place):
    step = 1
    while step < BLOCK:
        values = values + jnp.where(place >= step, pltpu.roll(values, step, 1), 0.0)
        step *= 2
    return values


def suffix_sum(values, place):
    step = 1
    while step < BLOCK:
        values = values + jnp.where(place < BLOCK - step, pltpu.roll(values, TILE - step, 1), 0.0)
        step *= 2
    return values


def skew(square, forward):
    rows = lax.broadcasted_iota(jnp.int32, (TILE, TILE), 0)
    step = 1
    while step < TILE:
        moved = pltpu.roll(square, step if forward else TILE - step, 1)
        square = jnp.where(jnp.bitwise_and(rows, step) != 0, moved, square)
        step *= 2
    return square


def to_band(square):
    return skew(square, False).T


def from_band(band):
    return skew(band.T, True)


def gate_terms(logits, valid, place):
    log_sig = jnp.minimum(logits, 0.0) - jnp.log1p(jnp.exp(-jnp.abs(logits)))
    logdecay = valid * log_sig * 0.125
    decay = jnp.exp(logdecay)
    series = -logdecay * (1.0 + logdecay * (0.5 + logdecay * (1.0 / 6.0 + logdecay * (1.0 / 24.0))))
    writes = valid * jnp.where(logdecay > -0.03, series, 1.0 - decay)
    inside = jnp.where(place == 0, 0.0, decay)
    before = prefix_sum(logdecay, place)
    after = suffix_sum(logdecay, place) - logdecay
    return decay, writes, inside, before, after


def stacked(values, lanes):
    return jnp.concatenate(
        [jnp.where(lanes < BLOCK, values, 0.0), jnp.where(lanes < BLOCK, 0.0, values)], axis=0
    )


def own_block(square, lanes):
    return jnp.where(lanes < BLOCK, square[:BLOCK], square[BLOCK:])


def forward_kernel(
    length_ref, qkv_ref, logit_ref, bias_ref,
    mixed_ref, state_ref, prob_ref, score_ref, mix_ref,
    gate_ref, carry_ref, band_ref,
):
    width = mixed_ref.shape[1]
    tiles = mixed_ref.shape[0] // TILE
    scale = width ** -0.5
    lanes, place = lane_place()
    bias = bias_ref[...]

    def valid_of(tile):
        return (lanes + tile * TILE < length_ref[0]).astype(jnp.float32)

    def rows_of(tile):
        return pl.ds(pl.multiple_of(tile * TILE, TILE), TILE)

    def gather_writes(tile, none):
        logits = logit_ref[tile] + bias
        decay, writes, inside, before, after = gate_terms(logits, valid_of(tile), place)
        gate_ref[tile, 0] = writes
        gate_ref[tile, 1] = inside
        gate_ref[tile, 2] = jnp.exp(before)
        gate_ref[tile, 3] = jnp.exp(before + after)
        high, low = split_low(stacked(jnp.exp(after) * writes, lanes))
        rows = qkv_ref[rows_of(tile), width:]
        added = dot_nn(high, rows) + dot_nn(low, rows)
        state_ref[tile] = added
        return none

    lax.fori_loop(0, tiles, gather_writes, 0)

    carry_ref[...] = jnp.zeros_like(carry_ref)

    def run_states(tile, none):
        for part in range(2):
            span = pl.ds(part * BLOCK, BLOCK)
            fade = gate_ref[tile, 3, :, part * BLOCK : part * BLOCK + 1]
            carried = carry_ref[...]
            added = state_ref[tile, span, :]
            state_ref[tile, span, :] = carried
            carry_ref[...] = fade * carried + added
        return none

    lax.fori_loop(0, tiles, run_states, 0)

    def mix_tile(tile, none):
        queries = qkv_ref[rows_of(tile), :width]
        key_rows = qkv_ref[rows_of(tile), width : 2 * width]
        value_rows = qkv_ref[rows_of(tile), 2 * width :]
        writes, inside, fade = gate_ref[tile, 0], gate_ref[tile, 1], gate_ref[tile, 2]
        band_ref[...] = to_band(dot_nt(queries, key_rows) * scale)
        high, low = split_low(state_ref[tile, :, :width])
        carried = own_block(dot_nt(high, queries) + dot_nt(low, queries), lanes)

        def lag_score(lag, carry):
            weighted, total = carry
            total = total + weighted * band_ref[pl.ds(jnp.bitwise_and(TILE - lag, TILE - 1), 1), :]
            return inside * pltpu.roll(weighted, 1, 1), total

        _, scores = lax.fori_loop(
            0, BLOCK, lag_score, (writes, fade * carried * scale), unroll=8
        )
        top = jnp.max(scores, axis=0, keepdims=True)
        raised = jnp.exp(scores - top)
        probs = raised / jnp.sum(raised, axis=0, keepdims=True)
        score_ref[tile] = scores
        prob_ref[tile] = probs
        band_ref[...] = jnp.zeros_like(band_ref)

        def lag_mix(lag, weighted):
            band_ref[pl.ds(jnp.bitwise_and(TILE - lag, TILE - 1), 1), :] = jnp.sum(
                probs * weighted, axis=0, keepdims=True
            )
            return inside * pltpu.roll(weighted, 1, 1)

        lax.fori_loop(0, BLOCK, lag_mix, writes, unroll=8)
        mixing = from_band(band_ref[...]).astype(jnp.bfloat16)
        mix_ref[tile] = mixing
        reach = stacked(probs * fade, lanes).T.astype(jnp.bfloat16)
        result = dot_nn(mixing, value_rows) + dot_nn(reach, state_ref[tile, :, width:].astype(jnp.bfloat16))
        rows = lax.broadcasted_iota(jnp.int32, (TILE, 1), 0) + tile * TILE
        mixed_ref[rows_of(tile), :] = jnp.where(rows < length_ref[0], result, 0.0).astype(jnp.bfloat16)
        return none

    lax.fori_loop(0, tiles, mix_tile, 0)


def backward_kernel(
    length_ref, qkv_ref, logit_ref, bias_ref, back_ref, state_ref, prob_ref, score_ref, mix_ref,
    d_qkv_ref, d_logit_ref, d_bias_ref,
    adjoint_ref, slope_ref, gain_ref, key_band_ref, value_band_ref, band_ref, carry_ref, end_ref, cross_ref,
):
    width = back_ref.shape[1]
    tiles = back_ref.shape[0] // TILE
    scale = width ** -0.5
    lanes, place = lane_place()
    bias = bias_ref[...]

    def valid_of(tile):
        return (lanes + tile * TILE < length_ref[0]).astype(jnp.float32)

    def rows_of(tile):
        return pl.ds(pl.multiple_of(tile * TILE, TILE), TILE)

    def back_of(tile):
        rows = lax.broadcasted_iota(jnp.int32, (TILE, 1), 0) + tile * TILE
        return jnp.where(rows < length_ref[0], back_ref[rows_of(tile), :], jnp.zeros((), back_ref.dtype))

    def slopes(tile, none):
        logits = logit_ref[tile] + bias
        decay, writes, inside, before, after = gate_terms(logits, valid_of(tile), place)
        fade = jnp.exp(before)
        queries = qkv_ref[rows_of(tile), :width]
        key_rows = qkv_ref[rows_of(tile), width : 2 * width]
        value_rows = qkv_ref[rows_of(tile), 2 * width :]
        back = back_of(tile)
        probs = prob_ref[tile]
        key_band_ref[...] = to_band(dot_nt(queries, key_rows) * scale)
        value_band_ref[...] = to_band(dot_nt(back, value_rows))
        high, low = split_low(state_ref[tile, :, width:])
        carried = own_block(dot_nt(high, back) + dot_nt(low, back), lanes)

        def lag_gain(lag, carry):
            weighted, total = carry
            total = total + weighted * value_band_ref[pl.ds(jnp.bitwise_and(TILE - lag, TILE - 1), 1), :]
            return inside * pltpu.roll(weighted, 1, 1), total

        _, gains = lax.fori_loop(0, BLOCK, lag_gain, (writes, fade * carried), unroll=8)
        d_scores = probs * (gains - jnp.sum(probs * gains, axis=0, keepdims=True))
        slope_ref[tile] = d_scores
        band_ref[...] = jnp.zeros_like(band_ref)

        def lag_mix(lag, weighted):
            band_ref[pl.ds(jnp.bitwise_and(TILE - lag, TILE - 1), 1), :] = jnp.sum(
                d_scores * weighted, axis=0, keepdims=True
            )
            return inside * pltpu.roll(weighted, 1, 1)

        lax.fori_loop(0, BLOCK, lag_mix, writes, unroll=8)
        mixing = (from_band(band_ref[...]) * scale).astype(jnp.bfloat16)

        def lag_write(count, total):
            lag = BLOCK - 1 - count
            row = pl.ds(jnp.bitwise_and(TILE - lag, TILE - 1), 1)
            return (
                d_scores * key_band_ref[row, :]
                + probs * value_band_ref[row, :]
                + pltpu.roll(inside * total, TILE - 1, 1)
            )

        gain_ref[tile, 0] = lax.fori_loop(0, BLOCK, lag_write, jnp.zeros((BLOCK, TILE), jnp.float32), unroll=8)
        gain_ref[tile, 1] = d_scores * score_ref[tile] + probs * gains
        gain_ref[tile, 2] = decay
        gain_ref[tile, 3] = writes
        gain_ref[tile, 4] = jnp.exp(after)
        gain_ref[tile, 5] = jnp.exp(before + after)
        reach = stacked(d_scores * fade * scale, lanes)
        reach_low = reach.astype(jnp.bfloat16)
        d_qkv_ref[rows_of(tile), :width] = (
            dot_nn(mixing, key_rows)
            + dot_nn(reach.T.astype(jnp.bfloat16), state_ref[tile, :, :width].astype(jnp.bfloat16))
        ).astype(jnp.bfloat16)
        adjoint_ref[tile, :, :width] = dot_nn(reach_low, queries)
        adjoint_ref[tile, :, width:] = dot_nn(stacked(probs * fade, lanes).astype(jnp.bfloat16), back)
        d_qkv_ref[rows_of(tile), width : 2 * width] = dot_nn(mixing.T, queries).astype(jnp.bfloat16)
        d_qkv_ref[rows_of(tile), 2 * width :] = dot_nn(mix_ref[tile].T, back).astype(jnp.bfloat16)
        return none

    lax.fori_loop(0, tiles, slopes, 0)

    carry_ref[...] = jnp.zeros_like(carry_ref)
    end_ref[...] = jnp.zeros_like(end_ref)

    def run_adjoints(count, none):
        tile = tiles - 1 - count
        for part in (1, 0):
            span = pl.ds(part * BLOCK, BLOCK)
            fade = gain_ref[tile, 5, :, part * BLOCK : part * BLOCK + 1]
            carried = carry_ref[...]
            added = adjoint_ref[tile, span, :]
            adjoint_ref[tile, span, :] = carried
            cross_ref[tile, span, :] = jnp.broadcast_to(
                jnp.sum(carried * end_ref[...], axis=1, keepdims=True), (BLOCK, TILE)
            )
            end_ref[...] = state_ref[tile, span, :]
            carry_ref[...] = fade * carried + added
        return none

    lax.fori_loop(0, tiles, run_adjoints, 0)

    d_bias_ref[...] = jnp.zeros_like(d_bias_ref)

    def finish(tile, none):
        key_rows = qkv_ref[rows_of(tile), width : 2 * width]
        value_rows = qkv_ref[rows_of(tile), 2 * width :]
        adjoint = adjoint_ref[tile]
        high, low = split_low(adjoint)
        rows = qkv_ref[rows_of(tile), width:]
        carried = own_block(dot_nt(high, rows) + dot_nt(low, rows), lanes)
        decay, writes, rest = gain_ref[tile, 2], gain_ref[tile, 3], gain_ref[tile, 4]
        d_writes = gain_ref[tile, 0] + rest * carried
        tail = stacked(rest * writes, lanes).T.astype(jnp.bfloat16)
        d_qkv_ref[rows_of(tile), width:] = (
            d_qkv_ref[rows_of(tile), width:].astype(jnp.float32) + dot_nn(tail, high)
        ).astype(jnp.bfloat16)
        cross = own_block(cross_ref[tile], lanes)
        d_decay = suffix_sum(gain_ref[tile, 1] - writes * d_writes, place) + cross - decay * d_writes
        logits = logit_ref[tile] + bias
        d_logit = valid_of(tile) * d_decay * jax.nn.sigmoid(-logits) * 0.125
        d_bias_ref[...] += jnp.broadcast_to(jnp.sum(d_logit, axis=1, keepdims=True), (BLOCK, TILE))
        d_logit_ref[tile] = d_logit.astype(jnp.bfloat16)
        return none

    lax.fori_loop(0, tiles, finish, 0)


def mixer_forward(length, qkv, logits, bias):
    rows, width = qkv.shape[0], qkv.shape[1] // 3
    tiles = rows // TILE
    f32 = jnp.float32
    return pl.pallas_call(
        forward_kernel,
        out_shape=(
            jax.ShapeDtypeStruct((rows, width), jnp.bfloat16),
            jax.ShapeDtypeStruct((tiles, TILE, 2 * width), f32),
            jax.ShapeDtypeStruct((tiles, BLOCK, TILE), f32),
            jax.ShapeDtypeStruct((tiles, BLOCK, TILE), f32),
            jax.ShapeDtypeStruct((tiles, TILE, TILE), jnp.bfloat16),
        ),
        in_specs=[pl.BlockSpec(memory_space=pltpu.SMEM)] + [pl.BlockSpec(memory_space=pltpu.VMEM)] * 3,
        out_specs=[pl.BlockSpec(memory_space=pltpu.VMEM)] * 5,
        scratch_shapes=[
            pltpu.VMEM((tiles, 4, BLOCK, TILE), f32),
            pltpu.VMEM((BLOCK, 2 * width), f32),
            pltpu.VMEM((TILE, TILE), f32),
        ],
        name="mixer_forward",
    )(length, qkv, logits, bias)


def mixer_backward(length, qkv, logits, bias, back, saved):
    rows, width = qkv.shape[0], qkv.shape[1] // 3
    tiles = rows // TILE
    f32 = jnp.float32
    return pl.pallas_call(
        backward_kernel,
        out_shape=(
            jax.ShapeDtypeStruct((rows, 3 * width), jnp.bfloat16),
            jax.ShapeDtypeStruct((tiles, BLOCK, TILE), jnp.bfloat16),
            jax.ShapeDtypeStruct((BLOCK, TILE), f32),
        ),
        in_specs=[pl.BlockSpec(memory_space=pltpu.SMEM)] + [pl.BlockSpec(memory_space=pltpu.VMEM)] * 8,
        out_specs=[pl.BlockSpec(memory_space=pltpu.VMEM)] * 3,
        scratch_shapes=[
            pltpu.VMEM((tiles, TILE, 2 * width), f32),
            pltpu.VMEM((tiles, BLOCK, TILE), f32),
            pltpu.VMEM((tiles, 6, BLOCK, TILE), f32),
            pltpu.VMEM((TILE, TILE), f32),
            pltpu.VMEM((TILE, TILE), f32),
            pltpu.VMEM((TILE, TILE), f32),
            pltpu.VMEM((BLOCK, 2 * width), f32),
            pltpu.VMEM((BLOCK, 2 * width), f32),
            pltpu.VMEM((tiles, TILE, TILE), f32),
        ],
        name="mixer_backward",
    )(length, qkv, logits, bias, back, *saved)


def to_low(values):
    return values.astype(jnp.bfloat16)


def to_wide(values):
    return values.astype(jnp.float32)


def dot_tn(left, right):
    return lax.dot_general(left, right, (((0,), (0,)), ((), ())), preferred_element_type=jnp.float32)


def after(values, *earlier):
    return lax.optimization_barrier((values,) + earlier)[0]


def ring_order(size):
    return list(range(0, size, 2)) + list(range(size - 1 - size % 2, 0, -2))


def hop_pairs(order, hop):
    size = len(order)
    return [(order[i], order[(i + hop) % size]) for i in range(size)]


def ring_gather(shard, order):
    size = len(order)
    up, down = hop_pairs(order, 1), hop_pairs(order, -1)
    pieces = [shard] + [None] * (size - 1)
    from_low, from_high = shard, shard
    for step in range(1, (size + 1) // 2):
        from_low = lax.ppermute(from_low, "dp", up)
        from_high = lax.ppermute(from_high, "dp", down)
        pieces[size - step], pieces[step] = from_low, from_high
    if size % 2 == 0:
        half = shard.shape[0] // 2
        first = lax.ppermute(from_low[:half], "dp", up)
        second = lax.ppermute(from_high[half:], "dp", down)
        pieces[size // 2] = jnp.concatenate([first, second], axis=0)
    return pieces


def ring_scatter(piece_of, order):
    size = len(order)
    up, down = hop_pairs(order, 1), hop_pairs(order, -1)
    half_count = (size - 1) // 2
    up_sum, down_sum = None, None
    if size % 2 == 0:
        farthest = piece_of(size // 2)
        half = farthest.shape[0] // 2
        up_half = lax.ppermute(to_low(farthest[:half]), "dp", up)
        down_half = lax.ppermute(to_low(farthest[half:]), "dp", down)
        up_sum = jnp.concatenate([to_wide(up_half), jnp.zeros(up_half.shape, jnp.float32)], axis=0)
        down_sum = jnp.concatenate([jnp.zeros(down_half.shape, jnp.float32), to_wide(down_half)], axis=0)
    for step in range(half_count, 0, -1):
        up_piece, down_piece = to_wide(piece_of(step)), to_wide(piece_of(size - step))
        if up_sum is not None:
            up_piece, down_piece = up_piece + up_sum, down_piece + down_sum
        up_sum = to_wide(lax.ppermute(to_low(up_piece), "dp", up))
        down_sum = to_wide(lax.ppermute(to_low(down_piece), "dp", down))
    total = to_wide(piece_of(0))
    if up_sum is not None:
        total = total + up_sum + down_sum
    return total


def spread_rows(rows, order):
    size = len(order)
    parts = [rows] + [lax.ppermute(rows, "dp", hop_pairs(order, -hop)) for hop in range(1, size)]
    return jnp.stack(parts)


def scatter_rows(rows, order):
    size = len(order)
    total = rows[0]
    for hop in range(1, size):
        total = total + lax.ppermute(rows[hop], "dp", hop_pairs(order, hop))
    return total


def move_kernel(places_ref, source_ref, target_ref):
    target_ref[...] = source_ref[...]


def move_columns(matrix, places, inverse):
    size = places.shape[0]
    rows, columns = matrix.shape
    width = columns // size
    if width % 128:
        split = matrix.reshape(rows, size, width)
        if inverse:
            places = jnp.argsort(places)
        return jnp.take(split, places, axis=1).reshape(rows, columns)

    def plain(step, places_ref):
        return (0, step)

    def placed(step, places_ref):
        return (0, places_ref[step])

    return pl.pallas_call(
        move_kernel,
        out_shape=jax.ShapeDtypeStruct(matrix.shape, matrix.dtype),
        grid_spec=pltpu.PrefetchScalarGridSpec(
            num_scalar_prefetch=1,
            grid=(size,),
            in_specs=[pl.BlockSpec((rows, width), plain if inverse else placed)],
            out_specs=pl.BlockSpec((rows, width), placed if inverse else plain),
        ),
        cost_estimate=pl.CostEstimate(flops=0, bytes_accessed=2 * matrix.size * matrix.dtype.itemsize, transcendentals=0),
        name="move_columns",
    )(places, matrix)


def head_sum(values, parts=2):
    heads = lax.axis_size("head")
    near = [(i, i ^ 1) for i in range(heads)]
    far = [(i, i ^ 2) for i in range(heads)]
    even = jnp.bitwise_and(lax.axis_index("head"), 1) == 0
    rows = values.shape[0] // parts
    sums = []
    for part in range(parts):
        piece = values[part * rows : (part + 1) * rows]
        low_half, high_half = piece[: rows // 2], piece[rows // 2 :]
        sent = to_low(jnp.where(even, high_half, low_half))
        kept = to_wide(jnp.where(even, low_half, high_half))
        kept = to_low(kept + to_wide(lax.ppermute(sent, "head", near)))
        kept = to_low(to_wide(kept) + to_wide(lax.ppermute(kept, "head", far)))
        other = lax.ppermute(kept, "head", near)
        sums += [jnp.where(even, kept, other), jnp.where(even, other, kept)]
    return jnp.concatenate(sums, axis=0)


def per_device(
    inputs,
    lengths,
    gain_attn,
    w_query,
    w_key,
    w_value,
    w_slot,
    gate_bias,
    w_out,
    gain_ffn,
    w_gate,
    w_up,
    w_down,
    cotangent,
):
    size = lax.axis_size("dp")
    order = ring_order(size)
    place = [order.index(i) for i in range(size)]
    me = lax.axis_index("dp")
    spot = jnp.array(place, jnp.int32)[me]
    places = jnp.array(order + order, jnp.int32)[spot + jnp.arange(size, dtype=jnp.int32)]
    share = gain_attn.shape[0]
    width = w_query.shape[1]
    hidden_count = w_gate.shape[1]
    cut = (hidden_count // 128 + 1) // 2 * 128
    spans = [(0, cut), (cut, hidden_count)]

    gains = spread_rows(jnp.concatenate([gain_attn, gain_ffn]), order)
    gain_one = to_wide(gains[:, :share].reshape(1, size * share))
    gain_two = to_wide(gains[:, share:].reshape(1, size * share))

    out_rows = w_out.T
    down_rows = w_down.T
    mix_shard = jnp.concatenate([w_query, w_key, w_value, w_slot], axis=1)
    mix_pieces = ring_gather(mix_shard, order)
    out_pieces = ring_gather(after(out_rows, mix_pieces[2]), order)
    feed_pieces = []
    earlier = mix_pieces[size // 2]
    for low, high in spans:
        shard = jnp.concatenate([w_gate[:, low:high], w_up[:, low:high], down_rows[:, low:high]], axis=1)
        pieces = ring_gather(after(shard, earlier), order)
        earlier = pieces[size // 2 - 1]
        feed_pieces.append(pieces)

    def joined(pieces, low, high):
        return jnp.concatenate([piece[:, low:high] for piece in pieces], axis=0)

    rows_in = to_wide(move_columns(inputs, places, False))
    back_low = move_columns(cotangent, places, False)
    factor_one = lax.rsqrt(jnp.mean(rows_in * rows_in, axis=-1, keepdims=True) + epsilon)
    normed = to_low(rows_in * factor_one * gain_one)

    full_qkv = joined(mix_pieces, 0, 3 * width)
    full_slot = joined(mix_pieces, 3 * width, mix_shard.shape[1])
    qkv = to_low(dot_nn(normed, full_qkv))
    logits = lax.dot_general(full_slot, normed, (((0,), (1,)), ((), ())), preferred_element_type=jnp.float32)
    slots, length = logits.shape
    logits = logits.reshape(slots, length // TILE, TILE).transpose(1, 0, 2)
    bias = gate_bias[:, None]
    mixed, *saved = mixer_forward(lengths, qkv, logits, bias)
    full_out = jnp.concatenate(out_pieces, axis=0)
    resid = rows_in + to_wide(head_sum(dot_nt(mixed, full_out)))
    factor_two = lax.rsqrt(jnp.mean(resid * resid, axis=-1, keepdims=True) + epsilon)
    normed_two = to_low(resid * factor_two * gain_two)

    result, d_normed_two, feed_grads = None, None, []
    for pieces, (low, high) in zip(feed_pieces, spans):
        count = high - low
        full_gate = joined(pieces, 0, count)
        full_up = joined(pieces, count, 2 * count)
        full_down = joined(pieces, 2 * count, 3 * count)
        gate_act = dot_nn(normed_two, full_gate)
        up_act = dot_nn(normed_two, full_up)
        d_hidden = dot_nn(back_low, full_down)
        sigma = jax.nn.sigmoid(gate_act)
        gated = gate_act * sigma
        hidden = to_low(gated * up_act)
        d_up = to_low(d_hidden * gated)
        d_gate = to_low(d_hidden * up_act * (sigma * (1.0 + gate_act * (1.0 - sigma))))
        grads = [
            to_low(dot_tn(normed_two, d_gate)),
            to_low(dot_tn(normed_two, d_up)),
            to_low(dot_tn(back_low, hidden)),
        ]

        def piece_of(index, grads=grads):
            return jnp.concatenate([grad[index * share : (index + 1) * share] for grad in grads], axis=1)

        feed_grads.append(ring_scatter(piece_of, order))
        term = dot_nt(hidden, full_down)
        result = term if result is None else result + term
        term = dot_nt(d_gate, full_gate) + dot_nt(d_up, full_up)
        d_normed_two = term if d_normed_two is None else d_normed_two + term

    d_normed_two = to_wide(head_sum(d_normed_two))
    hat_two = resid * factor_two
    grad_gain_two = jnp.sum(d_normed_two * hat_two, axis=0)
    scaled = gain_two * d_normed_two
    d_resid = to_wide(back_low) + factor_two * (
        scaled - hat_two * jnp.mean(scaled * hat_two, axis=-1, keepdims=True)
    )
    d_attn = to_low(d_resid)
    d_mixed = to_low(dot_nn(d_attn, full_out))
    grad_out = to_low(dot_tn(d_attn, mixed))
    d_qkv, d_logits, d_bias = mixer_backward(lengths, qkv, logits, bias, d_mixed, saved)
    d_logits = d_logits.transpose(1, 0, 2).reshape(slots, length)
    d_normed = head_sum(
        dot_nt(d_qkv, full_qkv)
        + lax.dot_general(d_logits, full_slot, (((0,), (1,)), ((), ())), preferred_element_type=jnp.float32)
    )
    grad_qkv = to_low(dot_tn(normed, d_qkv))
    grad_slot = to_low(lax.dot_general(normed, d_logits, (((0,), (1,)), ((), ())), preferred_element_type=jnp.float32))

    def out_piece(index):
        return grad_out[index * share : (index + 1) * share]

    def mix_piece(index):
        rows = slice(index * share, (index + 1) * share)
        return jnp.concatenate([grad_qkv[rows], grad_slot[rows]], axis=1)

    out_grad = ring_scatter(out_piece, order)
    mix_grad = ring_scatter(mix_piece, order)

    output = move_columns(to_low(resid + to_wide(head_sum(after(result, d_mixed)))), places, True)
    d_normed = to_wide(d_normed)
    hat_one = rows_in * factor_one
    grad_gain_one = jnp.sum(d_normed * hat_one, axis=0)
    scaled = gain_one * d_normed
    grad_inputs = move_columns(
        d_resid + factor_one * (scaled - hat_one * jnp.mean(scaled * hat_one, axis=-1, keepdims=True)),
        places,
        True,
    )
    small = jnp.concatenate(
        [
            grad_gain_one.reshape(size, share),
            grad_gain_two.reshape(size, share),
            jnp.broadcast_to(d_bias[:, 0], (size, slots)),
        ],
        axis=1,
    )
    small = scatter_rows(small, order)

    def feed_columns(index):
        columns = []
        for grad, (low, high) in zip(feed_grads, spans):
            count = high - low
            columns.append(grad[:, index * count : (index + 1) * count])
        return jnp.concatenate(columns, axis=1)

    return (
        output,
        grad_inputs,
        small[:share],
        mix_grad[:, :width],
        mix_grad[:, width : 2 * width],
        mix_grad[:, 2 * width : 3 * width],
        mix_grad[:, 3 * width :],
        small[2 * share :],
        out_grad.T,
        small[share : 2 * share],
        feed_columns(0),
        feed_columns(1),
        feed_columns(2).T,
    )


def solution(mesh):
    in_specs = (
        P("dp", None),
        P("dp"),
        P("dp"),
        P("dp", "head"),
        P("dp", "head"),
        P("dp", "head"),
        P("dp", "head"),
        P("head"),
        P("head", "dp"),
        P("dp"),
        P("dp", "head"),
        P("dp", "head"),
        P("head", "dp"),
        P("dp", None),
    )
    out_specs = (
        P("dp", None),
        P("dp", None),
        P("dp"),
        P("dp", "head"),
        P("dp", "head"),
        P("dp", "head"),
        P("dp", "head"),
        P("head"),
        P("head", "dp"),
        P("dp"),
        P("dp", "head"),
        P("dp", "head"),
        P("head", "dp"),
    )
    return jax.shard_map(
        per_device, mesh=mesh, in_specs=in_specs, out_specs=out_specs, check_vma=False
    )
```

```python
import jax
import jax.numpy as jnp
from jax import lax
from jax.experimental import pallas as pl
from jax.experimental.pallas import tpu as pltpu
from jax.sharding import PartitionSpec as P

BLOCK = 64
TILE = 128
epsilon = 1e-06
PAIR = 2


def split_low(values):
    high = values.astype(jnp.bfloat16)
    return high, (values - high.astype(jnp.float32)).astype(jnp.bfloat16)


def dot_nn(left, right):
    return lax.dot_general(left, right, (((1,), (0,)), ((), ())), preferred_element_type=jnp.float32)


def dot_nt(left, right):
    return lax.dot_general(left, right, (((1,), (1,)), ((), ())), preferred_element_type=jnp.float32)


def lane_place():
    lanes = lax.broadcasted_iota(jnp.int32, (BLOCK, TILE), 1)
    return lanes, jnp.bitwise_and(lanes, BLOCK - 1)


def prefix_sum(values, place):
    step = 1
    while step < BLOCK:
        values = values + jnp.where(place >= step, pltpu.roll(values, step, 1), 0.0)
        step *= 2
    return values


def suffix_sum(values, place):
    step = 1
    while step < BLOCK:
        values = values + jnp.where(place < BLOCK - step, pltpu.roll(values, TILE - step, 1), 0.0)
        step *= 2
    return values


def to_band(square):
    rows = lax.broadcasted_iota(jnp.int32, (TILE, TILE), 0)
    step = 1
    while step < TILE:
        square = jnp.where(jnp.bitwise_and(rows, step) != 0, pltpu.roll(square, TILE - step, 1), square)
        step *= 2
    return square.T


def from_band(band):
    return pltpu.roll(band.T, 0, 1, stride=1, stride_axis=0)


def lag_row(lag):
    return slice((TILE - lag) % TILE, (TILE - lag) % TILE + 1)


def fill_products(product_ref, slot, writes, inside):
    product_ref[slot, 0] = writes
    power, powers, reach = inside, [], 1
    while reach < BLOCK:
        powers.append(power)
        for lag in range(reach):
            product_ref[slot, reach + lag] = power * pltpu.roll(product_ref[slot, lag], reach, 1)
        power = power * pltpu.roll(power, reach, 1)
        reach *= 2
    return powers


def lag_total(product_ref, slot, band_ref, start):
    sums = [start, None, None, None]
    for lag in range(BLOCK):
        term = product_ref[slot, lag] * band_ref[slot, lag_row(lag), :]
        held = sums[lag % 4]
        sums[lag % 4] = term if held is None else held + term
    return (sums[0] + sums[1]) + (sums[2] + sums[3])


def lag_mix(product_ref, slot, band_ref, weights):
    for lag in range(BLOCK):
        band_ref[slot, lag_row(lag), :] = jnp.sum(weights * product_ref[slot, lag], axis=0, keepdims=True)


def lag_back(powers, term_of, low, count, stride=1):
    if count == 1:
        return term_of(low)
    half = count // 2
    left = lag_back(powers, term_of, low, half, stride)
    right = lag_back(powers, term_of, low + half, half, stride)
    return left + pltpu.roll(powers[half.bit_length() - 1] * right, TILE - half * stride, 1)


def gate_terms(logits, valid, place):
    log_sig = jnp.minimum(logits, 0.0) - jnp.log1p(jnp.exp(-jnp.abs(logits)))
    logdecay = valid * log_sig * 0.125
    decay = jnp.exp(logdecay)
    series = -logdecay * (1.0 + logdecay * (0.5 + logdecay * (1.0 / 6.0 + logdecay * (1.0 / 24.0))))
    writes = valid * jnp.where(logdecay > -0.03, series, 1.0 - decay)
    inside = jnp.where(place == 0, 0.0, decay)
    before = prefix_sum(logdecay, place)
    after = suffix_sum(logdecay, place) - logdecay
    return decay, writes, inside, before, after


def stacked(values, lanes):
    return jnp.concatenate(
        [jnp.where(lanes < BLOCK, values, 0.0), jnp.where(lanes < BLOCK, 0.0, values)], axis=0
    )


def own_block(square, lanes):
    return jnp.where(lanes < BLOCK, square[:BLOCK], square[BLOCK:])


def forward_kernel(
    length_ref, qkv_ref, logit_ref, bias_ref,
    mixed_ref, state_ref, prob_ref, score_ref, mix_ref,
    gate_ref, carry_ref, band_ref, mix_band_ref, product_ref,
):
    width = mixed_ref.shape[1]
    tiles = mixed_ref.shape[0] // TILE
    scale = width ** -0.5
    lanes, place = lane_place()
    bias = bias_ref[...]

    def valid_of(tile):
        return (lanes + tile * TILE < length_ref[0]).astype(jnp.float32)

    def rows_of(tile):
        return pl.ds(pl.multiple_of(tile * TILE, TILE), TILE)

    def gather_writes(tile, none):
        logits = logit_ref[tile] + bias
        decay, writes, inside, before, after = gate_terms(logits, valid_of(tile), place)
        gate_ref[tile, 0] = writes
        gate_ref[tile, 1] = inside
        gate_ref[tile, 2] = jnp.exp(before)
        gate_ref[tile, 3] = jnp.exp(before + after)
        high, low = split_low(stacked(jnp.exp(after) * writes, lanes))
        rows = qkv_ref[rows_of(tile), width:]
        added = dot_nn(high, rows) + dot_nn(low, rows)
        state_ref[tile] = added
        return none

    lax.fori_loop(0, tiles, gather_writes, 0)

    carry_ref[...] = jnp.zeros_like(carry_ref)

    def run_states(tile, none):
        for part in range(2):
            span = pl.ds(part * BLOCK, BLOCK)
            fade = gate_ref[tile, 3, :, part * BLOCK : part * BLOCK + 1]
            carried = carry_ref[...]
            added = state_ref[tile, span, :]
            state_ref[tile, span, :] = carried
            carry_ref[...] = fade * carried + added
        return none

    lax.fori_loop(0, tiles, run_states, 0)

    band_ref[...] = jnp.zeros_like(band_ref)
    mix_band_ref[...] = jnp.zeros_like(mix_band_ref)

    def mix_pair(pair, none):
        both = [(slot, PAIR * pair + slot) for slot in range(PAIR)]
        queries, scores, probs = {}, {}, {}
        for slot, tile in both:
            fill_products(product_ref, slot, gate_ref[tile, 0], gate_ref[tile, 1])
        for slot, tile in both:
            queries[slot] = qkv_ref[rows_of(tile), :width]
            band_ref[slot] = to_band(dot_nt(queries[slot], qkv_ref[rows_of(tile), width : 2 * width]) * scale)
        for slot, tile in both:
            high, low = split_low(state_ref[tile, :, :width])
            carried = own_block(dot_nt(high, queries[slot]) + dot_nt(low, queries[slot]), lanes)
            scores[slot] = gate_ref[tile, 2] * carried * scale
        for slot, tile in both:
            scores[slot] = lag_total(product_ref, slot, band_ref, scores[slot])
        for slot, tile in both:
            top = jnp.max(scores[slot], axis=0, keepdims=True)
            raised = jnp.exp(scores[slot] - top)
            probs[slot] = raised / jnp.sum(raised, axis=0, keepdims=True)
            score_ref[tile] = scores[slot]
            prob_ref[tile] = probs[slot]
        for slot, tile in both:
            lag_mix(product_ref, slot, mix_band_ref, probs[slot])
        for slot, tile in both:
            mixing = from_band(mix_band_ref[slot]).astype(jnp.bfloat16)
            mix_ref[tile] = mixing
            reach = stacked(probs[slot] * gate_ref[tile, 2], lanes).T.astype(jnp.bfloat16)
            result = dot_nn(mixing, qkv_ref[rows_of(tile), 2 * width :]) + dot_nn(
                reach, state_ref[tile, :, width:].astype(jnp.bfloat16)
            )
            rows = lax.broadcasted_iota(jnp.int32, (TILE, 1), 0) + tile * TILE
            mixed_ref[rows_of(tile), :] = jnp.where(rows < length_ref[0], result, 0.0).astype(jnp.bfloat16)
        return none

    lax.fori_loop(0, tiles // PAIR, mix_pair, 0)


def backward_kernel(
    length_ref, qkv_ref, logit_ref, bias_ref, back_ref, state_ref, prob_ref, score_ref, mix_ref,
    d_qkv_ref, d_bias_ref,
    adjoint_ref, gain_ref, key_band_ref, value_band_ref, band_ref, carry_ref, end_ref, cross_ref, product_ref,
):
    width = back_ref.shape[1]
    tiles = back_ref.shape[0] // TILE
    scale = width ** -0.5
    lanes, place = lane_place()
    bias = bias_ref[...]

    def valid_of(tile):
        return (lanes + tile * TILE < length_ref[0]).astype(jnp.float32)

    def rows_of(tile):
        return pl.ds(pl.multiple_of(tile * TILE, TILE), TILE)

    def back_of(tile):
        rows = lax.broadcasted_iota(jnp.int32, (TILE, 1), 0) + tile * TILE
        return jnp.where(rows < length_ref[0], back_ref[rows_of(tile), :], jnp.zeros((), back_ref.dtype))

    band_ref[...] = jnp.zeros_like(band_ref)

    def slopes(pair, none):
        both = [(slot, PAIR * pair + slot) for slot in range(PAIR)]
        fades, powers, queries, keys, backs, gains, d_scores = {}, {}, {}, {}, {}, {}, {}
        for slot, tile in both:
            decay, writes, inside, before, after = gate_terms(logit_ref[tile] + bias, valid_of(tile), place)
            fades[slot] = jnp.exp(before)
            gain_ref[tile, 2] = decay
            gain_ref[tile, 3] = writes
            gain_ref[tile, 4] = jnp.exp(after)
            gain_ref[tile, 5] = jnp.exp(before + after)
            powers[slot] = fill_products(product_ref, slot, writes, inside)
        for slot, tile in both:
            queries[slot] = qkv_ref[rows_of(tile), :width]
            keys[slot] = qkv_ref[rows_of(tile), width : 2 * width]
            backs[slot] = back_of(tile)
            key_band_ref[slot] = to_band(dot_nt(queries[slot], keys[slot]) * scale)
            value_band_ref[slot] = to_band(dot_nt(backs[slot], qkv_ref[rows_of(tile), 2 * width :]))
        for slot, tile in both:
            high, low = split_low(state_ref[tile, :, width:])
            carried = own_block(dot_nt(high, backs[slot]) + dot_nt(low, backs[slot]), lanes)
            gains[slot] = fades[slot] * carried
        for slot, tile in both:
            gains[slot] = lag_total(product_ref, slot, value_band_ref, gains[slot])
        for slot, tile in both:
            probs = prob_ref[tile]
            d_scores[slot] = probs * (gains[slot] - jnp.sum(probs * gains[slot], axis=0, keepdims=True))
            gain_ref[tile, 1] = d_scores[slot] * score_ref[tile] + probs * gains[slot]
        for slot, tile in both:
            lag_mix(product_ref, slot, band_ref, d_scores[slot])
        for slot, tile in both:
            probs = prob_ref[tile]

            def term_of(lag, slot=slot, probs=probs):
                row = lag_row(lag)
                return d_scores[slot] * key_band_ref[slot, row, :] + probs * value_band_ref[slot, row, :]

            group = 8
            for low in range(0, BLOCK, group):
                product_ref[slot, low // group] = lag_back(powers[slot], term_of, low, group)
            gain_ref[tile, 0] = lag_back(
                powers[slot][group.bit_length() - 1 :], lambda index, slot=slot: product_ref[slot, index], 0, BLOCK // group, group
            )
        for slot, tile in both:
            mixing = (from_band(band_ref[slot]) * scale).astype(jnp.bfloat16)
            reach = stacked(d_scores[slot] * fades[slot] * scale, lanes)
            held = stacked(prob_ref[tile] * fades[slot], lanes).astype(jnp.bfloat16)
            d_qkv_ref[rows_of(tile), :width] = (
                dot_nn(mixing, keys[slot])
                + dot_nn(reach.T.astype(jnp.bfloat16), state_ref[tile, :, :width].astype(jnp.bfloat16))
            ).astype(jnp.bfloat16)
            adjoint_ref[tile, :, :width] = dot_nn(reach.astype(jnp.bfloat16), queries[slot])
            adjoint_ref[tile, :, width:] = dot_nn(held, backs[slot])
            d_qkv_ref[rows_of(tile), width : 2 * width] = dot_nn(mixing.T, queries[slot]).astype(jnp.bfloat16)
            d_qkv_ref[rows_of(tile), 2 * width : 3 * width] = dot_nn(mix_ref[tile].T, backs[slot]).astype(jnp.bfloat16)
        return none

    lax.fori_loop(0, tiles // PAIR, slopes, 0)

    carry_ref[...] = jnp.zeros_like(carry_ref)
    end_ref[...] = jnp.zeros_like(end_ref)

    def run_adjoints(count, none):
        tile = tiles - 1 - count
        for part in (1, 0):
            span = pl.ds(part * BLOCK, BLOCK)
            fade = gain_ref[tile, 5, :, part * BLOCK : part * BLOCK + 1]
            carried = carry_ref[...]
            added = adjoint_ref[tile, span, :]
            adjoint_ref[tile, span, :] = carried
            cross_ref[tile, span, :] = jnp.broadcast_to(
                jnp.sum(carried * end_ref[...], axis=1, keepdims=True), (BLOCK, TILE)
            )
            end_ref[...] = state_ref[tile, span, :]
            carry_ref[...] = fade * carried + added
        return none

    lax.fori_loop(0, tiles, run_adjoints, 0)

    d_bias_ref[...] = jnp.zeros_like(d_bias_ref)

    def finish(tile, none):
        key_rows = qkv_ref[rows_of(tile), width : 2 * width]
        value_rows = qkv_ref[rows_of(tile), 2 * width :]
        adjoint = adjoint_ref[tile]
        high, low = split_low(adjoint)
        rows = qkv_ref[rows_of(tile), width:]
        carried = own_block(dot_nt(high, rows) + dot_nt(low, rows), lanes)
        decay, writes, rest = gain_ref[tile, 2], gain_ref[tile, 3], gain_ref[tile, 4]
        d_writes = gain_ref[tile, 0] + rest * carried
        tail = stacked(rest * writes, lanes).T.astype(jnp.bfloat16)
        d_qkv_ref[rows_of(tile), width : 3 * width] = (
            d_qkv_ref[rows_of(tile), width : 3 * width].astype(jnp.float32) + dot_nn(tail, high)
        ).astype(jnp.bfloat16)
        cross = own_block(cross_ref[tile], lanes)
        d_decay = suffix_sum(gain_ref[tile, 1] - writes * d_writes, place) + cross - decay * d_writes
        logits = logit_ref[tile] + bias
        d_logit = valid_of(tile) * d_decay * jax.nn.sigmoid(-logits) * 0.125
        d_bias_ref[...] += jnp.broadcast_to(jnp.sum(d_logit, axis=1, keepdims=True), (BLOCK, TILE))
        d_qkv_ref[rows_of(tile), 3 * width :] = d_logit.T.astype(jnp.bfloat16)
        return none

    lax.fori_loop(0, tiles, finish, 0)


def mixer_forward(length, qkv, logits, bias):
    rows, width = qkv.shape[0], qkv.shape[1] // 3
    tiles = rows // TILE
    f32 = jnp.float32
    return pl.pallas_call(
        forward_kernel,
        out_shape=(
            jax.ShapeDtypeStruct((rows, width), jnp.bfloat16),
            jax.ShapeDtypeStruct((tiles, TILE, 2 * width), f32),
            jax.ShapeDtypeStruct((tiles, BLOCK, TILE), f32),
            jax.ShapeDtypeStruct((tiles, BLOCK, TILE), f32),
            jax.ShapeDtypeStruct((tiles, TILE, TILE), jnp.bfloat16),
        ),
        in_specs=[pl.BlockSpec(memory_space=pltpu.SMEM)] + [pl.BlockSpec(memory_space=pltpu.VMEM)] * 3,
        out_specs=[pl.BlockSpec(memory_space=pltpu.VMEM)] * 5,
        scratch_shapes=[
            pltpu.VMEM((tiles, 4, BLOCK, TILE), f32),
            pltpu.VMEM((BLOCK, 2 * width), f32),
            pltpu.VMEM((PAIR, TILE, TILE), f32),
            pltpu.VMEM((PAIR, TILE, TILE), f32),
            pltpu.VMEM((PAIR, BLOCK, BLOCK, TILE), f32),
        ],
        name="mixer_forward",
    )(length, qkv, logits, bias)


def mixer_backward(length, qkv, logits, bias, back, saved):
    rows, width = qkv.shape[0], qkv.shape[1] // 3
    tiles = rows // TILE
    f32 = jnp.float32
    return pl.pallas_call(
        backward_kernel,
        out_shape=(
            jax.ShapeDtypeStruct((rows, 3 * width + BLOCK), jnp.bfloat16),
            jax.ShapeDtypeStruct((BLOCK, TILE), f32),
        ),
        in_specs=[pl.BlockSpec(memory_space=pltpu.SMEM)] + [pl.BlockSpec(memory_space=pltpu.VMEM)] * 8,
        out_specs=[pl.BlockSpec(memory_space=pltpu.VMEM)] * 2,
        scratch_shapes=[
            pltpu.VMEM((tiles, TILE, 2 * width), f32),
            pltpu.VMEM((tiles, 6, BLOCK, TILE), f32),
            pltpu.VMEM((PAIR, TILE, TILE), f32),
            pltpu.VMEM((PAIR, TILE, TILE), f32),
            pltpu.VMEM((PAIR, TILE, TILE), f32),
            pltpu.VMEM((BLOCK, 2 * width), f32),
            pltpu.VMEM((BLOCK, 2 * width), f32),
            pltpu.VMEM((tiles, TILE, TILE), f32),
            pltpu.VMEM((PAIR, BLOCK, BLOCK, TILE), f32),
        ],
        name="mixer_backward",
    )(length, qkv, logits, bias, back, *saved)


def to_low(values):
    return values.astype(jnp.bfloat16)


def to_wide(values):
    return values.astype(jnp.float32)


def dot_tn(left, right):
    return lax.dot_general(left, right, (((0,), (0,)), ((), ())), preferred_element_type=jnp.float32)


def tie(values, *earlier):
    return lax.optimization_barrier((values,) + earlier)[0]


def ring_order(size):
    return list(range(0, size, 2)) + list(range(size - 1 - size % 2, 0, -2))


def hop_pairs(order, hop):
    size = len(order)
    return [(order[i], order[(i + hop) % size]) for i in range(size)]


def ring_gather(shard, order):
    size = len(order)
    up, down = hop_pairs(order, 1), hop_pairs(order, -1)
    pieces = [shard] + [None] * (size - 1)
    from_low, from_high = shard, shard
    for step in range(1, (size + 1) // 2):
        from_low = lax.ppermute(from_low, "dp", up)
        from_high = lax.ppermute(from_high, "dp", down)
        pieces[size - step], pieces[step] = from_low, from_high
    if size % 2 == 0:
        half = shard.shape[0] // 2
        first = lax.ppermute(from_low[:half], "dp", up)
        second = lax.ppermute(from_high[half:], "dp", down)
        pieces[size // 2] = (first, second)
    return pieces


def ring_scatter(piece_of, order):
    size = len(order)
    up, down = hop_pairs(order, 1), hop_pairs(order, -1)
    half_count = (size - 1) // 2
    up_sum, down_sum = None, None
    if size % 2 == 0:
        farthest = piece_of(size // 2)
        half = farthest.shape[0] // 2
        up_half = lax.ppermute(to_low(farthest[:half]), "dp", up)
        down_half = lax.ppermute(to_low(farthest[half:]), "dp", down)
        up_sum = jnp.concatenate([to_wide(up_half), jnp.zeros(up_half.shape, jnp.float32)], axis=0)
        down_sum = jnp.concatenate([jnp.zeros(down_half.shape, jnp.float32), to_wide(down_half)], axis=0)
    for step in range(half_count, 0, -1):
        up_piece, down_piece = to_wide(piece_of(step)), to_wide(piece_of(size - step))
        if up_sum is not None:
            up_piece, down_piece = up_piece + up_sum, down_piece + down_sum
        up_sum = to_wide(lax.ppermute(to_low(up_piece), "dp", up))
        down_sum = to_wide(lax.ppermute(to_low(down_piece), "dp", down))
    total = to_wide(piece_of(0))
    if up_sum is not None:
        total = total + up_sum + down_sum
    return total


def spread_rows(rows, order):
    size = len(order)
    parts = [rows] + [lax.ppermute(rows, "dp", hop_pairs(order, -hop)) for hop in range(1, size)]
    return jnp.stack(parts)


def scatter_rows(rows, order):
    size = len(order)
    total = rows[0]
    for hop in range(1, size):
        total = total + lax.ppermute(rows[hop], "dp", hop_pairs(order, hop))
    return total


def move_kernel(places_ref, source_ref, target_ref):
    target_ref[...] = source_ref[...]


def move_columns(matrix, places, inverse):
    size = places.shape[0]
    rows, columns = matrix.shape
    width = columns // size
    if width % 128:
        split = matrix.reshape(rows, size, width)
        if inverse:
            places = jnp.argsort(places)
        return jnp.take(split, places, axis=1).reshape(rows, columns)

    def plain(step, places_ref):
        return (0, step)

    def placed(step, places_ref):
        return (0, places_ref[step])

    return pl.pallas_call(
        move_kernel,
        out_shape=jax.ShapeDtypeStruct(matrix.shape, matrix.dtype),
        grid_spec=pltpu.PrefetchScalarGridSpec(
            num_scalar_prefetch=1,
            grid=(size,),
            in_specs=[pl.BlockSpec((rows, width), plain if inverse else placed)],
            out_specs=pl.BlockSpec((rows, width), placed if inverse else plain),
        ),
        cost_estimate=pl.CostEstimate(flops=0, bytes_accessed=2 * matrix.size * matrix.dtype.itemsize, transcendentals=0),
        name="move_columns",
    )(places, matrix)


ROWS = 128
WIDE = 256
LIMIT = 62 * 1024 * 1024


def vmem_call(body, name, out_shape, operands, scratch=(), scalars=1, anywhere=0, flops=0, moved=0):
    spaces = (
        [pl.BlockSpec(memory_space=pltpu.SMEM)] * scalars
        + [pl.BlockSpec(memory_space=pltpu.VMEM)] * (len(operands) - scalars - anywhere)
        + [pl.BlockSpec(memory_space=pl.ANY)] * anywhere
    )
    return pl.pallas_call(
        body,
        out_shape=out_shape,
        in_specs=spaces,
        out_specs=[pl.BlockSpec(memory_space=pltpu.VMEM)] * len(out_shape),
        scratch_shapes=list(scratch),
        compiler_params=pltpu.CompilerParams(vmem_limit_bytes=LIMIT),
        cost_estimate=pl.CostEstimate(flops=flops, bytes_accessed=moved, transcendentals=0),
        name=name,
    )(*operands)


def load_all(sources, target_ref, sems):
    copies, start = [], 0
    for index, source in enumerate(sources):
        rows = source.shape[0]
        copies.append(pltpu.make_async_copy(source, target_ref.at[pl.ds(start, rows)], sems.at[index]))
        start += rows
    for copy in copies:
        copy.start()
    return copies


def flat_pieces(pieces):
    flat = []
    for piece in pieces:
        flat += list(piece) if isinstance(piece, tuple) else [piece]
    return flat


def give_halves(block_ref, parity, parts, columns, kept_refs, sent_refs):
    rows = block_ref.shape[0] // parts // 2
    for part in range(parts):
        kept_refs[part][:, columns] = block_ref[pl.ds((2 * part + parity) * rows, rows), :].astype(jnp.bfloat16)
        sent_refs[part][:, columns] = block_ref[pl.ds((2 * part + 1 - parity) * rows, rows), :].astype(jnp.bfloat16)


def project_call(left, pieces, parity, parts):
    rows, depth = left.shape
    flat = flat_pieces(pieces)
    count = len(flat)
    total = sum(piece.shape[0] for piece in flat)

    def body(parity_ref, left_ref, *refs):
        sources, outs = refs[:count], refs[count : count + 2 * parts]
        weight_ref, block_ref, sems = refs[count + 2 * parts :]
        copies = load_all(sources, weight_ref, sems)
        for copy in copies:
            copy.wait()
        parity = parity_ref[0]

        def one(step, none):
            columns = pl.ds(pl.multiple_of(step * WIDE, WIDE), WIDE)
            block_ref[...] = dot_nt(left_ref[...], weight_ref[columns, :])
            give_halves(block_ref, parity, parts, columns, outs[:parts], outs[parts:])
            return none

        lax.fori_loop(0, total // WIDE, one, 0)

    half = jax.ShapeDtypeStruct((rows // parts // 2, total), jnp.bfloat16)
    outs = vmem_call(
        body, "project", [half] * (2 * parts), (parity, left, *flat),
        scratch=[
            pltpu.VMEM((total, depth), jnp.bfloat16),
            pltpu.VMEM((rows, WIDE), jnp.float32),
            pltpu.SemaphoreType.DMA((count,)),
        ],
        anywhere=count, flops=2 * rows * depth * total, moved=2 * (rows * depth + depth * total + rows * total),
    )
    return outs[:parts], outs[parts:]


def query_call(normed, pieces, slots):
    rows, depth = normed.shape
    flat = flat_pieces(pieces)
    count = len(flat)
    columns_all = flat[0].shape[1]
    wide = columns_all - slots

    def body(normed_ref, *refs):
        sources = refs[:count]
        qkv_ref, logit_ref, weight_ref, sems = refs[count:]
        copies = load_all(sources, weight_ref, sems)
        for copy in copies:
            copy.wait()

        def one(step, none):
            columns = pl.ds(pl.multiple_of(step * WIDE, WIDE), WIDE)
            qkv_ref[:, columns] = dot_nn(normed_ref[...], weight_ref[:, columns]).astype(jnp.bfloat16)
            return none

        lax.fori_loop(0, wide // WIDE, one, 0)
        logits = dot_nn(normed_ref[...], weight_ref[:, wide:])
        for tile in range(rows // TILE):
            logit_ref[tile] = logits[tile * TILE : (tile + 1) * TILE, :].T

    return vmem_call(
        body, "query",
        [
            jax.ShapeDtypeStruct((rows, wide), jnp.bfloat16),
            jax.ShapeDtypeStruct((rows // TILE, slots, TILE), jnp.float32),
        ],
        (normed, *flat),
        scratch=[pltpu.VMEM((depth, columns_all), jnp.bfloat16), pltpu.SemaphoreType.DMA((count,))],
        scalars=0, anywhere=count,
        flops=2 * rows * depth * columns_all, moved=2 * (rows + columns_all) * depth + 2 * rows * columns_all,
    )


def feed_call(normed, back, pieces, parity, earlier, parts):
    rows, depth = normed.shape
    flat = flat_pieces(pieces)
    count = len(flat)
    hidden = flat[0].shape[1] // 3
    given = 0 if earlier is None else 2

    def body(parity_ref, *refs):
        sources = refs[: count + 2 + given]
        outs = refs[count + 2 + given :]
        hidden_ref, pair_ref = outs[:2]
        total_refs = outs[2 : 4 if earlier is None else 4 + 2 * parts]
        outs = outs[2 + len(total_refs) :]
        weight_ref, normed_ref, back_ref, block_ref = outs[:4]
        sems = outs[-1]
        held = [
            pltpu.make_async_copy(sources[count], normed_ref, sems.at[count]),
            pltpu.make_async_copy(sources[count + 1], back_ref, sems.at[count + 1]),
        ]
        held[0].start()
        copies = load_all(sources[:count], weight_ref, sems)
        held[1].start()
        if given:
            sum_ref = outs[4]
            held += [
                pltpu.make_async_copy(sources[count + 2 + i], sum_ref.at[i], sems.at[count + 2 + i]) for i in range(2)
            ]
            held[2].start()
            held[3].start()
        for copy in copies + held:
            copy.wait()

        def act(start, span):
            def columns(base):
                return pl.ds(start + base, span)

            gate_act = dot_nn(normed_ref[...], weight_ref[:, columns(0)])
            up_act = dot_nn(normed_ref[...], weight_ref[:, columns(hidden)])
            d_hidden = dot_nn(back_ref[...], weight_ref[:, columns(2 * hidden)])
            sigma = 1.0 / (1.0 + jnp.exp(-gate_act))
            gated = gate_act * sigma
            hidden_ref[:, columns(0)] = (gated * up_act).astype(jnp.bfloat16)
            pair_ref[:, columns(hidden)] = (d_hidden * gated).astype(jnp.bfloat16)
            pair_ref[:, columns(0)] = (
                d_hidden * up_act * (sigma * (1.0 + gate_act * (1.0 - sigma)))
            ).astype(jnp.bfloat16)

        def act_wide(step, none):
            act(pl.multiple_of(step * WIDE, WIDE), WIDE)
            return none

        lax.fori_loop(0, hidden // WIDE, act_wide, 0)
        if hidden % WIDE:
            act(hidden // WIDE * WIDE, hidden % WIDE)
        parity = parity_ref[0]

        def one(step, none):
            columns = pl.ds(pl.multiple_of(step * WIDE, WIDE), WIDE)
            d_block = dot_nt(pair_ref[...], weight_ref[columns, : 2 * hidden])
            y_block = dot_nt(hidden_ref[...], weight_ref[columns, 2 * hidden :])
            if not given:
                total_refs[0][:, columns] = d_block.astype(jnp.bfloat16)
                total_refs[1][:, columns] = y_block.astype(jnp.bfloat16)
            else:
                block_ref[...] = d_block + sum_ref[0, :, columns].astype(jnp.float32)
                give_halves(block_ref, parity, parts, columns, total_refs[:parts], total_refs[parts : 2 * parts])
                block_ref[...] = y_block + sum_ref[1, :, columns].astype(jnp.float32)
                give_halves(block_ref, parity, 1, columns, total_refs[2 * parts :][:1], total_refs[2 * parts + 1 :])
            return none

        lax.fori_loop(0, depth // WIDE, one, 0)

    low = jnp.bfloat16
    outs = [jax.ShapeDtypeStruct((rows, hidden), low), jax.ShapeDtypeStruct((rows, 2 * hidden), low)]
    if earlier is None:
        outs += [jax.ShapeDtypeStruct((rows, depth), low)] * 2
    else:
        outs += [jax.ShapeDtypeStruct((rows // parts // 2, depth), low)] * (2 * parts)
        outs += [jax.ShapeDtypeStruct((rows // 2, depth), low)] * 2
    scratch = [
        pltpu.VMEM((depth, 3 * hidden), low),
        pltpu.VMEM((rows, depth), low),
        pltpu.VMEM((rows, depth), low),
        pltpu.VMEM((rows, WIDE), jnp.float32),
    ]
    if given:
        scratch.append(pltpu.VMEM((2, rows, depth), low))
    scratch.append(pltpu.SemaphoreType.DMA((count + 2 + given,)))
    return vmem_call(
        body, "feed", outs, (parity, *flat, normed, back, *(earlier or ())),
        scratch=scratch, anywhere=count + 2 + given,
        flops=2 * rows * depth * hidden * 6, moved=2 * (3 * rows * depth + 3 * depth * hidden + 3 * rows * hidden),
    )


def sum_specs(parts, steps, rows, depth):
    share = steps // parts // 2

    def spec(index):
        return pl.BlockSpec((rows, depth), lambda step, scalars: (jnp.clip(step - index * share, 0, share - 1), 0))

    return [spec(index) for index in range(2 * parts)]


def place_row(parts, steps):
    share = steps // parts // 2

    def place(step, scalars):
        span = step // share
        part, other = span // 2, span % 2
        half = jnp.where(other == 0, scalars[0], 1 - scalars[0])
        return ((2 * part + half) * share + step % share, 0)

    return place


def pick_sum(step, share, refs):
    value = refs[0][...]
    for index, ref in enumerate(refs[1:]):
        value = jnp.where(step >= (index + 1) * share, ref[...], value)
    return value.astype(jnp.float32)


def row_call(body, name, scalars, parts, sums, whole, fixed, outs, fixed_outs):
    rows, depth = whole[0].shape
    steps = rows // ROWS
    block = pl.BlockSpec((ROWS, depth), place_row(parts, steps))
    one = pl.BlockSpec((1, depth), lambda step, scalars: (0, 0))
    moved = sum(a.size * a.dtype.itemsize for a in list(sums) + list(whole))
    moved += sum(rows * depth * jnp.dtype(kind).itemsize for kind in outs)
    return pl.pallas_call(
        body,
        out_shape=[jax.ShapeDtypeStruct((rows, depth), kind) for kind in outs]
        + [jax.ShapeDtypeStruct((1, depth), jnp.float32)] * fixed_outs,
        grid_spec=pltpu.PrefetchScalarGridSpec(
            num_scalar_prefetch=1,
            grid=(steps,),
            in_specs=sum_specs(parts, steps, ROWS, depth) + [block] * len(whole) + [one] * len(fixed),
            out_specs=[block] * len(outs) + [one] * fixed_outs,
        ),
        compiler_params=pltpu.CompilerParams(vmem_limit_bytes=LIMIT),
        cost_estimate=pl.CostEstimate(flops=10 * rows * depth, bytes_accessed=moved, transcendentals=0),
        name=name,
    )(scalars, *sums, *whole, *fixed)


def norm_factor(values):
    return lax.rsqrt(jnp.mean(values * values, axis=-1, keepdims=True) + epsilon)


def norm_call(scalars, sums, rows_in, gain):
    parts, steps = len(sums) // 2, rows_in.shape[0] // ROWS

    def body(scalar_ref, *refs):
        sum_refs = refs[: 2 * parts]
        rows_ref, gain_ref, resid_ref, normed_ref = refs[2 * parts :]
        total = pick_sum(pl.program_id(0), steps // parts // 2, sum_refs)
        resid = rows_ref[...].astype(jnp.float32) + total
        resid_ref[...] = resid
        normed_ref[...] = (resid * norm_factor(resid) * gain_ref[...]).astype(jnp.bfloat16)

    return row_call(body, "norm", scalars, parts, sums, [rows_in], [gain], [jnp.float32, jnp.bfloat16], 0)


def norm_back(total, values, gain):
    factor = norm_factor(values)
    hat = values * factor
    scaled = gain * total
    slope = factor * (scaled - hat * jnp.mean(scaled * hat, axis=-1, keepdims=True))
    return slope, jnp.sum(total * hat, axis=0, keepdims=True)


def norm_back_call(scalars, sums, resid, back, gain):
    parts, steps = len(sums) // 2, resid.shape[0] // ROWS

    def body(scalar_ref, *refs):
        sum_refs = refs[: 2 * parts]
        resid_ref, back_ref, gain_ref, d_resid_ref, d_attn_ref, d_gain_ref = refs[2 * parts :]
        step = pl.program_id(0)
        total = pick_sum(step, steps // parts // 2, sum_refs)
        slope, d_gain = norm_back(total, resid_ref[...], gain_ref[...])
        d_resid = back_ref[...].astype(jnp.float32) + slope
        d_resid_ref[...] = d_resid
        d_attn_ref[...] = d_resid.astype(jnp.bfloat16)

        @pl.when(step == 0)
        def _():
            d_gain_ref[...] = d_gain

        @pl.when(step > 0)
        def _():
            d_gain_ref[...] += d_gain

    return row_call(body, "norm_back", scalars, parts, sums, [resid, back], [gain], [jnp.float32, jnp.bfloat16], 1)


def store_placed(target_ref, values, scalar_ref, size):
    share = values.shape[1] // size
    if share % 128:
        target_ref[...] = values
        return
    for index in range(size):
        columns = pl.ds(pl.multiple_of(scalar_ref[1 + index] * share, 128), share)
        target_ref[:, columns] = values[:, index * share : (index + 1) * share]


def replaced(matrix, places):
    size = places.shape[0]
    share = matrix.shape[1] // size
    if share % 128 == 0:
        return matrix
    return jnp.take(matrix.reshape(-1, size, share), jnp.argsort(places), axis=1).reshape(matrix.shape)


def last_call(scalars, sums, d_resid, rows_in, gain, size):
    parts, steps = len(sums) // 2, rows_in.shape[0] // ROWS

    def body(scalar_ref, *refs):
        sum_refs = refs[: 2 * parts]
        d_resid_ref, rows_ref, gain_ref, out_ref, d_gain_ref = refs[2 * parts :]
        step = pl.program_id(0)
        total = pick_sum(step, steps // parts // 2, sum_refs)
        slope, d_gain = norm_back(total, rows_ref[...].astype(jnp.float32), gain_ref[...])
        store_placed(out_ref, d_resid_ref[...] + slope, scalar_ref, size)

        @pl.when(step == 0)
        def _():
            d_gain_ref[...] = d_gain

        @pl.when(step > 0)
        def _():
            d_gain_ref[...] += d_gain

    out, d_gain = row_call(body, "last", scalars, parts, sums, [d_resid, rows_in], [gain], [jnp.float32], 1)
    return replaced(out, scalars[1:]), d_gain


def output_call(scalars, sums, resid, size):
    parts, steps = len(sums) // 2, resid.shape[0] // ROWS

    def body(scalar_ref, *refs):
        sum_refs = refs[: 2 * parts]
        resid_ref, out_ref = refs[2 * parts :]
        total = pick_sum(pl.program_id(0), steps // parts // 2, sum_refs)
        store_placed(out_ref, (resid_ref[...] + total).astype(jnp.bfloat16), scalar_ref, size)

    (out,) = row_call(body, "output", scalars, parts, sums, [resid], [], [jnp.bfloat16], 0)
    return replaced(out, scalars[1:])


def exchange(kept, sent):
    heads = lax.axis_size("head")
    near = [(i, i ^ 1) for i in range(heads)]
    far = [(i, i ^ 2) for i in range(heads)]
    sums = []
    for own, given in zip(kept, sent):
        own = to_low(to_wide(own) + to_wide(lax.ppermute(given, "head", near)))
        own = to_low(to_wide(own) + to_wide(lax.ppermute(own, "head", far)))
        sums += [own, lax.ppermute(own, "head", near)]
    return sums


def per_device(
    inputs,
    lengths,
    gain_attn,
    w_query,
    w_key,
    w_value,
    w_slot,
    gate_bias,
    w_out,
    gain_ffn,
    w_gate,
    w_up,
    w_down,
    cotangent,
):
    size = lax.axis_size("dp")
    order = ring_order(size)
    spots = [order.index(i) for i in range(size)]
    spot = jnp.array(spots, jnp.int32)[lax.axis_index("dp")]
    places = jnp.array(order + order, jnp.int32)[spot + jnp.arange(size, dtype=jnp.int32)]
    parity = jnp.bitwise_and(lax.axis_index("head"), 1).astype(jnp.int32)[None]
    scalars = jnp.concatenate([parity, places])
    share = gain_attn.shape[0]
    width, slots = w_query.shape[1], w_slot.shape[1]
    hidden_count = w_gate.shape[1]
    cut = (hidden_count // WIDE + 1) // 2 * WIDE
    spans = [(0, cut), (cut, hidden_count)]

    mix_shard = jnp.concatenate([w_query, w_key, w_value, w_slot], axis=1)
    mix_pieces = ring_gather(mix_shard, order)
    gains = spread_rows(jnp.concatenate([gain_attn, gain_ffn]), order)
    gain_one = to_wide(gains[:, :share].reshape(1, size * share))
    gain_two = to_wide(gains[:, share:].reshape(1, size * share))
    out_pieces = ring_gather(tie(w_out.T, mix_pieces[2]), order)
    down_rows = w_down.T
    feed_pieces = []
    earlier = out_pieces[2]
    for low, high in spans:
        shard = jnp.concatenate([w_gate[:, low:high], w_up[:, low:high], down_rows[:, low:high]], axis=1)
        pieces = ring_gather(tie(shard, earlier), order)
        earlier = pieces[size // 2 - 1]
        feed_pieces.append(pieces)

    rows_low = move_columns(inputs, places, False)
    back_low = move_columns(cotangent, places, False)
    rows_in = to_wide(rows_low)
    normed = to_low(rows_in * norm_factor(rows_in) * gain_one)

    qkv, logits = query_call(normed, mix_pieces, slots)
    bias = gate_bias[:, None]
    mixed, *saved = mixer_forward(lengths, qkv, logits, bias)
    sums = exchange(*project_call(mixed, out_pieces, parity, 2))
    resid, normed_two = norm_call(scalars, sums, rows_low, gain_two)

    partial, feed_grads = None, []
    for pieces in feed_pieces:
        hidden, pair, *partial = feed_call(normed_two, back_low, pieces, parity, partial, 2)
        grads = [to_low(dot_tn(normed_two, pair)), to_low(dot_tn(back_low, hidden))]

        def piece_of(index, grads=grads):
            return jnp.concatenate([grad[index * share : (index + 1) * share] for grad in grads], axis=1)

        feed_grads.append(ring_scatter(piece_of, order))

    sums = exchange(partial[:2], partial[2:4])
    d_resid, d_attn, grad_gain_two = norm_back_call(scalars, sums, resid, back_low, gain_two)
    full_out = jnp.concatenate(flat_pieces(out_pieces), axis=0)
    d_mixed = to_low(dot_nn(d_attn, full_out))
    grad_out = to_low(dot_tn(d_attn, mixed))
    d_all, d_bias = mixer_backward(lengths, qkv, logits, bias, d_mixed, saved)
    grad_all = to_low(dot_tn(normed, d_all))

    def mix_piece(index):
        rows = slice(index * share, (index + 1) * share)
        return jnp.concatenate([grad_all[rows], grad_out[rows]], axis=1)

    mix_grad = ring_scatter(mix_piece, order)
    sums = exchange(*project_call(d_all, mix_pieces, parity, 2))
    grad_inputs, grad_gain_one = last_call(scalars, sums, d_resid, rows_low, gain_one, size)
    sums = exchange([tie(partial[4], d_mixed)], partial[5:])
    output = output_call(scalars, sums, resid, size)
    small = jnp.concatenate(
        [
            grad_gain_one.reshape(size, share),
            grad_gain_two.reshape(size, share),
            jnp.broadcast_to(d_bias[:, 0], (size, slots)),
        ],
        axis=1,
    )
    small = scatter_rows(small, order)

    def feed_columns(index):
        columns = []
        for grad, (low, high) in zip(feed_grads, spans):
            count = high - low
            columns.append(grad[:, index * count : (index + 1) * count])
        return jnp.concatenate(columns, axis=1)

    return (
        output,
        grad_inputs,
        small[:share],
        mix_grad[:, :width],
        mix_grad[:, width : 2 * width],
        mix_grad[:, 2 * width : 3 * width],
        mix_grad[:, 3 * width : 3 * width + slots],
        small[2 * share :],
        mix_grad[:, 3 * width + slots :].T,
        small[share : 2 * share],
        feed_columns(0),
        feed_columns(1),
        feed_columns(2).T,
    )


def solution(mesh):
    in_specs = (
        P("dp", None),
        P("dp"),
        P("dp"),
        P("dp", "head"),
        P("dp", "head"),
        P("dp", "head"),
        P("dp", "head"),
        P("head"),
        P("head", "dp"),
        P("dp"),
        P("dp", "head"),
        P("dp", "head"),
        P("head", "dp"),
        P("dp", None),
    )
    out_specs = (
        P("dp", None),
        P("dp", None),
        P("dp"),
        P("dp", "head"),
        P("dp", "head"),
        P("dp", "head"),
        P("dp", "head"),
        P("head"),
        P("head", "dp"),
        P("dp"),
        P("dp", "head"),
        P("dp", "head"),
        P("head", "dp"),
    )
    return jax.shard_map(
        per_device, mesh=mesh, in_specs=in_specs, out_specs=out_specs, check_vma=False
    )
```

```python
import jax
import jax.numpy as jnp
from jax import lax
from jax.experimental import pallas as pl
from jax.experimental.pallas import tpu as pltpu
from jax.sharding import PartitionSpec as P

BLOCK = 64
TILE = 128
DP, HEAD = "dp", "head"
epsilon = 1e-06
PAIR = 2


def split_low(values):
    high = values.astype(jnp.bfloat16)
    return high, (values - high.astype(jnp.float32)).astype(jnp.bfloat16)


def dot_nn(left, right):
    return lax.dot_general(left, right, (((1,), (0,)), ((), ())), preferred_element_type=jnp.float32)


def dot_nt(left, right):
    return lax.dot_general(left, right, (((1,), (1,)), ((), ())), preferred_element_type=jnp.float32)


def lane_place():
    lanes = lax.broadcasted_iota(jnp.int32, (BLOCK, TILE), 1)
    return lanes, jnp.bitwise_and(lanes, BLOCK - 1)


def prefix_sum(values, place):
    step = 1
    while step < BLOCK:
        values = values + jnp.where(place >= step, pltpu.roll(values, step, 1), 0.0)
        step *= 2
    return values


def suffix_sum(values, place):
    step = 1
    while step < BLOCK:
        values = values + jnp.where(place < BLOCK - step, pltpu.roll(values, TILE - step, 1), 0.0)
        step *= 2
    return values


def to_band(square):
    rows = lax.broadcasted_iota(jnp.int32, (TILE, TILE), 0)
    step = 1
    while step < TILE:
        square = jnp.where(jnp.bitwise_and(rows, step) != 0, pltpu.roll(square, TILE - step, 1), square)
        step *= 2
    return square.T


def from_band(band):
    return pltpu.roll(band.T, 0, 1, stride=1, stride_axis=0)


def lag_row(lag):
    return slice((TILE - lag) % TILE, (TILE - lag) % TILE + 1)


def fill_products(product_ref, slot, writes, inside):
    product_ref[slot, 0] = writes
    power, powers, reach = inside, [], 1
    while reach < BLOCK:
        powers.append(power)
        for lag in range(reach):
            product_ref[slot, reach + lag] = power * pltpu.roll(product_ref[slot, lag], reach, 1)
        power = power * pltpu.roll(power, reach, 1)
        reach *= 2
    return powers


def lag_total(product_ref, slot, band_ref, start):
    sums = [start, None, None, None]
    for lag in range(BLOCK):
        term = product_ref[slot, lag] * band_ref[slot, lag_row(lag), :]
        held = sums[lag % 4]
        sums[lag % 4] = term if held is None else held + term
    return (sums[0] + sums[1]) + (sums[2] + sums[3])


def lag_mix(product_ref, slot, band_ref, weights):
    for lag in range(BLOCK):
        band_ref[slot, lag_row(lag), :] = jnp.sum(weights * product_ref[slot, lag], axis=0, keepdims=True)


def lag_back(powers, term_of, low, count, stride=1):
    if count == 1:
        return term_of(low)
    half = count // 2
    left = lag_back(powers, term_of, low, half, stride)
    right = lag_back(powers, term_of, low + half, half, stride)
    return left + pltpu.roll(powers[half.bit_length() - 1] * right, TILE - half * stride, 1)


def gate_terms(logits, valid, place):
    log_sig = jnp.minimum(logits, 0.0) - jnp.log1p(jnp.exp(-jnp.abs(logits)))
    logdecay = valid * log_sig * 0.125
    decay = jnp.exp(logdecay)
    series = -logdecay * (1.0 + logdecay * (0.5 + logdecay * (1.0 / 6.0 + logdecay * (1.0 / 24.0))))
    writes = valid * jnp.where(logdecay > -0.03, series, 1.0 - decay)
    inside = jnp.where(place == 0, 0.0, decay)
    before = prefix_sum(logdecay, place)
    after = suffix_sum(logdecay, place) - logdecay
    return decay, writes, inside, before, after


def stacked(values, lanes):
    return jnp.concatenate(
        [jnp.where(lanes < BLOCK, values, 0.0), jnp.where(lanes < BLOCK, 0.0, values)], axis=0
    )


def own_block(square, lanes):
    return jnp.where(lanes < BLOCK, square[:BLOCK], square[BLOCK:])


def forward_kernel(
    length_ref, qkv_ref, logit_ref, bias_ref,
    mixed_ref, state_ref, prob_ref, score_ref, mix_ref,
    gate_ref, carry_ref, band_ref, mix_band_ref, product_ref,
):
    width = mixed_ref.shape[1]
    tiles = mixed_ref.shape[0] // TILE
    scale = width ** -0.5
    lanes, place = lane_place()
    bias = bias_ref[...]

    def valid_of(tile):
        return (lanes + tile * TILE < length_ref[0]).astype(jnp.float32)

    def rows_of(tile):
        return pl.ds(pl.multiple_of(tile * TILE, TILE), TILE)

    def gather_writes(tile, none):
        logits = logit_ref[tile] + bias
        _, writes, inside, before, after = gate_terms(logits, valid_of(tile), place)
        gate_ref[tile, 0] = writes
        gate_ref[tile, 1] = inside
        gate_ref[tile, 2] = jnp.exp(before)
        gate_ref[tile, 3] = jnp.exp(before + after)
        high, low = split_low(stacked(jnp.exp(after) * writes, lanes))
        rows = qkv_ref[rows_of(tile), width:]
        added = dot_nn(high, rows) + dot_nn(low, rows)
        state_ref[tile] = added
        return none

    lax.fori_loop(0, tiles, gather_writes, 0)

    carry_ref[...] = jnp.zeros_like(carry_ref)

    def run_states(tile, none):
        for part in range(2):
            span = pl.ds(part * BLOCK, BLOCK)
            fade = gate_ref[tile, 3, :, part * BLOCK : part * BLOCK + 1]
            carried = carry_ref[...]
            added = state_ref[tile, span, :]
            state_ref[tile, span, :] = carried
            carry_ref[...] = fade * carried + added
        return none

    lax.fori_loop(0, tiles, run_states, 0)

    band_ref[...] = jnp.zeros_like(band_ref)
    mix_band_ref[...] = jnp.zeros_like(mix_band_ref)

    def mix_pair(pair, none):
        both = [(slot, PAIR * pair + slot) for slot in range(PAIR)]
        queries, scores, probs = {}, {}, {}
        for slot, tile in both:
            fill_products(product_ref, slot, gate_ref[tile, 0], gate_ref[tile, 1])
        for slot, tile in both:
            queries[slot] = qkv_ref[rows_of(tile), :width]
            band_ref[slot] = to_band(dot_nt(queries[slot], qkv_ref[rows_of(tile), width : 2 * width]) * scale)
        for slot, tile in both:
            high, low = split_low(state_ref[tile, :, :width])
            carried = own_block(dot_nt(high, queries[slot]) + dot_nt(low, queries[slot]), lanes)
            scores[slot] = gate_ref[tile, 2] * carried * scale
        for slot, tile in both:
            scores[slot] = lag_total(product_ref, slot, band_ref, scores[slot])
        for slot, tile in both:
            top = jnp.max(scores[slot], axis=0, keepdims=True)
            raised = jnp.exp(scores[slot] - top)
            probs[slot] = raised / jnp.sum(raised, axis=0, keepdims=True)
            score_ref[tile] = scores[slot]
            prob_ref[tile] = probs[slot]
        for slot, tile in both:
            lag_mix(product_ref, slot, mix_band_ref, probs[slot])
        for slot, tile in both:
            mixing = from_band(mix_band_ref[slot]).astype(jnp.bfloat16)
            mix_ref[tile] = mixing
            reach = stacked(probs[slot] * gate_ref[tile, 2], lanes).T.astype(jnp.bfloat16)
            result = dot_nn(mixing, qkv_ref[rows_of(tile), 2 * width :]) + dot_nn(
                reach, state_ref[tile, :, width:].astype(jnp.bfloat16)
            )
            rows = lax.broadcasted_iota(jnp.int32, (TILE, 1), 0) + tile * TILE
            mixed_ref[rows_of(tile), :] = jnp.where(rows < length_ref[0], result, 0.0).astype(jnp.bfloat16)
        return none

    lax.fori_loop(0, tiles // PAIR, mix_pair, 0)


def backward_kernel(
    length_ref, qkv_ref, logit_ref, bias_ref, back_ref, state_ref, prob_ref, score_ref, mix_ref,
    d_qkv_ref, d_bias_ref,
    adjoint_ref, gain_ref, key_band_ref, value_band_ref, band_ref, carry_ref, end_ref, cross_ref, product_ref,
):
    width = back_ref.shape[1]
    tiles = back_ref.shape[0] // TILE
    scale = width ** -0.5
    lanes, place = lane_place()
    bias = bias_ref[...]

    def valid_of(tile):
        return (lanes + tile * TILE < length_ref[0]).astype(jnp.float32)

    def rows_of(tile):
        return pl.ds(pl.multiple_of(tile * TILE, TILE), TILE)

    def back_of(tile):
        rows = lax.broadcasted_iota(jnp.int32, (TILE, 1), 0) + tile * TILE
        return jnp.where(rows < length_ref[0], back_ref[rows_of(tile), :], jnp.zeros((), back_ref.dtype))

    band_ref[...] = jnp.zeros_like(band_ref)

    def slopes(pair, none):
        both = [(slot, PAIR * pair + slot) for slot in range(PAIR)]
        fades, powers, queries, keys, backs, gains, d_scores = {}, {}, {}, {}, {}, {}, {}
        for slot, tile in both:
            decay, writes, inside, before, after = gate_terms(logit_ref[tile] + bias, valid_of(tile), place)
            fades[slot] = jnp.exp(before)
            gain_ref[tile, 2] = decay
            gain_ref[tile, 3] = writes
            gain_ref[tile, 4] = jnp.exp(after)
            gain_ref[tile, 5] = jnp.exp(before + after)
            powers[slot] = fill_products(product_ref, slot, writes, inside)
        for slot, tile in both:
            queries[slot] = qkv_ref[rows_of(tile), :width]
            keys[slot] = qkv_ref[rows_of(tile), width : 2 * width]
            backs[slot] = back_of(tile)
            key_band_ref[slot] = to_band(dot_nt(queries[slot], keys[slot]) * scale)
            value_band_ref[slot] = to_band(dot_nt(backs[slot], qkv_ref[rows_of(tile), 2 * width :]))
        for slot, tile in both:
            high, low = split_low(state_ref[tile, :, width:])
            carried = own_block(dot_nt(high, backs[slot]) + dot_nt(low, backs[slot]), lanes)
            gains[slot] = fades[slot] * carried
        for slot, tile in both:
            gains[slot] = lag_total(product_ref, slot, value_band_ref, gains[slot])
        for slot, tile in both:
            probs = prob_ref[tile]
            d_scores[slot] = probs * (gains[slot] - jnp.sum(probs * gains[slot], axis=0, keepdims=True))
            gain_ref[tile, 1] = d_scores[slot] * score_ref[tile] + probs * gains[slot]
        for slot, tile in both:
            lag_mix(product_ref, slot, band_ref, d_scores[slot])
        for slot, tile in both:
            probs = prob_ref[tile]

            def term_of(lag, slot=slot, probs=probs):
                row = lag_row(lag)
                return d_scores[slot] * key_band_ref[slot, row, :] + probs * value_band_ref[slot, row, :]

            group = 8
            for low in range(0, BLOCK, group):
                product_ref[slot, low // group] = lag_back(powers[slot], term_of, low, group)
            gain_ref[tile, 0] = lag_back(
                powers[slot][group.bit_length() - 1 :], lambda index, slot=slot: product_ref[slot, index], 0, BLOCK // group, group
            )
        for slot, tile in both:
            mixing = (from_band(band_ref[slot]) * scale).astype(jnp.bfloat16)
            reach = stacked(d_scores[slot] * fades[slot] * scale, lanes)
            held = stacked(prob_ref[tile] * fades[slot], lanes).astype(jnp.bfloat16)
            d_qkv_ref[rows_of(tile), :width] = (
                dot_nn(mixing, keys[slot])
                + dot_nn(reach.T.astype(jnp.bfloat16), state_ref[tile, :, :width].astype(jnp.bfloat16))
            ).astype(jnp.bfloat16)
            adjoint_ref[tile, :, :width] = dot_nn(reach.astype(jnp.bfloat16), queries[slot])
            adjoint_ref[tile, :, width:] = dot_nn(held, backs[slot])
            d_qkv_ref[rows_of(tile), width : 2 * width] = dot_nn(mixing.T, queries[slot]).astype(jnp.bfloat16)
            d_qkv_ref[rows_of(tile), 2 * width : 3 * width] = dot_nn(mix_ref[tile].T, backs[slot]).astype(jnp.bfloat16)
        return none

    lax.fori_loop(0, tiles // PAIR, slopes, 0)

    carry_ref[...] = jnp.zeros_like(carry_ref)
    end_ref[...] = jnp.zeros_like(end_ref)

    def run_adjoints(count, none):
        tile = tiles - 1 - count
        for part in (1, 0):
            span = pl.ds(part * BLOCK, BLOCK)
            fade = gain_ref[tile, 5, :, part * BLOCK : part * BLOCK + 1]
            carried = carry_ref[...]
            added = adjoint_ref[tile, span, :]
            adjoint_ref[tile, span, :] = carried
            cross_ref[tile, span, :] = jnp.broadcast_to(
                jnp.sum(carried * end_ref[...], axis=1, keepdims=True), (BLOCK, TILE)
            )
            end_ref[...] = state_ref[tile, span, :]
            carry_ref[...] = fade * carried + added
        return none

    lax.fori_loop(0, tiles, run_adjoints, 0)

    d_bias_ref[...] = jnp.zeros_like(d_bias_ref)

    def finish(tile, none):
        key_rows = qkv_ref[rows_of(tile), width : 2 * width]
        value_rows = qkv_ref[rows_of(tile), 2 * width :]
        adjoint = adjoint_ref[tile]
        high, low = split_low(adjoint)
        rows = qkv_ref[rows_of(tile), width:]
        carried = own_block(dot_nt(high, rows) + dot_nt(low, rows), lanes)
        decay, writes, rest = gain_ref[tile, 2], gain_ref[tile, 3], gain_ref[tile, 4]
        d_writes = gain_ref[tile, 0] + rest * carried
        tail = stacked(rest * writes, lanes).T.astype(jnp.bfloat16)
        d_qkv_ref[rows_of(tile), width : 3 * width] = (
            d_qkv_ref[rows_of(tile), width : 3 * width].astype(jnp.float32) + dot_nn(tail, high)
        ).astype(jnp.bfloat16)
        cross = own_block(cross_ref[tile], lanes)
        d_decay = suffix_sum(gain_ref[tile, 1] - writes * d_writes, place) + cross - decay * d_writes
        logits = logit_ref[tile] + bias
        d_logit = valid_of(tile) * d_decay * jax.nn.sigmoid(-logits) * 0.125
        d_bias_ref[...] += jnp.broadcast_to(jnp.sum(d_logit, axis=1, keepdims=True), (BLOCK, TILE))
        d_qkv_ref[rows_of(tile), 3 * width :] = jnp.concatenate([d_logit, jnp.zeros_like(d_logit)], axis=0).T.astype(jnp.bfloat16)
        return none

    lax.fori_loop(0, tiles, finish, 0)


def mixer_forward(length, qkv, logits, bias):
    rows, width = qkv.shape[0], qkv.shape[1] // 3
    tiles = rows // TILE
    f32 = jnp.float32
    return pl.pallas_call(
        forward_kernel,
        out_shape=(
            jax.ShapeDtypeStruct((rows, width), jnp.bfloat16),
            jax.ShapeDtypeStruct((tiles, TILE, 2 * width), f32),
            jax.ShapeDtypeStruct((tiles, BLOCK, TILE), f32),
            jax.ShapeDtypeStruct((tiles, BLOCK, TILE), f32),
            jax.ShapeDtypeStruct((tiles, TILE, TILE), jnp.bfloat16),
        ),
        in_specs=[pl.BlockSpec(memory_space=pltpu.SMEM)] + [pl.BlockSpec(memory_space=pltpu.VMEM)] * 3,
        out_specs=[pl.BlockSpec(memory_space=pltpu.VMEM)] * 5,
        scratch_shapes=[
            pltpu.VMEM((tiles, 4, BLOCK, TILE), f32),
            pltpu.VMEM((BLOCK, 2 * width), f32),
            pltpu.VMEM((PAIR, TILE, TILE), f32),
            pltpu.VMEM((PAIR, TILE, TILE), f32),
            pltpu.VMEM((PAIR, BLOCK, BLOCK, TILE), f32),
        ],
        name="mixer_forward",
    )(length, qkv, logits, bias)


def mixer_backward(length, qkv, logits, bias, back, saved):
    rows, width = qkv.shape[0], qkv.shape[1] // 3
    tiles = rows // TILE
    f32 = jnp.float32
    return pl.pallas_call(
        backward_kernel,
        out_shape=(
            jax.ShapeDtypeStruct((rows, 3 * width + 2 * BLOCK), jnp.bfloat16),
            jax.ShapeDtypeStruct((BLOCK, TILE), f32),
        ),
        in_specs=[pl.BlockSpec(memory_space=pltpu.SMEM)] + [pl.BlockSpec(memory_space=pltpu.VMEM)] * 8,
        out_specs=[pl.BlockSpec(memory_space=pltpu.VMEM)] * 2,
        scratch_shapes=[
            pltpu.VMEM((tiles, TILE, 2 * width), f32),
            pltpu.VMEM((tiles, 6, BLOCK, TILE), f32),
            pltpu.VMEM((PAIR, TILE, TILE), f32),
            pltpu.VMEM((PAIR, TILE, TILE), f32),
            pltpu.VMEM((PAIR, TILE, TILE), f32),
            pltpu.VMEM((BLOCK, 2 * width), f32),
            pltpu.VMEM((BLOCK, 2 * width), f32),
            pltpu.VMEM((tiles, TILE, TILE), f32),
            pltpu.VMEM((PAIR, BLOCK, BLOCK, TILE), f32),
        ],
        name="mixer_backward",
    )(length, qkv, logits, bias, back, *saved)


def to_low(values):
    return values.astype(jnp.bfloat16)


def to_wide(values):
    return values.astype(jnp.float32)


def dot_tn(left, right):
    return lax.dot_general(left, right, (((0,), (0,)), ((), ())), preferred_element_type=jnp.float32)


def tie(values, *earlier):
    return lax.optimization_barrier((values,) + earlier)[0]


def ring_order(size):
    return list(range(0, size, 2)) + list(range(size - 1 - size % 2, 0, -2))


def hop_pairs(order, hop):
    size = len(order)
    return [(order[i], order[(i + hop) % size]) for i in range(size)]


def ring_gather(shard, order):
    size = len(order)
    up, down = hop_pairs(order, 1), hop_pairs(order, -1)
    pieces = [shard] + [None] * (size - 1)
    from_low, from_high = shard, shard
    for step in range(1, (size + 1) // 2):
        from_low = lax.ppermute(from_low, DP, up)
        from_high = lax.ppermute(from_high, DP, down)
        pieces[size - step], pieces[step] = from_low, from_high
    if size % 2 == 0:
        half = shard.shape[0] // 2
        first = lax.ppermute(from_low[:half], DP, up)
        second = lax.ppermute(from_high[half:], DP, down)
        pieces[size // 2] = (first, second)
    return pieces


def ring_scatter(piece_of, order):
    size = len(order)
    up, down = hop_pairs(order, 1), hop_pairs(order, -1)
    half_count = (size - 1) // 2
    up_sum, down_sum = None, None
    if size % 2 == 0:
        farthest = piece_of(size // 2)
        half = farthest.shape[0] // 2
        up_half = lax.ppermute(to_low(farthest[:half]), DP, up)
        down_half = lax.ppermute(to_low(farthest[half:]), DP, down)
        up_sum = jnp.concatenate([to_wide(up_half), jnp.zeros(up_half.shape, jnp.float32)], axis=0)
        down_sum = jnp.concatenate([jnp.zeros(down_half.shape, jnp.float32), to_wide(down_half)], axis=0)
    for step in range(half_count, 0, -1):
        up_piece, down_piece = to_wide(piece_of(step)), to_wide(piece_of(size - step))
        if up_sum is not None:
            up_piece, down_piece = up_piece + up_sum, down_piece + down_sum
        up_sum = to_wide(lax.ppermute(to_low(up_piece), DP, up))
        down_sum = to_wide(lax.ppermute(to_low(down_piece), DP, down))
    return piece_of(0), to_low(up_sum), to_low(down_sum)


def total_sum(values, axis):
    count = lax.axis_size(axis)
    step = 1
    while step < count:
        values = values + lax.ppermute(values, axis, [(i, i ^ step) for i in range(count)])
        step *= 2
    return values


def move_kernel(places_ref, source_ref, target_ref):
    target_ref[...] = source_ref[...]


def move_columns(matrix, places, inverse):
    size = places.shape[0]
    rows, columns = matrix.shape
    width = columns // size
    if width % 128:
        split = matrix.reshape(rows, size, width)
        if inverse:
            places = jnp.argsort(places)
        return jnp.take(split, places, axis=1).reshape(rows, columns)

    def plain(step, places_ref):
        return (0, step)

    def placed(step, places_ref):
        return (0, places_ref[step])

    return pl.pallas_call(
        move_kernel,
        out_shape=jax.ShapeDtypeStruct(matrix.shape, matrix.dtype),
        grid_spec=pltpu.PrefetchScalarGridSpec(
            num_scalar_prefetch=1,
            grid=(size,),
            in_specs=[pl.BlockSpec((rows, width), plain if inverse else placed)],
            out_specs=pl.BlockSpec((rows, width), placed if inverse else plain),
        ),
        cost_estimate=pl.CostEstimate(flops=0, bytes_accessed=2 * matrix.size * matrix.dtype.itemsize, transcendentals=0),
    )(places, matrix)


ROWS = 128
WIDE = 256
LIMIT = 62 * 1024 * 1024


def vmem_call(body, out_shape, operands, scratch=(), scalars=1, anywhere=0, flops=0, moved=0):
    spaces = (
        [pl.BlockSpec(memory_space=pltpu.SMEM)] * scalars
        + [pl.BlockSpec(memory_space=pltpu.VMEM)] * (len(operands) - scalars - anywhere)
        + [pl.BlockSpec(memory_space=pl.ANY)] * anywhere
    )
    return pl.pallas_call(
        body,
        out_shape=out_shape,
        in_specs=spaces,
        out_specs=[pl.BlockSpec(memory_space=pltpu.VMEM)] * len(out_shape),
        scratch_shapes=list(scratch),
        compiler_params=pltpu.CompilerParams(vmem_limit_bytes=LIMIT),
        cost_estimate=pl.CostEstimate(flops=flops, bytes_accessed=moved, transcendentals=0),
    )(*operands)


def load_blocks(sources, target_ref, sems, blocks, low=0):
    groups = []
    for block in blocks:
        copies = []
        for first, span in block:
            start = 0
            for source in sources:
                rows = source.shape[0]
                index = sum(map(len, groups)) + len(copies)
                copies.append(
                    pltpu.make_async_copy(
                        source.at[:, pl.ds(low + first, span)],
                        target_ref.at[pl.ds(start, rows), pl.ds(first, span)],
                        sems.at[index],
                    )
                )
                start += rows
        groups.append(copies)
    for copies in groups:
        for copy in copies:
            copy.start()
    return groups


def finish(copies):
    for copy in copies:
        copy.wait()


def flat_pieces(pieces):
    flat = []
    for piece in pieces:
        flat += list(piece) if isinstance(piece, tuple) else [piece]
    return flat


def give_halves(block_ref, parity, parts, columns, kept_refs, sent_refs):
    rows = block_ref.shape[0] // parts // 2
    for part in range(parts):
        kept_refs[part][:, columns] = block_ref[pl.ds((2 * part + parity) * rows, rows), :].astype(jnp.bfloat16)
        sent_refs[part][:, columns] = block_ref[pl.ds((2 * part + 1 - parity) * rows, rows), :].astype(jnp.bfloat16)


def project_call(left, pieces, parity, parts, low, keep):
    rows, depth = left.shape
    flat = flat_pieces(pieces)
    count = len(flat)
    total = sum(piece.shape[0] for piece in flat)

    def body(parity_ref, left_ref, *refs):
        sources, outs = refs[:count], refs[count:]
        block_ref, sems = outs[-2:]
        weight_ref = outs[-3]
        finish(load_blocks(sources, weight_ref, sems, [[(0, depth)]], low)[0])
        parity = parity_ref[0]

        def one(step, none):
            columns = pl.ds(pl.multiple_of(step * WIDE, WIDE), WIDE)
            block_ref[...] = dot_nt(left_ref[...], weight_ref[columns, :])
            give_halves(block_ref, parity, parts, columns, outs[:parts], outs[parts : 2 * parts])
            return none

        lax.fori_loop(0, total // WIDE, one, 0)

    half = jax.ShapeDtypeStruct((rows // parts // 2, total), jnp.bfloat16)
    weight = (total, depth)
    outs = vmem_call(
        body,
        [half] * (2 * parts) + ([jax.ShapeDtypeStruct(weight, jnp.bfloat16)] if keep else []),
        (parity, left, *flat),
        scratch=([] if keep else [pltpu.VMEM(weight, jnp.bfloat16)])
        + [
            pltpu.VMEM((rows, WIDE), jnp.float32),
            pltpu.SemaphoreType.DMA((count,)),
        ],
        anywhere=count, flops=2 * rows * depth * total, moved=2 * (rows * depth + depth * total + rows * total),
    )
    return outs[:parts], outs[parts : 2 * parts], outs[2 * parts :]


def query_call(rows_low, factor, pieces, slots, columns_all):
    rows, depth = rows_low.shape
    flat = flat_pieces(pieces)
    count = len(flat)
    wide = columns_all - 2 * slots
    blocks = [[(wide, 2 * slots)]] + [[(start, 2 * WIDE)] for start in range(0, wide, 2 * WIDE)]

    def body(rows_ref, factor_ref, *refs):
        sources = refs[:count]
        qkv_ref, logit_ref, normed_ref, gain_ref, weight_ref, sems = refs[count:]
        groups = load_blocks(sources, weight_ref, sems, blocks)
        finish(groups[0])
        gain_ref[...] = weight_ref[:, wide:].astype(jnp.float32).T[slots : slots + 8]

        def norm_rows(step, none):
            span = pl.ds(pl.multiple_of(step * TILE, TILE), TILE)
            values = rows_ref[span, :].astype(jnp.float32)
            normed_ref[span, :] = (values * factor_ref[span, :] * gain_ref[0:1, :]).astype(jnp.bfloat16)
            return none

        lax.fori_loop(0, rows // TILE, norm_rows, 0)
        logits = dot_nn(normed_ref[...], weight_ref[:, wide:])
        for tile in range(rows // TILE):
            logit_ref[tile] = logits[tile * TILE : (tile + 1) * TILE, :].T[:slots]
        for copies in groups[1:]:
            finish(copies)

        def one(step, none):
            columns = pl.ds(pl.multiple_of(step * WIDE, WIDE), WIDE)
            qkv_ref[:, columns] = dot_nn(normed_ref[...], weight_ref[:, columns]).astype(jnp.bfloat16)
            return none

        lax.fori_loop(0, wide // WIDE, one, 0)

    return vmem_call(
        body,
        [
            jax.ShapeDtypeStruct((rows, wide), jnp.bfloat16),
            jax.ShapeDtypeStruct((rows // TILE, slots, TILE), jnp.float32),
            jax.ShapeDtypeStruct((rows, depth), jnp.bfloat16),
            jax.ShapeDtypeStruct((8, depth), jnp.float32),
        ],
        (rows_low, factor, *flat),
        scratch=[pltpu.VMEM((depth, columns_all), jnp.bfloat16), pltpu.SemaphoreType.DMA((count * len(blocks),))],
        scalars=0, anywhere=count,
        flops=2 * rows * depth * columns_all, moved=2 * (rows + columns_all) * depth + 2 * rows * columns_all,
    )


def feed_call(normed, back, pieces, parity, earlier, parts):
    rows, depth = normed.shape
    flat = flat_pieces(pieces)
    count = len(flat)
    hidden = flat[0].shape[1] // 3
    given = 0 if earlier is None else 2
    blocks = [
        [(part * hidden, WIDE) for part in range(3)],
        [(part * hidden + WIDE, hidden - WIDE) for part in range(3)],
    ]

    def body(parity_ref, *refs):
        sources = refs[: count + 2 + given]
        outs = refs[count + 2 + given :]
        hidden_ref, pair_ref = outs[:2]
        total_refs = outs[2 : 4 if earlier is None else 4 + 2 * parts]
        outs = outs[2 + len(total_refs) :]
        weight_ref, normed_ref, back_ref, block_ref = outs[:4]
        sems = outs[-1]
        held = [
            pltpu.make_async_copy(sources[count], normed_ref, sems.at[6 * count]),
            pltpu.make_async_copy(sources[count + 1], back_ref, sems.at[6 * count + 1]),
        ]
        held[0].start()
        held[1].start()
        groups = load_blocks(sources[:count], weight_ref, sems, blocks)
        if given:
            sum_ref = outs[4]
            held += [
                pltpu.make_async_copy(sources[count + 2 + i], sum_ref.at[i], sems.at[6 * count + 2 + i]) for i in range(2)
            ]
            held[2].start()
            held[3].start()

        def act(start, span):
            def columns(base):
                return pl.ds(start + base, span)

            gate_act = dot_nn(normed_ref[...], weight_ref[:, columns(0)])
            up_act = dot_nn(normed_ref[...], weight_ref[:, columns(hidden)])
            d_hidden = dot_nn(back_ref[...], weight_ref[:, columns(2 * hidden)])
            sigma = 1.0 / (1.0 + jnp.exp(-gate_act))
            gated = gate_act * sigma
            hidden_ref[:, columns(0)] = (gated * up_act).astype(jnp.bfloat16)
            pair_ref[:, columns(hidden)] = (d_hidden * gated).astype(jnp.bfloat16)
            pair_ref[:, columns(0)] = (
                d_hidden * up_act * (sigma * (1.0 + gate_act * (1.0 - sigma)))
            ).astype(jnp.bfloat16)

        finish(held[:2])
        finish(groups[0])
        act(0, WIDE)
        for copies in groups[1:]:
            finish(copies)

        def act_wide(step, none):
            act(pl.multiple_of(step * WIDE, WIDE), WIDE)
            return none

        lax.fori_loop(1, hidden // WIDE, act_wide, 0)
        if hidden % WIDE:
            act(hidden // WIDE * WIDE, hidden % WIDE)
        finish(held[2:])
        parity = parity_ref[0]

        def one(step, none):
            columns = pl.ds(pl.multiple_of(step * WIDE, WIDE), WIDE)
            d_block = dot_nt(pair_ref[...], weight_ref[columns, : 2 * hidden])
            y_block = dot_nt(hidden_ref[...], weight_ref[columns, 2 * hidden :])
            if not given:
                total_refs[0][:, columns] = d_block.astype(jnp.bfloat16)
                total_refs[1][:, columns] = y_block.astype(jnp.bfloat16)
            else:
                block_ref[...] = d_block + sum_ref[0, :, columns].astype(jnp.float32)
                give_halves(block_ref, parity, parts, columns, total_refs[:parts], total_refs[parts : 2 * parts])
                block_ref[...] = y_block + sum_ref[1, :, columns].astype(jnp.float32)
                give_halves(block_ref, parity, 1, columns, total_refs[2 * parts :][:1], total_refs[2 * parts + 1 :])
            return none

        lax.fori_loop(0, depth // WIDE, one, 0)

    low = jnp.bfloat16
    outs = [jax.ShapeDtypeStruct((rows, hidden), low), jax.ShapeDtypeStruct((rows, 2 * hidden), low)]
    if earlier is None:
        outs += [jax.ShapeDtypeStruct((rows, depth), low)] * 2
    else:
        outs += [jax.ShapeDtypeStruct((rows // parts // 2, depth), low)] * (2 * parts)
        outs += [jax.ShapeDtypeStruct((rows // 2, depth), low)] * 2
    scratch = [
        pltpu.VMEM((depth, 3 * hidden), low),
        pltpu.VMEM((rows, depth), low),
        pltpu.VMEM((rows, depth), low),
        pltpu.VMEM((rows, WIDE), jnp.float32),
    ]
    if given:
        scratch.append(pltpu.VMEM((2, rows, depth), low))
    scratch.append(pltpu.SemaphoreType.DMA((6 * count + 2 + given,)))
    return vmem_call(
        body, outs, (parity, *flat, normed, back, *(earlier or ())),
        scratch=scratch, anywhere=count + 2 + given,
        flops=2 * rows * depth * hidden * 6, moved=2 * (3 * rows * depth + 3 * depth * hidden + 3 * rows * hidden),
    )


def sum_specs(parts, steps, rows, depth):
    share = steps // parts // 2

    def spec(index):
        return pl.BlockSpec((rows, depth), lambda step, scalars: (jnp.clip(step - index * share, 0, share - 1), 0))

    return [spec(index) for index in range(2 * parts)]


def place_row(parts, steps):
    share = steps // parts // 2

    def place(step, scalars):
        span = step // share
        part, other = span // 2, span % 2
        half = jnp.where(other == 0, scalars[0], 1 - scalars[0])
        return ((2 * part + half) * share + step % share, 0)

    return place


def pick_sum(step, share, refs):
    value = refs[0][...]
    for index, ref in enumerate(refs[1:]):
        value = jnp.where(step >= (index + 1) * share, ref[...], value)
    return value.astype(jnp.float32)


def row_call(body, scalars, parts, sums, whole, fixed, outs, narrow=()):
    rows, depth = whole[0].shape
    steps = rows // ROWS
    place = place_row(parts, steps)
    block = pl.BlockSpec((ROWS, depth), place)
    ones = [pl.BlockSpec(array.shape, lambda step, scalars: (0, 0)) for array in fixed]
    moved = sum(a.size * a.dtype.itemsize for a in list(sums) + list(whole))
    moved += sum(rows * depth * jnp.dtype(kind).itemsize for kind in outs)
    return pl.pallas_call(
        body,
        out_shape=[jax.ShapeDtypeStruct((rows, depth), kind) for kind in outs]
        + [jax.ShapeDtypeStruct((rows, count), jnp.bfloat16) for count in narrow],
        grid_spec=pltpu.PrefetchScalarGridSpec(
            num_scalar_prefetch=1,
            grid=(steps,),
            in_specs=sum_specs(parts, steps, ROWS, depth) + [block] * len(whole) + ones,
            out_specs=[block] * len(outs) + [pl.BlockSpec((ROWS, count), place) for count in narrow],
        ),
        compiler_params=pltpu.CompilerParams(vmem_limit_bytes=LIMIT),
        cost_estimate=pl.CostEstimate(flops=10 * rows * depth, bytes_accessed=moved, transcendentals=0),
    )(scalars, *sums, *whole, *fixed)


def norm_factor(values):
    return lax.rsqrt(jnp.mean(values * values, axis=-1, keepdims=True) + epsilon)


def norm_call(scalars, sums, rows_in, gain):
    parts, steps = len(sums) // 2, rows_in.shape[0] // ROWS

    def body(scalar_ref, *refs):
        sum_refs = refs[: 2 * parts]
        rows_ref, gain_ref, resid_ref, normed_ref = refs[2 * parts :]
        total = pick_sum(pl.program_id(0), steps // parts // 2, sum_refs)
        resid = rows_ref[...].astype(jnp.float32) + total
        resid_ref[...] = resid.astype(jnp.bfloat16)
        normed_ref[...] = (resid * norm_factor(resid) * gain_ref[...]).astype(jnp.bfloat16)

    return row_call(body, scalars, parts, sums, [rows_in], [gain], [jnp.bfloat16, jnp.bfloat16])


def norm_back(total, values, gain):
    factor = norm_factor(values)
    hat = values * factor
    scaled = gain * total
    return factor * (scaled - hat * jnp.mean(scaled * hat, axis=-1, keepdims=True))


def norm_back_call(scalars, sums, resid, back, gain, full_out):
    parts, steps = len(sums) // 2, resid.shape[0] // ROWS

    def body(scalar_ref, *refs):
        sum_refs = refs[: 2 * parts]
        resid_ref, back_ref, gain_ref, out_ref, d_attn_ref, d_mixed_ref = refs[2 * parts :]
        total = pick_sum(pl.program_id(0), steps // parts // 2, sum_refs)
        slope = norm_back(total, resid_ref[...].astype(jnp.float32), gain_ref[...])
        d_attn = (back_ref[...].astype(jnp.float32) + slope).astype(jnp.bfloat16)
        d_attn_ref[...] = d_attn
        d_mixed_ref[...] = dot_nn(d_attn, out_ref[...]).astype(jnp.bfloat16)

    return row_call(body, scalars, parts, sums, [resid, back], [gain, full_out], [jnp.bfloat16], [full_out.shape[1]])


def store_placed(target_ref, values, scalar_ref, size):
    share = values.shape[1] // size
    if share % 128:
        target_ref[...] = values
        return
    for index in range(size):
        columns = pl.ds(pl.multiple_of(scalar_ref[1 + index] * share, 128), share)
        target_ref[:, columns] = values[:, index * share : (index + 1) * share]


def replaced(matrix, places):
    size = places.shape[0]
    share = matrix.shape[1] // size
    if share % 128 == 0:
        return matrix
    return jnp.take(matrix.reshape(-1, size, share), jnp.argsort(places), axis=1).reshape(matrix.shape)


def last_call(scalars, sums, d_resid, rows_in, gain, size):
    parts, steps = len(sums) // 2, rows_in.shape[0] // ROWS

    def body(scalar_ref, *refs):
        sum_refs = refs[: 2 * parts]
        d_resid_ref, rows_ref, gain_ref, out_ref = refs[2 * parts :]
        total = pick_sum(pl.program_id(0), steps // parts // 2, sum_refs)
        slope = norm_back(total, rows_ref[...].astype(jnp.float32), gain_ref[...])
        store_placed(out_ref, d_resid_ref[...].astype(jnp.float32) + slope, scalar_ref, size)

    (out,) = row_call(body, scalars, parts, sums, [d_resid, rows_in], [gain], [jnp.float32])
    return replaced(out, scalars[1:])


def output_call(scalars, sums, resid, size):
    parts, steps = len(sums) // 2, resid.shape[0] // ROWS

    def body(scalar_ref, *refs):
        sum_refs = refs[: 2 * parts]
        resid_ref, out_ref = refs[2 * parts :]
        total = pick_sum(pl.program_id(0), steps // parts // 2, sum_refs)
        store_placed(out_ref, (resid_ref[...].astype(jnp.float32) + total).astype(jnp.bfloat16), scalar_ref, size)

    (out,) = row_call(body, scalars, parts, sums, [resid], [], [jnp.bfloat16])
    return replaced(out, scalars[1:])


def sum_refs_of(refs):
    total = refs[0][...].astype(jnp.float32)
    for ref in refs[1:]:
        total = total + ref[...].astype(jnp.float32)
    return total


def finish_feed(grads, w_gate, w_up, spans):
    share, count = w_gate.shape

    def body(*refs):
        grad_refs = refs[: len(grads)]
        gate_ref, up_ref, d_gate_ref, d_up_ref, d_down_ref, gain_ref = refs[len(grads) :]
        for index, (low, high) in enumerate(spans):
            span = high - low
            total = sum_refs_of(grad_refs[3 * index : 3 * index + 3])
            d_gate_ref[:, low:high] = total[:, :span]
            d_up_ref[:, low:high] = total[:, span : 2 * span]
            d_down_ref[low:high, :] = total[:, 2 * span :].T
        gain_ref[...] = jnp.sum(
            gate_ref[...].astype(jnp.float32) * d_gate_ref[...] + up_ref[...].astype(jnp.float32) * d_up_ref[...],
            axis=1, keepdims=True,
        )

    shapes = [(share, count), (share, count), (count, share), (share, 1)]
    return vmem_call(
        body, [jax.ShapeDtypeStruct(shape, jnp.float32) for shape in shapes],
        (*grads, w_gate, w_up), scalars=0, moved=share * count * 36,
    )


def finish_mix(grads, mix_shard, width, slots):
    share = mix_shard.shape[0]
    used, start = 3 * width + slots, 3 * width + 2 * BLOCK

    def body(*refs):
        grad_refs = refs[: len(grads)]
        shard_ref, query_ref, key_ref, value_ref, slot_ref, out_ref, gain_ref = refs[len(grads) :]
        total = sum_refs_of(grad_refs)
        for index, ref in enumerate((query_ref, key_ref, value_ref)):
            ref[...] = total[:, index * width : (index + 1) * width]
        slot_ref[...] = total[:, 3 * width : used]
        out_ref[...] = total[:, start:].T
        gain_ref[...] = jnp.sum(shard_ref[:, :used].astype(jnp.float32) * total[:, :used], axis=1, keepdims=True)

    shapes = [(share, width)] * 3 + [(share, slots), (width, share), (share, 1)]
    return vmem_call(
        body, [jax.ShapeDtypeStruct(shape, jnp.float32) for shape in shapes],
        (*grads, mix_shard), scalars=0, moved=share * start * 14,
    )


def exchange(kept, sent):
    heads = lax.axis_size(HEAD)
    near = [(i, i ^ 1) for i in range(heads)]
    far = [(i, i ^ 2) for i in range(heads)]
    sums = []
    for own, given in zip(kept, sent):
        own = to_low(to_wide(own) + to_wide(lax.ppermute(given, HEAD, near)))
        own = to_low(to_wide(own) + to_wide(lax.ppermute(own, HEAD, far)))
        sums += [own, lax.ppermute(own, HEAD, near)]
    return sums


def layer(
    inputs,
    lengths,
    gain_attn,
    w_query,
    w_key,
    w_value,
    w_slot,
    gate_bias,
    w_out,
    gain_ffn,
    w_gate,
    w_up,
    w_down,
    cotangent,
):
    size = lax.axis_size(DP)
    order = ring_order(size)
    spots = [order.index(i) for i in range(size)]
    spot = jnp.array(spots, jnp.int32)[lax.axis_index(DP)]
    places = jnp.array(order + order, jnp.int32)[spot + jnp.arange(size, dtype=jnp.int32)]
    parity = jnp.bitwise_and(lax.axis_index(HEAD), 1).astype(jnp.int32)[None]
    scalars = jnp.concatenate([parity, places])
    share = gain_attn.shape[0]
    width, slots = w_query.shape[1], w_slot.shape[1]
    hidden_count = w_gate.shape[1]
    cut = (hidden_count // WIDE + 1) // 2 * WIDE
    spans = [(0, cut), (cut, hidden_count)]

    spare = jnp.zeros((share, 2 * BLOCK - slots - 2), w_slot.dtype)
    mix_shard = jnp.concatenate(
        [w_query, w_key, w_value, w_slot, gain_attn[:, None], gain_ffn[:, None], spare, w_out.T], axis=1
    )
    mix_count = 3 * width + 2 * BLOCK
    mix_pieces = ring_gather(mix_shard, order)
    down_rows = w_down.T
    feed_pieces = []
    for low, high in spans:
        shard = jnp.concatenate([w_gate[:, low:high], w_up[:, low:high], down_rows[:, low:high]], axis=1)
        feed_pieces.append(ring_gather(tie(shard, *flat_pieces([mix_pieces[size // 2]])), order))

    rows_low = move_columns(inputs, places, False)
    factor = norm_factor(to_wide(rows_low))
    back_low = move_columns(cotangent, places, False)
    rows_low, factor, _ = lax.optimization_barrier((rows_low, factor, back_low))

    qkv, logits, normed, gains = query_call(rows_low, factor, mix_pieces, slots, mix_count)
    gain_one, gain_two = gains[0:1], gains[1:2]
    bias = gate_bias[:, None]
    mixed, *saved = mixer_forward(lengths, qkv, logits, bias)
    kept, sent, (full_out,) = project_call(mixed, mix_pieces, parity, 2, mix_count, True)
    sums = exchange(kept, sent)
    resid, normed_two = norm_call(scalars, sums, rows_low, gain_two)

    middle = size // 2

    def grads_of(pairs):
        span = slice(middle * share, (middle + 1) * share)
        far = to_low(jnp.concatenate([dot_tn(left[:, span], right) for left, right in pairs], axis=1))
        grads = [to_low(dot_tn(left, right)) for left, right in pairs]

        def piece_of(index):
            if index == middle:
                return far
            return jnp.concatenate([grad[index * share : (index + 1) * share] for grad in grads], axis=1)

        return piece_of

    partial, feed_grads = None, []
    for pieces in feed_pieces:
        hidden, pair, *partial = feed_call(normed_two, back_low, pieces, parity, partial, 2)
        piece_of = grads_of([(normed_two, pair), (back_low, hidden)])
        feed_grads += ring_scatter(piece_of, order)

    sums = exchange(partial[:2], partial[2:4])
    d_attn, d_mixed = norm_back_call(scalars, sums, resid, back_low, gain_two, full_out)
    d_all, d_bias = mixer_backward(lengths, qkv, logits, bias, d_mixed, saved)
    bias_sum = total_sum(d_bias[:, 0], DP)
    mix_grads = ring_scatter(grads_of([(normed, d_all), (d_attn, mixed)]), order)
    kept, sent, _ = project_call(d_all, mix_pieces, parity, 2, 0, False)
    sums = exchange(kept, sent)
    early = exchange([partial[4]], partial[5:])
    output = output_call(scalars, early, resid, size)
    *feed_out, gain_sum_two = finish_feed(feed_grads, w_gate, w_up, spans)
    sums[0] = tie(sums[0], output)
    grad_inputs = last_call(scalars, sums, d_attn, rows_low, gain_one, size)
    *mix_out, gain_sum_one = finish_mix(mix_grads, mix_shard, width, slots)
    gain_sums = total_sum(jnp.stack([gain_sum_one[:, 0], gain_sum_two[:, 0]]), HEAD)

    return (
        output,
        grad_inputs,
        gain_sums[0] / to_wide(gain_attn),
        *mix_out[:4],
        bias_sum,
        mix_out[4],
        gain_sums[1] / to_wide(gain_ffn),
        *feed_out,
    )


def solution(mesh):
    in_specs = (
        P(DP, None),
        P(DP),
        P(DP),
        P(DP, HEAD),
        P(DP, HEAD),
        P(DP, HEAD),
        P(DP, HEAD),
        P(HEAD),
        P(HEAD, DP),
        P(DP),
        P(DP, HEAD),
        P(DP, HEAD),
        P(HEAD, DP),
        P(DP, None),
    )
    out_specs = (
        P(DP, None),
        P(DP, None),
        P(DP),
        P(DP, HEAD),
        P(DP, HEAD),
        P(DP, HEAD),
        P(DP, HEAD),
        P(HEAD),
        P(HEAD, DP),
        P(DP),
        P(DP, HEAD),
        P(DP, HEAD),
        P(HEAD, DP),
    )
    return jax.shard_map(layer, mesh=mesh, in_specs=in_specs, out_specs=out_specs, check_vma=False)
```

```python
import jax
import jax.numpy as jnp
from jax import lax
from jax.experimental import pallas as pl
from jax.experimental.pallas import tpu as pltpu
from jax.sharding import PartitionSpec as P

BLOCK = 64
TILE = 128
DP, HEAD = "dp", "head"
epsilon = 1e-06
PAIR = 2
LAGS = 16


def split_low(values):
    high = values.astype(jnp.bfloat16)
    return high, (values - high.astype(jnp.float32)).astype(jnp.bfloat16)


def dot_nn(left, right):
    return lax.dot_general(left, right, (((1,), (0,)), ((), ())), preferred_element_type=jnp.float32)


def dot_nt(left, right):
    return lax.dot_general(left, right, (((1,), (1,)), ((), ())), preferred_element_type=jnp.float32)


def lane_place():
    lanes = lax.broadcasted_iota(jnp.int32, (BLOCK, TILE), 1)
    return lanes, jnp.bitwise_and(lanes, BLOCK - 1)


def suffix_sum(values, place):
    step = 1
    while step < BLOCK:
        values = values + jnp.where(place < BLOCK - step, pltpu.roll(values, TILE - step, 1), 0.0)
        step *= 2
    return values


def square_iotas():
    return (
        lax.broadcasted_iota(jnp.int32, (TILE, TILE), 0),
        lax.broadcasted_iota(jnp.int32, (TILE, TILE), 1),
    )


def level_masks():
    rows, columns = square_iotas()
    masks = []
    for half in (LAGS, 2 * LAGS):
        same = jnp.bitwise_and(rows, -2 * half) == jnp.bitwise_and(columns, -2 * half)
        apart = (jnp.bitwise_and(rows, half) == 0) & (jnp.bitwise_and(columns, half) != 0)
        masks.append(same & apart)
    return masks


def level_parts(square, masks):
    return jnp.concatenate([jnp.where(mask, square, 0.0) for mask in masks], axis=1)


def take_band(square, band_ref, slot):
    rows, columns = square_iotas()
    apart = columns - rows
    for lag in range(LAGS):
        band_ref[slot, lag : lag + 1, :] = jnp.sum(jnp.where(apart == lag, square, 0.0), axis=0, keepdims=True)


def put_band(square, band_ref, slot):
    rows, columns = square_iotas()
    apart = columns - rows
    for lag in range(LAGS):
        square = jnp.where(apart == lag, band_ref[slot, lag : lag + 1, :], square)
    return square


def fill_products(product_ref, slot, writes, inside):
    product_ref[slot, 0] = writes
    power, powers, reach = inside, [], 1
    while reach < LAGS:
        powers.append(power)
        for lag in range(reach):
            product_ref[slot, reach + lag] = power * pltpu.roll(product_ref[slot, lag], reach, 1)
        power = power * pltpu.roll(power, reach, 1)
        reach *= 2
    return powers


def lag_total(product_ref, slot, band_ref, start):
    sums = [start, None]
    for lag in range(LAGS):
        term = product_ref[slot, lag] * band_ref[slot, lag : lag + 1, :]
        held = sums[lag % 2]
        sums[lag % 2] = term if held is None else held + term
    return sums[0] + sums[1]


def lag_mix(product_ref, slot, band_ref, weights):
    for lag in range(LAGS):
        band_ref[slot, lag : lag + 1, :] = jnp.sum(weights * product_ref[slot, lag], axis=0, keepdims=True)


def lag_back(powers, term_of, low, count):
    if count == 1:
        return term_of(low)
    half = count // 2
    left = lag_back(powers, term_of, low, half)
    right = lag_back(powers, term_of, low + half, half)
    return left + pltpu.roll(powers[half.bit_length() - 1] * right, TILE - half, 1)


def two_rows(values):
    high, low = split_low(values)
    return jnp.concatenate([high, low], axis=0)


def level_total(near, parts, faded):
    high, low = split_low(parts)
    lefts = jnp.concatenate([two_rows(left) for left in near], axis=0)
    tall = dot_nn(lefts, high)
    short = dot_nn(jnp.concatenate([split_low(left)[0] for left in near], axis=0), low)
    total = 0.0
    for index, right in enumerate(faded):
        span = slice(index * TILE, (index + 1) * TILE)
        rows = tall[2 * index * BLOCK : 2 * (index + 1) * BLOCK, span]
        total = total + right * (rows[:BLOCK] + rows[BLOCK:] + short[index * BLOCK : (index + 1) * BLOCK, span])
    return total


def level_mix(square, near, faded, masks):
    for left, right, mask in zip(near, faded, masks):
        square = jnp.where(
            mask,
            lax.dot_general(
                left.astype(jnp.bfloat16), right.astype(jnp.bfloat16), (((0,), (0,)), ((), ())),
                preferred_element_type=jnp.float32,
            ),
            square,
        )
    return square


def level_back(lefts, parts, rest):
    rows = jnp.concatenate([two_rows(left) for left in lefts], axis=0)
    high, low = split_low(jnp.concatenate(parts, axis=0))
    tall = dot_nt(rows, high)
    short = dot_nt(jnp.concatenate([split_low(left)[0] for left in lefts], axis=0), low)
    total = 0.0
    for index, factor in enumerate(rest):
        span = slice(index * TILE, (index + 1) * TILE)
        one = tall[2 * index * BLOCK : 2 * (index + 1) * BLOCK, span]
        total = total + factor * (one[:BLOCK] + one[BLOCK:] + short[index * BLOCK : (index + 1) * BLOCK, span])
    return total


def gate_terms(logits, valid, place):
    log_sig = jnp.minimum(logits, 0.0) - jnp.log1p(jnp.exp(-jnp.abs(logits)))
    logdecay = valid * log_sig * 0.125
    decay = jnp.exp(logdecay)
    series = -logdecay * (1.0 + logdecay * (0.5 + logdecay * (1.0 / 6.0 + logdecay * (1.0 / 24.0))))
    writes = valid * jnp.where(logdecay > -0.03, series, 1.0 - decay)
    low = jnp.bitwise_and(place, LAGS - 1)
    inside = jnp.where(low == 0, 0.0, decay)
    before, rest, step = logdecay, logdecay, 1
    while step < LAGS:
        before = before + jnp.where(low >= step, pltpu.roll(before, step, 1), 0.0)
        rest = rest + jnp.where(low < LAGS - step, pltpu.roll(rest, TILE - step, 1), 0.0)
        step *= 2
    rest = rest - logdecay
    scans = []
    while step < BLOCK:
        scans.append((jnp.exp(before), jnp.exp(rest)))
        total, upper = before + rest, jnp.bitwise_and(place, step) != 0
        before = before + jnp.where(upper, pltpu.roll(total, step, 1), 0.0)
        rest = rest + jnp.where(upper, 0.0, pltpu.roll(total, TILE - step, 1))
        step *= 2
    return decay, writes, inside, before, rest, scans


def stacked(values, lanes):
    return jnp.concatenate(
        [jnp.where(lanes < BLOCK, values, 0.0), jnp.where(lanes < BLOCK, 0.0, values)], axis=0
    )


def own_block(square, lanes):
    return jnp.where(lanes < BLOCK, square[:BLOCK], square[BLOCK:])


def forward_kernel(
    length_ref, qkv_ref, logit_ref, bias_ref,
    mixed_ref, state_ref, prob_ref, score_ref, mix_ref,
    gate_ref, carry_ref, band_ref, mix_band_ref, product_ref,
):
    width = mixed_ref.shape[1]
    tiles = mixed_ref.shape[0] // TILE
    scale = width ** -0.5
    lanes, place = lane_place()
    bias = bias_ref[...]

    def valid_of(tile):
        return (lanes + tile * TILE < length_ref[0]).astype(jnp.float32)

    def rows_of(tile):
        return pl.ds(pl.multiple_of(tile * TILE, TILE), TILE)

    def gather_writes(tile, none):
        logits = logit_ref[tile] + bias
        _, writes, inside, before, after, scans = gate_terms(logits, valid_of(tile), place)
        for index, (faded, rest) in enumerate(scans):
            gate_ref[tile, 4 + 2 * index] = faded
            gate_ref[tile, 5 + 2 * index] = rest * writes
        gate_ref[tile, 0] = writes
        gate_ref[tile, 1] = inside
        gate_ref[tile, 2] = jnp.exp(before)
        gate_ref[tile, 3] = jnp.exp(before + after)
        high, low = split_low(stacked(jnp.exp(after) * writes, lanes))
        rows = qkv_ref[rows_of(tile), width:]
        added = dot_nn(high, rows) + dot_nn(low, rows)
        state_ref[tile] = added
        return none

    lax.fori_loop(0, tiles, gather_writes, 0)

    carry_ref[...] = jnp.zeros_like(carry_ref)

    def run_states(tile, none):
        for part in range(2):
            span = pl.ds(part * BLOCK, BLOCK)
            fade = gate_ref[tile, 3, :, part * BLOCK : part * BLOCK + 1]
            carried = carry_ref[...]
            added = state_ref[tile, span, :]
            state_ref[tile, span, :] = carried
            carry_ref[...] = fade * carried + added
        return none

    lax.fori_loop(0, tiles, run_states, 0)

    masks = level_masks()

    def mix_pair(pair, none):
        both = [(slot, PAIR * pair + slot) for slot in range(PAIR)]
        queries, scores, probs, squares = {}, {}, {}, {}

        def faded_of(tile):
            return [gate_ref[tile, 4], gate_ref[tile, 6]]

        def near_of(tile):
            return [gate_ref[tile, 5], gate_ref[tile, 7]]

        for slot, tile in both:
            queries[slot] = qkv_ref[rows_of(tile), :width]
            squares[slot] = dot_nt(qkv_ref[rows_of(tile), width : 2 * width], queries[slot]) * scale
        for slot, tile in both:
            fill_products(product_ref, slot, gate_ref[tile, 0], gate_ref[tile, 1])
        for slot, tile in both:
            high, low = split_low(state_ref[tile, :, :width])
            carried = own_block(dot_nt(high, queries[slot]) + dot_nt(low, queries[slot]), lanes)
            scores[slot] = gate_ref[tile, 2] * carried * scale
        for slot, tile in both:
            take_band(squares[slot], band_ref, slot)
            scores[slot] = scores[slot] + level_total(
                near_of(tile), level_parts(squares[slot], masks), faded_of(tile)
            )
        for slot, tile in both:
            scores[slot] = lag_total(product_ref, slot, band_ref, scores[slot])
        for slot, tile in both:
            top = jnp.max(scores[slot], axis=0, keepdims=True)
            raised = jnp.exp(scores[slot] - top)
            probs[slot] = raised / jnp.sum(raised, axis=0, keepdims=True)
            score_ref[tile] = scores[slot]
            prob_ref[tile] = probs[slot]
        for slot, tile in both:
            lag_mix(product_ref, slot, mix_band_ref, probs[slot])
        for slot, tile in both:
            mixing = put_band(jnp.zeros((TILE, TILE), jnp.float32), mix_band_ref, slot)
            mixing = level_mix(mixing, near_of(tile), [probs[slot] * one for one in faded_of(tile)], masks)
            mixing = mixing.astype(jnp.bfloat16)
            mix_ref[tile] = mixing
            reach = stacked(probs[slot] * gate_ref[tile, 2], lanes).T.astype(jnp.bfloat16)
            result = dot_nn(mixing.T, qkv_ref[rows_of(tile), 2 * width :]) + dot_nn(
                reach, state_ref[tile, :, width:].astype(jnp.bfloat16)
            )
            rows = lax.broadcasted_iota(jnp.int32, (TILE, 1), 0) + tile * TILE
            mixed_ref[rows_of(tile), :] = jnp.where(rows < length_ref[0], result, 0.0).astype(jnp.bfloat16)
        return none

    lax.fori_loop(0, tiles // PAIR, mix_pair, 0)


def backward_kernel(
    length_ref, qkv_ref, logit_ref, bias_ref, back_ref, state_ref, prob_ref, score_ref, mix_ref,
    d_qkv_ref, d_bias_ref,
    adjoint_ref, gain_ref, key_band_ref, value_band_ref, band_ref, carry_ref, end_ref, cross_ref, product_ref,
):
    width = back_ref.shape[1]
    tiles = back_ref.shape[0] // TILE
    scale = width ** -0.5
    lanes, place = lane_place()
    bias = bias_ref[...]

    def valid_of(tile):
        return (lanes + tile * TILE < length_ref[0]).astype(jnp.float32)

    def rows_of(tile):
        return pl.ds(pl.multiple_of(tile * TILE, TILE), TILE)

    def back_of(tile):
        rows = lax.broadcasted_iota(jnp.int32, (TILE, 1), 0) + tile * TILE
        return jnp.where(rows < length_ref[0], back_ref[rows_of(tile), :], jnp.zeros((), back_ref.dtype))

    masks = level_masks()

    def slopes(pair, none):
        both = [(slot, PAIR * pair + slot) for slot in range(PAIR)]
        fades, powers, queries, keys, backs, gains, d_scores, faded, rests, near = ({} for _ in range(10))
        key_squares, value_squares = {}, {}
        for slot, tile in both:
            queries[slot] = qkv_ref[rows_of(tile), :width]
            keys[slot] = qkv_ref[rows_of(tile), width : 2 * width]
            backs[slot] = back_of(tile)
            key_squares[slot] = dot_nt(keys[slot], queries[slot]) * scale
            value_squares[slot] = dot_nt(qkv_ref[rows_of(tile), 2 * width :], backs[slot])
        for slot, tile in both:
            decay, writes, inside, before, after, scans = gate_terms(logit_ref[tile] + bias, valid_of(tile), place)
            faded[slot], rests[slot] = [one for one, _ in scans], [one for _, one in scans]
            near[slot] = [one * writes for one in rests[slot]]
            fades[slot] = jnp.exp(before)
            gain_ref[tile, 2] = decay
            gain_ref[tile, 3] = writes
            gain_ref[tile, 4] = jnp.exp(after)
            gain_ref[tile, 5] = jnp.exp(before + after)
            powers[slot] = fill_products(product_ref, slot, writes, inside)
        for slot, tile in both:
            high, low = split_low(state_ref[tile, :, width:])
            carried = own_block(dot_nt(high, backs[slot]) + dot_nt(low, backs[slot]), lanes)
            gains[slot] = fades[slot] * carried
        for slot, tile in both:
            take_band(key_squares[slot], key_band_ref, slot)
            take_band(value_squares[slot], value_band_ref, slot)
            gains[slot] = gains[slot] + level_total(
                near[slot], level_parts(value_squares[slot], masks), faded[slot]
            )
        for slot, tile in both:
            gains[slot] = lag_total(product_ref, slot, value_band_ref, gains[slot])
        for slot, tile in both:
            probs = prob_ref[tile]
            d_scores[slot] = probs * (gains[slot] - jnp.sum(probs * gains[slot], axis=0, keepdims=True))
            gain_ref[tile, 1] = d_scores[slot] * score_ref[tile] + probs * gains[slot]
        for slot, tile in both:
            lag_mix(product_ref, slot, band_ref, d_scores[slot])
        for slot, tile in both:
            probs = prob_ref[tile]

            def term_of(lag, slot=slot, probs=probs):
                row = slice(lag, lag + 1)
                return d_scores[slot] * key_band_ref[slot, row, :] + probs * value_band_ref[slot, row, :]

            lefts = [jnp.concatenate([d_scores[slot] * one, probs * one], axis=1) for one in faded[slot]]
            parts = [
                jnp.concatenate(
                    [jnp.where(mask, key_squares[slot], 0.0), jnp.where(mask, value_squares[slot], 0.0)], axis=1
                )
                for mask in masks
            ]
            gain_ref[tile, 0] = lag_back(powers[slot], term_of, 0, LAGS) + level_back(lefts, parts, rests[slot])
        for slot, tile in both:
            mixing = put_band(jnp.zeros((TILE, TILE), jnp.float32), band_ref, slot)
            mixing = level_mix(mixing, near[slot], [d_scores[slot] * one for one in faded[slot]], masks)
            mixing = (mixing * scale).astype(jnp.bfloat16)
            reach = stacked(d_scores[slot] * fades[slot] * scale, lanes)
            held = stacked(prob_ref[tile] * fades[slot], lanes).astype(jnp.bfloat16)
            d_qkv_ref[rows_of(tile), :width] = (
                dot_nn(mixing.T, keys[slot])
                + dot_nn(reach.T.astype(jnp.bfloat16), state_ref[tile, :, :width].astype(jnp.bfloat16))
            ).astype(jnp.bfloat16)
            adjoint_ref[tile, :, :width] = dot_nn(reach.astype(jnp.bfloat16), queries[slot])
            adjoint_ref[tile, :, width:] = dot_nn(held, backs[slot])
            d_qkv_ref[rows_of(tile), width : 2 * width] = dot_nn(mixing, queries[slot]).astype(jnp.bfloat16)
            d_qkv_ref[rows_of(tile), 2 * width : 3 * width] = dot_nn(mix_ref[tile], backs[slot]).astype(jnp.bfloat16)
        return none

    lax.fori_loop(0, tiles // PAIR, slopes, 0)

    carry_ref[...] = jnp.zeros_like(carry_ref)
    end_ref[...] = jnp.zeros_like(end_ref)

    def run_adjoints(count, none):
        tile = tiles - 1 - count
        for part in (1, 0):
            span = pl.ds(part * BLOCK, BLOCK)
            fade = gain_ref[tile, 5, :, part * BLOCK : part * BLOCK + 1]
            carried = carry_ref[...]
            added = adjoint_ref[tile, span, :]
            adjoint_ref[tile, span, :] = carried
            cross_ref[tile, span, :] = jnp.broadcast_to(
                jnp.sum(carried * end_ref[...], axis=1, keepdims=True), (BLOCK, TILE)
            )
            end_ref[...] = state_ref[tile, span, :]
            carry_ref[...] = fade * carried + added
        return none

    lax.fori_loop(0, tiles, run_adjoints, 0)

    d_bias_ref[...] = jnp.zeros_like(d_bias_ref)

    def finish(tile, none):
        key_rows = qkv_ref[rows_of(tile), width : 2 * width]
        value_rows = qkv_ref[rows_of(tile), 2 * width :]
        adjoint = adjoint_ref[tile]
        high, low = split_low(adjoint)
        rows = qkv_ref[rows_of(tile), width:]
        carried = own_block(dot_nt(high, rows) + dot_nt(low, rows), lanes)
        decay, writes, rest = gain_ref[tile, 2], gain_ref[tile, 3], gain_ref[tile, 4]
        d_writes = gain_ref[tile, 0] + rest * carried
        tail = stacked(rest * writes, lanes).T.astype(jnp.bfloat16)
        d_qkv_ref[rows_of(tile), width : 3 * width] = (
            d_qkv_ref[rows_of(tile), width : 3 * width].astype(jnp.float32) + dot_nn(tail, high)
        ).astype(jnp.bfloat16)
        cross = own_block(cross_ref[tile], lanes)
        d_decay = suffix_sum(gain_ref[tile, 1] - writes * d_writes, place) + cross - decay * d_writes
        logits = logit_ref[tile] + bias
        d_logit = valid_of(tile) * d_decay * jax.nn.sigmoid(-logits) * 0.125
        d_bias_ref[...] += jnp.broadcast_to(jnp.sum(d_logit, axis=1, keepdims=True), (BLOCK, TILE))
        d_qkv_ref[rows_of(tile), 3 * width :] = jnp.concatenate([d_logit, jnp.zeros_like(d_logit)], axis=0).T.astype(jnp.bfloat16)
        return none

    lax.fori_loop(0, tiles, finish, 0)


def mixer_forward(length, qkv, logits, bias):
    rows, width = qkv.shape[0], qkv.shape[1] // 3
    tiles = rows // TILE
    f32 = jnp.float32
    return pl.pallas_call(
        forward_kernel,
        out_shape=(
            jax.ShapeDtypeStruct((rows, width), jnp.bfloat16),
            jax.ShapeDtypeStruct((tiles, TILE, 2 * width), f32),
            jax.ShapeDtypeStruct((tiles, BLOCK, TILE), f32),
            jax.ShapeDtypeStruct((tiles, BLOCK, TILE), f32),
            jax.ShapeDtypeStruct((tiles, TILE, TILE), jnp.bfloat16),
        ),
        in_specs=[pl.BlockSpec(memory_space=pltpu.SMEM)] + [pl.BlockSpec(memory_space=pltpu.VMEM)] * 3,
        out_specs=[pl.BlockSpec(memory_space=pltpu.VMEM)] * 5,
        scratch_shapes=[
            pltpu.VMEM((tiles, 8, BLOCK, TILE), f32),
            pltpu.VMEM((BLOCK, 2 * width), f32),
            pltpu.VMEM((PAIR, LAGS, TILE), f32),
            pltpu.VMEM((PAIR, LAGS, TILE), f32),
            pltpu.VMEM((PAIR, LAGS, BLOCK, TILE), f32),
        ],
        compiler_params=pltpu.CompilerParams(vmem_limit_bytes=22 * MEBI),
        name="mixer_forward",
    )(length, qkv, logits, bias)


def mixer_backward(length, qkv, logits, bias, back, saved):
    rows, width = qkv.shape[0], qkv.shape[1] // 3
    tiles = rows // TILE
    f32 = jnp.float32
    return pl.pallas_call(
        backward_kernel,
        out_shape=(
            jax.ShapeDtypeStruct((rows, 3 * width + 2 * BLOCK), jnp.bfloat16),
            jax.ShapeDtypeStruct((BLOCK, TILE), f32),
        ),
        in_specs=[pl.BlockSpec(memory_space=pltpu.SMEM)] + [pl.BlockSpec(memory_space=pltpu.VMEM)] * 8,
        out_specs=[pl.BlockSpec(memory_space=pltpu.VMEM)] * 2,
        scratch_shapes=[
            pltpu.VMEM((tiles, TILE, 2 * width), f32),
            pltpu.VMEM((tiles, 6, BLOCK, TILE), f32),
            pltpu.VMEM((PAIR, LAGS, TILE), f32),
            pltpu.VMEM((PAIR, LAGS, TILE), f32),
            pltpu.VMEM((PAIR, LAGS, TILE), f32),
            pltpu.VMEM((BLOCK, 2 * width), f32),
            pltpu.VMEM((BLOCK, 2 * width), f32),
            pltpu.VMEM((tiles, TILE, TILE), f32),
            pltpu.VMEM((PAIR, LAGS, BLOCK, TILE), f32),
        ],
        compiler_params=pltpu.CompilerParams(vmem_limit_bytes=32 * MEBI),
        name="mixer_backward",
    )(length, qkv, logits, bias, back, *saved)


def to_low(values):
    return values.astype(jnp.bfloat16)


def to_wide(values):
    return values.astype(jnp.float32)


def dot_tn(left, right):
    return lax.dot_general(left, right, (((0,), (0,)), ((), ())), preferred_element_type=jnp.float32)


def tie(values, *earlier):
    return lax.optimization_barrier((values,) + earlier)[0]


def ring_order(size):
    return list(range(0, size, 2)) + list(range(size - 1 - size % 2, 0, -2))


def hop_pairs(order, hop):
    size = len(order)
    return [(order[i], order[(i + hop) % size]) for i in range(size)]


def ring_gather(shard, order):
    size = len(order)
    up, down = hop_pairs(order, 1), hop_pairs(order, -1)
    pieces = [shard] + [None] * (size - 1)
    from_low, from_high = shard, shard
    for step in range(1, (size + 1) // 2):
        from_low = lax.ppermute(from_low, DP, up)
        from_high = lax.ppermute(from_high, DP, down)
        pieces[size - step], pieces[step] = from_low, from_high
    if size % 2 == 0:
        half = shard.shape[0] // 2
        first = lax.ppermute(from_low[:half], DP, up)
        second = lax.ppermute(from_high[half:], DP, down)
        pieces[size // 2] = (first, second)
    return pieces


def ring_scatter(piece_of, order):
    size = len(order)
    up, down = hop_pairs(order, 1), hop_pairs(order, -1)
    half_count = (size - 1) // 2
    up_sum, down_sum = None, None
    if size % 2 == 0:
        farthest = piece_of(size // 2)
        half = farthest.shape[0] // 2
        up_half = lax.ppermute(to_low(farthest[:half]), DP, up)
        down_half = lax.ppermute(to_low(farthest[half:]), DP, down)
        up_sum = jnp.concatenate([to_wide(up_half), jnp.zeros(up_half.shape, jnp.float32)], axis=0)
        down_sum = jnp.concatenate([jnp.zeros(down_half.shape, jnp.float32), to_wide(down_half)], axis=0)
    for step in range(half_count, 0, -1):
        up_piece, down_piece = to_wide(piece_of(step)), to_wide(piece_of(size - step))
        if up_sum is not None:
            up_piece, down_piece = up_piece + up_sum, down_piece + down_sum
        up_sum = to_wide(lax.ppermute(to_low(up_piece), DP, up))
        down_sum = to_wide(lax.ppermute(to_low(down_piece), DP, down))
    return piece_of(0), to_low(up_sum), to_low(down_sum)


def total_sum(values, axis):
    count = lax.axis_size(axis)
    step = 1
    while step < count:
        values = values + lax.ppermute(values, axis, [(i, i ^ step) for i in range(count)])
        step *= 2
    return values


def move_kernel(places_ref, source_ref, target_ref):
    target_ref[...] = source_ref[...]


def move_columns(matrix, places, inverse):
    size = places.shape[0]
    rows, columns = matrix.shape
    width = columns // size
    if width % 128:
        split = matrix.reshape(rows, size, width)
        if inverse:
            places = jnp.argsort(places)
        return jnp.take(split, places, axis=1).reshape(rows, columns)

    def plain(step, places_ref):
        return (0, step)

    def placed(step, places_ref):
        return (0, places_ref[step])

    return pl.pallas_call(
        move_kernel,
        out_shape=jax.ShapeDtypeStruct(matrix.shape, matrix.dtype),
        grid_spec=pltpu.PrefetchScalarGridSpec(
            num_scalar_prefetch=1,
            grid=(size,),
            in_specs=[pl.BlockSpec((rows, width), plain if inverse else placed)],
            out_specs=pl.BlockSpec((rows, width), placed if inverse else plain),
        ),
        compiler_params=pltpu.CompilerParams(vmem_limit_bytes=8 * MEBI),
        cost_estimate=pl.CostEstimate(flops=0, bytes_accessed=2 * matrix.size * matrix.dtype.itemsize, transcendentals=0),
    )(places, matrix)


ROWS = 128
WIDE = 256
MEBI = 1024 * 1024


def vmem_call(body, out_shape, operands, limit, scratch=(), scalars=1, anywhere=0, flops=0, moved=0):
    spaces = (
        [pl.BlockSpec(memory_space=pltpu.SMEM)] * scalars
        + [pl.BlockSpec(memory_space=pltpu.VMEM)] * (len(operands) - scalars - anywhere)
        + [pl.BlockSpec(memory_space=pl.ANY)] * anywhere
    )
    return pl.pallas_call(
        body,
        out_shape=out_shape,
        in_specs=spaces,
        out_specs=[pl.BlockSpec(memory_space=pltpu.VMEM)] * len(out_shape),
        scratch_shapes=list(scratch),
        compiler_params=pltpu.CompilerParams(vmem_limit_bytes=limit * MEBI),
        cost_estimate=pl.CostEstimate(flops=flops, bytes_accessed=moved, transcendentals=0),
    )(*operands)


def load_blocks(sources, target_ref, sems, blocks, low=0):
    groups = []
    for block in blocks:
        copies = []
        for first, span in block:
            start = 0
            for source in sources:
                rows = source.shape[0]
                index = sum(map(len, groups)) + len(copies)
                copies.append(
                    pltpu.make_async_copy(
                        source.at[:, pl.ds(low + first, span)],
                        target_ref.at[pl.ds(start, rows), pl.ds(first, span)],
                        sems.at[index],
                    )
                )
                start += rows
        groups.append(copies)
    for copies in groups:
        for copy in copies:
            copy.start()
    return groups


def finish(copies):
    for copy in copies:
        copy.wait()


def flat_pieces(pieces):
    flat = []
    for piece in pieces:
        flat += list(piece) if isinstance(piece, tuple) else [piece]
    return flat


def give_halves(block_ref, parity, parts, columns, kept_refs, sent_refs):
    rows = block_ref.shape[0] // parts // 2
    for part in range(parts):
        kept_refs[part][:, columns] = block_ref[pl.ds((2 * part + parity) * rows, rows), :].astype(jnp.bfloat16)
        sent_refs[part][:, columns] = block_ref[pl.ds((2 * part + 1 - parity) * rows, rows), :].astype(jnp.bfloat16)


def project_call(left, pieces, parity, parts, low, keep):
    rows, depth = left.shape
    flat = flat_pieces(pieces)
    count = len(flat)
    total = sum(piece.shape[0] for piece in flat)

    def body(parity_ref, left_ref, *refs):
        sources, outs = refs[:count], refs[count:]
        block_ref, sems = outs[-2:]
        weight_ref = outs[-3]
        finish(load_blocks(sources, weight_ref, sems, [[(0, depth)]], low)[0])
        parity = parity_ref[0]

        def one(step, none):
            columns = pl.ds(pl.multiple_of(step * WIDE, WIDE), WIDE)
            block_ref[...] = dot_nt(left_ref[...], weight_ref[columns, :])
            give_halves(block_ref, parity, parts, columns, outs[:parts], outs[parts : 2 * parts])
            return none

        lax.fori_loop(0, total // WIDE, one, 0)

    half = jax.ShapeDtypeStruct((rows // parts // 2, total), jnp.bfloat16)
    weight = (total, depth)
    outs = vmem_call(
        body,
        [half] * (2 * parts) + ([jax.ShapeDtypeStruct(weight, jnp.bfloat16)] if keep else []),
        (parity, left, *flat), 12 if keep else 22,
        scratch=([] if keep else [pltpu.VMEM(weight, jnp.bfloat16)])
        + [
            pltpu.VMEM((rows, WIDE), jnp.float32),
            pltpu.SemaphoreType.DMA((count,)),
        ],
        anywhere=count, flops=2 * rows * depth * total, moved=2 * (rows * depth + depth * total + rows * total),
    )
    return outs[:parts], outs[parts : 2 * parts], outs[2 * parts :]


def query_call(rows_low, factor, pieces, slots, columns_all):
    rows, depth = rows_low.shape
    flat = flat_pieces(pieces)
    count = len(flat)
    wide = columns_all - 2 * slots
    blocks = [[(wide, 2 * slots)]] + [[(start, 2 * WIDE)] for start in range(0, wide, 2 * WIDE)]

    def body(rows_ref, factor_ref, *refs):
        sources = refs[:count]
        qkv_ref, logit_ref, normed_ref, gain_ref, weight_ref, sems = refs[count:]
        groups = load_blocks(sources, weight_ref, sems, blocks)
        finish(groups[0])
        gain_ref[...] = weight_ref[:, wide:].astype(jnp.float32).T[slots : slots + 8]

        def norm_rows(step, none):
            span = pl.ds(pl.multiple_of(step * TILE, TILE), TILE)
            values = rows_ref[span, :].astype(jnp.float32)
            normed_ref[span, :] = (values * factor_ref[span, :] * gain_ref[0:1, :]).astype(jnp.bfloat16)
            return none

        lax.fori_loop(0, rows // TILE, norm_rows, 0)
        logits = dot_nn(normed_ref[...], weight_ref[:, wide:])
        for tile in range(rows // TILE):
            logit_ref[tile] = logits[tile * TILE : (tile + 1) * TILE, :].T[:slots]
        for copies in groups[1:]:
            finish(copies)

        def one(step, none):
            columns = pl.ds(pl.multiple_of(step * WIDE, WIDE), WIDE)
            qkv_ref[:, columns] = dot_nn(normed_ref[...], weight_ref[:, columns]).astype(jnp.bfloat16)
            return none

        lax.fori_loop(0, wide // WIDE, one, 0)

    return vmem_call(
        body,
        [
            jax.ShapeDtypeStruct((rows, wide), jnp.bfloat16),
            jax.ShapeDtypeStruct((rows // TILE, slots, TILE), jnp.float32),
            jax.ShapeDtypeStruct((rows, depth), jnp.bfloat16),
            jax.ShapeDtypeStruct((8, depth), jnp.float32),
        ],
        (rows_low, factor, *flat), 28,
        scratch=[pltpu.VMEM((depth, columns_all), jnp.bfloat16), pltpu.SemaphoreType.DMA((count * len(blocks),))],
        scalars=0, anywhere=count,
        flops=2 * rows * depth * columns_all, moved=2 * (rows + columns_all) * depth + 2 * rows * columns_all,
    )


def act_columns(start, span, hidden, normed_ref, back_ref, weight_ref, hidden_ref, pair_ref):
    def columns(base):
        return pl.ds(start + base, span)

    gate_act = dot_nn(normed_ref[...], weight_ref[:, columns(0)])
    up_act = dot_nn(normed_ref[...], weight_ref[:, columns(hidden)])
    d_hidden = dot_nn(back_ref[...], weight_ref[:, columns(2 * hidden)])
    sigma = 1.0 / (1.0 + jnp.exp(-gate_act))
    gated = gate_act * sigma
    hidden_ref[:, columns(0)] = (gated * up_act).astype(jnp.bfloat16)
    pair_ref[:, columns(hidden)] = (d_hidden * gated).astype(jnp.bfloat16)
    pair_ref[:, columns(0)] = (d_hidden * up_act * (sigma * (1.0 + gate_act * (1.0 - sigma)))).astype(jnp.bfloat16)


def feed_call(normed, back, pieces, parity, earlier, parts):
    rows, depth = normed.shape
    flat = flat_pieces(pieces)
    count = len(flat)
    hidden = flat[0].shape[1] // 3
    given = 0 if earlier is None else 2
    blocks = [
        [(part * hidden, WIDE) for part in range(3)],
        [(part * hidden + WIDE, hidden - WIDE) for part in range(3)],
    ]

    def body(parity_ref, *refs):
        sources = refs[: count + 2 + given]
        outs = refs[count + 2 + given :]
        hidden_ref, pair_ref = outs[:2]
        total_refs = outs[2 : 4 if earlier is None else 4 + 2 * parts]
        outs = outs[2 + len(total_refs) :]
        weight_ref, normed_ref, back_ref, block_ref = outs[:4]
        sems = outs[-1]
        held = [
            pltpu.make_async_copy(sources[count], normed_ref, sems.at[6 * count]),
            pltpu.make_async_copy(sources[count + 1], back_ref, sems.at[6 * count + 1]),
        ]
        held[0].start()
        held[1].start()
        groups = load_blocks(sources[:count], weight_ref, sems, blocks)
        if given:
            sum_ref = outs[4]
            held += [
                pltpu.make_async_copy(sources[count + 2 + i], sum_ref.at[i], sems.at[6 * count + 2 + i]) for i in range(2)
            ]
            held[2].start()
            held[3].start()

        def act(start, span):
            act_columns(start, span, hidden, normed_ref, back_ref, weight_ref, hidden_ref, pair_ref)

        finish(held[:2])
        finish(groups[0])
        act(0, WIDE)
        for copies in groups[1:]:
            finish(copies)

        def act_wide(step, none):
            act(pl.multiple_of(step * WIDE, WIDE), WIDE)
            return none

        lax.fori_loop(1, hidden // WIDE, act_wide, 0)
        if hidden % WIDE:
            act(hidden // WIDE * WIDE, hidden % WIDE)
        finish(held[2:])
        parity = parity_ref[0]

        def one(step, none):
            columns = pl.ds(pl.multiple_of(step * WIDE, WIDE), WIDE)
            d_block = dot_nt(pair_ref[...], weight_ref[columns, : 2 * hidden])
            y_block = dot_nt(hidden_ref[...], weight_ref[columns, 2 * hidden :])
            if not given:
                total_refs[0][:, columns] = d_block.astype(jnp.bfloat16)
                total_refs[1][:, columns] = y_block.astype(jnp.bfloat16)
            else:
                block_ref[...] = d_block + sum_ref[0, :, columns].astype(jnp.float32)
                give_halves(block_ref, parity, parts, columns, total_refs[:parts], total_refs[parts : 2 * parts])
                block_ref[...] = y_block + sum_ref[1, :, columns].astype(jnp.float32)
                give_halves(block_ref, parity, 1, columns, total_refs[2 * parts :][:1], total_refs[2 * parts + 1 :])
            return none

        lax.fori_loop(0, depth // WIDE, one, 0)

    low = jnp.bfloat16
    outs = [jax.ShapeDtypeStruct((rows, hidden), low), jax.ShapeDtypeStruct((rows, 2 * hidden), low)]
    if earlier is None:
        outs += [jax.ShapeDtypeStruct((rows, depth), low)] * 2
    else:
        outs += [jax.ShapeDtypeStruct((rows // parts // 2, depth), low)] * (2 * parts)
        outs += [jax.ShapeDtypeStruct((rows // 2, depth), low)] * 2
    scratch = [
        pltpu.VMEM((depth, 3 * hidden), low),
        pltpu.VMEM((rows, depth), low),
        pltpu.VMEM((rows, depth), low),
        pltpu.VMEM((rows, WIDE), jnp.float32),
    ]
    if given:
        scratch.append(pltpu.VMEM((2, rows, depth), low))
    scratch.append(pltpu.SemaphoreType.DMA((6 * count + 2 + given,)))
    return vmem_call(
        body, outs, (parity, *flat, normed, back, *(earlier or ())), 48,
        scratch=scratch, anywhere=count + 2 + given,
        flops=2 * rows * depth * hidden * 6, moved=2 * (3 * rows * depth + 3 * depth * hidden + 3 * rows * hidden),
    )


def act_call(normed, back, pieces):
    rows, depth = normed.shape
    flat = flat_pieces(pieces)
    count = len(flat)
    hidden = flat[0].shape[1] // 3
    blocks = [
        [(part * hidden, WIDE) for part in range(3)],
        [(part * hidden + WIDE, hidden - WIDE) for part in range(3)],
    ]

    def body(*refs):
        sources, (hidden_ref, pair_ref, weight_ref), (normed_ref, back_ref, sems) = refs[:-6], refs[-6:-3], refs[-3:]
        held = [
            pltpu.make_async_copy(sources[count], normed_ref, sems.at[6 * count]),
            pltpu.make_async_copy(sources[count + 1], back_ref, sems.at[6 * count + 1]),
        ]
        held[0].start()
        held[1].start()
        groups = load_blocks(sources[:count], weight_ref, sems, blocks)

        def act(start, span):
            act_columns(start, span, hidden, normed_ref, back_ref, weight_ref, hidden_ref, pair_ref)

        finish(held + groups[0])
        act(0, WIDE)
        finish(groups[1])

        def act_wide(step, none):
            act(pl.multiple_of(step * WIDE, WIDE), WIDE)
            return none

        lax.fori_loop(1, hidden // WIDE, act_wide, 0)
        if hidden % WIDE:
            act(hidden // WIDE * WIDE, hidden % WIDE)

    low = jnp.bfloat16
    return vmem_call(
        body,
        [
            jax.ShapeDtypeStruct((rows, hidden), low),
            jax.ShapeDtypeStruct((rows, 2 * hidden), low),
            jax.ShapeDtypeStruct((depth, 3 * hidden), low),
        ],
        (*flat, normed, back), 36,
        scratch=[
            pltpu.VMEM((rows, depth), low),
            pltpu.VMEM((rows, depth), low),
            pltpu.SemaphoreType.DMA((6 * count + 2,)),
        ],
        scalars=0, anywhere=count + 2,
        flops=2 * rows * depth * hidden * 3, moved=2 * (2 * rows * depth + 6 * depth * hidden + 3 * rows * hidden),
    )


def back_call(hidden_rows, pair_rows, weight, parity, earlier, parts):
    rows, hidden = hidden_rows.shape
    depth = weight.shape[0]

    def body(parity_ref, hidden_ref, pair_ref, weight_ref, d_ref, y_ref, *refs):
        outs, block_ref = refs[:-1], refs[-1]
        parity, whole = parity_ref[0], slice(0, WIDE)
        block_ref[...] = dot_nt(pair_ref[...], weight_ref[:, : 2 * hidden]) + d_ref[...].astype(jnp.float32)
        give_halves(block_ref, parity, parts, whole, outs[:parts], outs[parts : 2 * parts])
        block_ref[...] = dot_nt(hidden_ref[...], weight_ref[:, 2 * hidden :]) + y_ref[...].astype(jnp.float32)
        give_halves(block_ref, parity, 1, whole, outs[2 * parts : 2 * parts + 1], outs[2 * parts + 1 :])

    def still(step, parity_ref):
        return (0, 0)

    def across(step, parity_ref):
        return (0, step)

    def down(step, parity_ref):
        return (step, 0)

    heights = [rows // parts // 2] * (2 * parts) + [rows // 2] * 2
    return pl.pallas_call(
        body,
        out_shape=[jax.ShapeDtypeStruct((height, depth), jnp.bfloat16) for height in heights],
        grid_spec=pltpu.PrefetchScalarGridSpec(
            num_scalar_prefetch=1,
            grid=(depth // WIDE,),
            in_specs=[
                pl.BlockSpec((rows, hidden), still),
                pl.BlockSpec((rows, 2 * hidden), still),
                pl.BlockSpec((WIDE, 3 * hidden), down),
                pl.BlockSpec((rows, WIDE), across),
                pl.BlockSpec((rows, WIDE), across),
            ],
            out_specs=[pl.BlockSpec((height, WIDE), across) for height in heights],
            scratch_shapes=[pltpu.VMEM((rows, WIDE), jnp.float32)],
        ),
        compiler_params=pltpu.CompilerParams(vmem_limit_bytes=26 * MEBI),
        cost_estimate=pl.CostEstimate(
            flops=2 * rows * depth * hidden * 3, bytes_accessed=2 * (4 * rows * depth + 3 * depth * hidden), transcendentals=0
        ),
    )(parity, hidden_rows, pair_rows, weight, *earlier)


def sum_specs(parts, steps, rows, depth):
    share = steps // parts // 2

    def spec(index):
        return pl.BlockSpec((rows, depth), lambda step, scalars: (jnp.clip(step - index * share, 0, share - 1), 0))

    return [spec(index) for index in range(2 * parts)]


def place_row(parts, steps):
    share = steps // parts // 2

    def place(step, scalars):
        span = step // share
        part, other = span // 2, span % 2
        half = jnp.where(other == 0, scalars[0], 1 - scalars[0])
        return ((2 * part + half) * share + step % share, 0)

    return place


def pick_sum(step, share, refs):
    value = refs[0][...]
    for index, ref in enumerate(refs[1:]):
        value = jnp.where(step >= (index + 1) * share, ref[...], value)
    return value.astype(jnp.float32)


def row_call(body, scalars, parts, sums, whole, fixed, outs, narrow=(), limit=16):
    rows, depth = whole[0].shape
    steps = rows // ROWS
    place = place_row(parts, steps)
    block = pl.BlockSpec((ROWS, depth), place)
    ones = [pl.BlockSpec(array.shape, lambda step, scalars: (0, 0)) for array in fixed]
    moved = sum(a.size * a.dtype.itemsize for a in list(sums) + list(whole))
    moved += sum(rows * depth * jnp.dtype(kind).itemsize for kind in outs)
    return pl.pallas_call(
        body,
        out_shape=[jax.ShapeDtypeStruct((rows, depth), kind) for kind in outs]
        + [jax.ShapeDtypeStruct((rows, count), jnp.bfloat16) for count in narrow],
        grid_spec=pltpu.PrefetchScalarGridSpec(
            num_scalar_prefetch=1,
            grid=(steps,),
            in_specs=sum_specs(parts, steps, ROWS, depth) + [block] * len(whole) + ones,
            out_specs=[block] * len(outs) + [pl.BlockSpec((ROWS, count), place) for count in narrow],
        ),
        compiler_params=pltpu.CompilerParams(vmem_limit_bytes=limit * MEBI),
        cost_estimate=pl.CostEstimate(flops=10 * rows * depth, bytes_accessed=moved, transcendentals=0),
    )(scalars, *sums, *whole, *fixed)


def norm_factor(values):
    return lax.rsqrt(jnp.mean(values * values, axis=-1, keepdims=True) + epsilon)


def norm_call(scalars, sums, rows_in, gain):
    parts, steps = len(sums) // 2, rows_in.shape[0] // ROWS

    def body(scalar_ref, *refs):
        sum_refs = refs[: 2 * parts]
        rows_ref, gain_ref, resid_ref, normed_ref = refs[2 * parts :]
        total = pick_sum(pl.program_id(0), steps // parts // 2, sum_refs)
        resid = rows_ref[...].astype(jnp.float32) + total
        resid_ref[...] = resid.astype(jnp.bfloat16)
        normed_ref[...] = (resid * norm_factor(resid) * gain_ref[...]).astype(jnp.bfloat16)

    return row_call(body, scalars, parts, sums, [rows_in], [gain], [jnp.bfloat16, jnp.bfloat16])


def norm_back(total, values, gain):
    factor = norm_factor(values)
    hat = values * factor
    scaled = gain * total
    return factor * (scaled - hat * jnp.mean(scaled * hat, axis=-1, keepdims=True))


def norm_back_call(scalars, sums, resid, back, gain, full_out):
    parts, steps = len(sums) // 2, resid.shape[0] // ROWS

    def body(scalar_ref, *refs):
        sum_refs = refs[: 2 * parts]
        resid_ref, back_ref, gain_ref, out_ref, d_attn_ref, d_mixed_ref = refs[2 * parts :]
        total = pick_sum(pl.program_id(0), steps // parts // 2, sum_refs)
        slope = norm_back(total, resid_ref[...].astype(jnp.float32), gain_ref[...])
        d_attn = (back_ref[...].astype(jnp.float32) + slope).astype(jnp.bfloat16)
        d_attn_ref[...] = d_attn
        d_mixed_ref[...] = dot_nn(d_attn, out_ref[...]).astype(jnp.bfloat16)

    return row_call(body, scalars, parts, sums, [resid, back], [gain, full_out], [jnp.bfloat16], [full_out.shape[1]])


def store_placed(target_ref, values, scalar_ref, size):
    share = values.shape[1] // size
    if share % 128:
        target_ref[...] = values
        return
    for index in range(size):
        columns = pl.ds(pl.multiple_of(scalar_ref[1 + index] * share, 128), share)
        target_ref[:, columns] = values[:, index * share : (index + 1) * share]


def replaced(matrix, places):
    size = places.shape[0]
    share = matrix.shape[1] // size
    if share % 128 == 0:
        return matrix
    return jnp.take(matrix.reshape(-1, size, share), jnp.argsort(places), axis=1).reshape(matrix.shape)


def last_call(scalars, sums, d_resid, rows_in, gain, size):
    parts, steps = len(sums) // 2, rows_in.shape[0] // ROWS

    def body(scalar_ref, *refs):
        sum_refs = refs[: 2 * parts]
        d_resid_ref, rows_ref, gain_ref, out_ref = refs[2 * parts :]
        total = pick_sum(pl.program_id(0), steps // parts // 2, sum_refs)
        slope = norm_back(total, rows_ref[...].astype(jnp.float32), gain_ref[...])
        store_placed(out_ref, d_resid_ref[...].astype(jnp.float32) + slope, scalar_ref, size)

    (out,) = row_call(body, scalars, parts, sums, [d_resid, rows_in], [gain], [jnp.float32], limit=60)
    return replaced(out, scalars[1:])


def output_call(scalars, sums, resid, size):
    parts, steps = len(sums) // 2, resid.shape[0] // ROWS

    def body(scalar_ref, *refs):
        sum_refs = refs[: 2 * parts]
        resid_ref, out_ref = refs[2 * parts :]
        total = pick_sum(pl.program_id(0), steps // parts // 2, sum_refs)
        store_placed(out_ref, (resid_ref[...].astype(jnp.float32) + total).astype(jnp.bfloat16), scalar_ref, size)

    (out,) = row_call(body, scalars, parts, sums, [resid], [], [jnp.bfloat16])
    return replaced(out, scalars[1:])


def sum_refs_of(refs):
    total = refs[0][...].astype(jnp.float32)
    for ref in refs[1:]:
        total = total + ref[...].astype(jnp.float32)
    return total


def finish_feed(grads, w_gate, w_up, spans):
    share, count = w_gate.shape

    def body(*refs):
        grad_refs = refs[: len(grads)]
        gate_ref, up_ref, d_gate_ref, d_up_ref, d_down_ref, gain_ref = refs[len(grads) :]
        for index, (low, high) in enumerate(spans):
            span = high - low
            total = sum_refs_of(grad_refs[3 * index : 3 * index + 3])
            d_gate_ref[:, low:high] = total[:, :span]
            d_up_ref[:, low:high] = total[:, span : 2 * span]
            d_down_ref[low:high, :] = total[:, 2 * span :].T
        gain_ref[...] = jnp.sum(
            gate_ref[...].astype(jnp.float32) * d_gate_ref[...] + up_ref[...].astype(jnp.float32) * d_up_ref[...],
            axis=1, keepdims=True,
        )

    shapes = [(share, count), (share, count), (count, share), (share, 1)]
    return vmem_call(
        body, [jax.ShapeDtypeStruct(shape, jnp.float32) for shape in shapes],
        (*grads, w_gate, w_up), 24, scalars=0, moved=share * count * 36,
    )


def finish_mix(grads, mix_shard, width, slots):
    share = mix_shard.shape[0]
    used, start = 3 * width + slots, 3 * width + 2 * BLOCK

    def body(*refs):
        grad_refs = refs[: len(grads)]
        shard_ref, query_ref, key_ref, value_ref, slot_ref, out_ref, gain_ref = refs[len(grads) :]
        total = sum_refs_of(grad_refs)
        for index, ref in enumerate((query_ref, key_ref, value_ref)):
            ref[...] = total[:, index * width : (index + 1) * width]
        slot_ref[...] = total[:, 3 * width : used]
        out_ref[...] = total[:, start:].T
        gain_ref[...] = jnp.sum(shard_ref[:, :used].astype(jnp.float32) * total[:, :used], axis=1, keepdims=True)

    shapes = [(share, width)] * 3 + [(share, slots), (width, share), (share, 1)]
    return vmem_call(
        body, [jax.ShapeDtypeStruct(shape, jnp.float32) for shape in shapes],
        (*grads, mix_shard), 16, scalars=0, moved=share * start * 14,
    )


def exchange(kept, sent, held=()):
    heads = lax.axis_size(HEAD)
    near = [(i, i ^ 1) for i in range(heads)]
    far = [(i, i ^ 2) for i in range(heads)]
    sums, halves = [], []
    for own, given in zip(kept, sent):
        own = to_low(to_wide(own) + to_wide(lax.ppermute(given, HEAD, near)))
        halves.append(own)
        own = to_low(to_wide(own) + to_wide(tie(lax.ppermute(own, HEAD, far), *held)))
        sums += [own, lax.ppermute(own, HEAD, near)]
    return sums, halves


def layer(
    inputs,
    lengths,
    gain_attn,
    w_query,
    w_key,
    w_value,
    w_slot,
    gate_bias,
    w_out,
    gain_ffn,
    w_gate,
    w_up,
    w_down,
    cotangent,
):
    size = lax.axis_size(DP)
    order = ring_order(size)
    spots = [order.index(i) for i in range(size)]
    spot = jnp.array(spots, jnp.int32)[lax.axis_index(DP)]
    places = jnp.array(order + order, jnp.int32)[spot + jnp.arange(size, dtype=jnp.int32)]
    parity = jnp.bitwise_and(lax.axis_index(HEAD), 1).astype(jnp.int32)[None]
    scalars = jnp.concatenate([parity, places])
    share = gain_attn.shape[0]
    width, slots = w_query.shape[1], w_slot.shape[1]
    hidden_count = w_gate.shape[1]
    cut = (hidden_count // WIDE + 1) // 2 * WIDE
    spans = [(0, cut), (cut, hidden_count)]

    spare = jnp.zeros((share, 2 * BLOCK - slots - 2), w_slot.dtype)
    mix_shard = jnp.concatenate(
        [w_query, w_key, w_value, w_slot, gain_attn[:, None], gain_ffn[:, None], spare, w_out.T], axis=1
    )
    mix_count = 3 * width + 2 * BLOCK
    mix_pieces = ring_gather(mix_shard, order)
    down_rows = w_down.T
    feed_pieces = []
    for low, high in spans:
        shard = jnp.concatenate([w_gate[:, low:high], w_up[:, low:high], down_rows[:, low:high]], axis=1)
        feed_pieces.append(ring_gather(tie(shard, *flat_pieces([mix_pieces[size // 2]])), order))

    rows_low = move_columns(inputs, places, False)
    factor = norm_factor(to_wide(rows_low))
    back_low = move_columns(cotangent, places, False)
    rows_low, factor, _ = lax.optimization_barrier((rows_low, factor, back_low))

    qkv, logits, normed, gains = query_call(rows_low, factor, mix_pieces, slots, mix_count)
    gain_one, gain_two = gains[0:1], gains[1:2]
    bias = gate_bias[:, None]
    mixed, *saved = mixer_forward(lengths, qkv, logits, bias)
    kept, sent, (full_out,) = project_call(mixed, mix_pieces, parity, 2, mix_count, True)
    sums, _ = exchange(kept, sent)
    resid, normed_two = norm_call(scalars, sums, rows_low, gain_two)

    middle = size // 2

    def grads_of(pairs):
        span = slice(middle * share, (middle + 1) * share)
        far = to_low(jnp.concatenate([dot_tn(left[:, span], right) for left, right in pairs], axis=1))
        grads = [to_low(dot_tn(left, right)) for left, right in pairs]

        def piece_of(index):
            if index == middle:
                return far
            return jnp.concatenate([grad[index * share : (index + 1) * share] for grad in grads], axis=1)

        return piece_of

    partial, feed_grads = None, []
    for pieces in feed_pieces:
        if partial is None:
            hidden, pair, *partial = feed_call(normed_two, back_low, pieces, parity, None, 2)
        else:
            hidden, pair, weight = act_call(normed_two, back_low, pieces)
            partial = back_call(hidden, pair, weight, parity, partial, 2)
        piece_of = grads_of([(normed_two, pair), (back_low, hidden)])
        feed_grads += ring_scatter(piece_of, order)

    sums, _ = exchange(partial[:2], partial[2:4])
    d_attn, d_mixed = norm_back_call(scalars, sums, resid, back_low, gain_two, full_out)
    d_all, d_bias = mixer_backward(lengths, qkv, logits, bias, d_mixed, saved)
    bias_sum = total_sum(d_bias[:, 0], DP)
    mix_grads = ring_scatter(grads_of([(normed, d_all), (d_attn, mixed)]), order)
    kept, sent, _ = project_call(d_all, mix_pieces, parity, 2, 0, False)
    sums, halves = exchange(kept, sent)
    early, _ = exchange([partial[4]], partial[5:], halves)
    output = output_call(scalars, early, resid, size)
    *feed_out, gain_sum_two = finish_feed(feed_grads, w_gate, w_up, spans)
    sums[0] = tie(sums[0], output)
    grad_inputs = last_call(scalars, sums, d_attn, rows_low, gain_one, size)
    *mix_out, gain_sum_one = finish_mix(mix_grads, mix_shard, width, slots)
    gain_sums = total_sum(jnp.stack([gain_sum_one[:, 0], gain_sum_two[:, 0]]), HEAD)

    return (
        output,
        grad_inputs,
        gain_sums[0] / to_wide(gain_attn),
        *mix_out[:4],
        bias_sum,
        mix_out[4],
        gain_sums[1] / to_wide(gain_ffn),
        *feed_out,
    )


def solution(mesh):
    in_specs = (
        P(DP, None),
        P(DP),
        P(DP),
        P(DP, HEAD),
        P(DP, HEAD),
        P(DP, HEAD),
        P(DP, HEAD),
        P(HEAD),
        P(HEAD, DP),
        P(DP),
        P(DP, HEAD),
        P(DP, HEAD),
        P(HEAD, DP),
        P(DP, None),
    )
    out_specs = (
        P(DP, None),
        P(DP, None),
        P(DP),
        P(DP, HEAD),
        P(DP, HEAD),
        P(DP, HEAD),
        P(DP, HEAD),
        P(HEAD),
        P(HEAD, DP),
        P(DP),
        P(DP, HEAD),
        P(DP, HEAD),
        P(HEAD, DP),
    )
    return jax.shard_map(layer, mesh=mesh, in_specs=in_specs, out_specs=out_specs, check_vma=False)
```

```python
import jax
import jax.numpy as jnp
from jax import lax
from jax.experimental import pallas as pl
from jax.experimental.pallas import tpu as pltpu
from jax.sharding import PartitionSpec as P

BLOCK = 64
TILE = 128
DP, HEAD = "dp", "head"
epsilon = 1e-06
PAIR = 2
LAGS = 16


def split_low(values):
    high = values.astype(jnp.bfloat16)
    return high, (values - high.astype(jnp.float32)).astype(jnp.bfloat16)


def dot_nn(left, right):
    return lax.dot_general(left, right, (((1,), (0,)), ((), ())), preferred_element_type=jnp.float32)


def dot_nt(left, right):
    return lax.dot_general(left, right, (((1,), (1,)), ((), ())), preferred_element_type=jnp.float32)


def lane_place():
    lanes = lax.broadcasted_iota(jnp.int32, (BLOCK, TILE), 1)
    return lanes, jnp.bitwise_and(lanes, BLOCK - 1)


def suffix_sum(values, place):
    step = 1
    while step < BLOCK:
        values = values + jnp.where(place < BLOCK - step, pltpu.roll(values, TILE - step, 1), 0.0)
        step *= 2
    return values


def square_iotas():
    return (
        lax.broadcasted_iota(jnp.int32, (TILE, TILE), 0),
        lax.broadcasted_iota(jnp.int32, (TILE, TILE), 1),
    )


def level_masks():
    rows, columns = square_iotas()
    masks = []
    for half in (LAGS, 2 * LAGS):
        same = jnp.bitwise_and(rows, -2 * half) == jnp.bitwise_and(columns, -2 * half)
        apart = (jnp.bitwise_and(rows, half) == 0) & (jnp.bitwise_and(columns, half) != 0)
        masks.append(same & apart)
    return masks


def level_parts(square, masks):
    return jnp.concatenate([jnp.where(mask, square, 0.0) for mask in masks], axis=1)


def take_band(square, band_ref, slot):
    rows, columns = square_iotas()
    apart = columns - rows
    for lag in range(LAGS):
        band_ref[slot, lag : lag + 1, :] = jnp.sum(jnp.where(apart == lag, square, 0.0), axis=0, keepdims=True)


def put_band(square, band_ref, slot):
    rows, columns = square_iotas()
    apart = columns - rows
    for lag in range(LAGS):
        square = jnp.where(apart == lag, band_ref[slot, lag : lag + 1, :], square)
    return square


def fill_products(product_ref, slot, writes, inside):
    product_ref[slot, 0] = writes
    power, powers, reach = inside, [], 1
    while reach < LAGS:
        powers.append(power)
        for lag in range(reach):
            product_ref[slot, reach + lag] = power * pltpu.roll(product_ref[slot, lag], reach, 1)
        power = power * pltpu.roll(power, reach, 1)
        reach *= 2
    return powers


def lag_total(product_ref, slot, band_ref, start):
    sums = [start, None]
    for lag in range(LAGS):
        term = product_ref[slot, lag] * band_ref[slot, lag : lag + 1, :]
        held = sums[lag % 2]
        sums[lag % 2] = term if held is None else held + term
    return sums[0] + sums[1]


def lag_mix(product_ref, slot, band_ref, weights):
    for lag in range(LAGS):
        band_ref[slot, lag : lag + 1, :] = jnp.sum(weights * product_ref[slot, lag], axis=0, keepdims=True)


def lag_back(powers, term_of, low, count):
    if count == 1:
        return term_of(low)
    half = count // 2
    left = lag_back(powers, term_of, low, half)
    right = lag_back(powers, term_of, low + half, half)
    return left + pltpu.roll(powers[half.bit_length() - 1] * right, TILE - half, 1)


def two_rows(values):
    high, low = split_low(values)
    return jnp.concatenate([high, low], axis=0)


def level_total(near, parts, faded):
    high, low = split_low(parts)
    lefts = jnp.concatenate([two_rows(left) for left in near], axis=0)
    tall = dot_nn(lefts, high)
    short = dot_nn(jnp.concatenate([split_low(left)[0] for left in near], axis=0), low)
    total = 0.0
    for index, right in enumerate(faded):
        span = slice(index * TILE, (index + 1) * TILE)
        rows = tall[2 * index * BLOCK : 2 * (index + 1) * BLOCK, span]
        total = total + right * (rows[:BLOCK] + rows[BLOCK:] + short[index * BLOCK : (index + 1) * BLOCK, span])
    return total


def level_mix(square, near, faded, masks):
    for left, right, mask in zip(near, faded, masks):
        square = jnp.where(
            mask,
            lax.dot_general(
                left.astype(jnp.bfloat16), right.astype(jnp.bfloat16), (((0,), (0,)), ((), ())),
                preferred_element_type=jnp.float32,
            ),
            square,
        )
    return square


def level_back(lefts, parts, rest):
    rows = jnp.concatenate([two_rows(left) for left in lefts], axis=0)
    high, low = split_low(jnp.concatenate(parts, axis=0))
    tall = dot_nt(rows, high)
    short = dot_nt(jnp.concatenate([split_low(left)[0] for left in lefts], axis=0), low)
    total = 0.0
    for index, factor in enumerate(rest):
        span = slice(index * TILE, (index + 1) * TILE)
        one = tall[2 * index * BLOCK : 2 * (index + 1) * BLOCK, span]
        total = total + factor * (one[:BLOCK] + one[BLOCK:] + short[index * BLOCK : (index + 1) * BLOCK, span])
    return total


def gate_terms(logits, valid, place):
    log_sig = jnp.minimum(logits, 0.0) - jnp.log1p(jnp.exp(-jnp.abs(logits)))
    logdecay = valid * log_sig * 0.125
    decay = jnp.exp(logdecay)
    series = -logdecay * (1.0 + logdecay * (0.5 + logdecay * (1.0 / 6.0 + logdecay * (1.0 / 24.0))))
    writes = valid * jnp.where(logdecay > -0.03, series, 1.0 - decay)
    low = jnp.bitwise_and(place, LAGS - 1)
    inside = jnp.where(low == 0, 0.0, decay)
    before, rest, step = logdecay, logdecay, 1
    while step < LAGS:
        before = before + jnp.where(low >= step, pltpu.roll(before, step, 1), 0.0)
        rest = rest + jnp.where(low < LAGS - step, pltpu.roll(rest, TILE - step, 1), 0.0)
        step *= 2
    rest = rest - logdecay
    scans = []
    while step < BLOCK:
        scans.append((jnp.exp(before), jnp.exp(rest)))
        total, upper = before + rest, jnp.bitwise_and(place, step) != 0
        before = before + jnp.where(upper, pltpu.roll(total, step, 1), 0.0)
        rest = rest + jnp.where(upper, 0.0, pltpu.roll(total, TILE - step, 1))
        step *= 2
    return decay, writes, inside, before, rest, scans


def stacked(values, lanes):
    return jnp.concatenate(
        [jnp.where(lanes < BLOCK, values, 0.0), jnp.where(lanes < BLOCK, 0.0, values)], axis=0
    )


def own_block(square, lanes):
    return jnp.where(lanes < BLOCK, square[:BLOCK], square[BLOCK:])


def forward_kernel(
    length_ref, qkv_ref, logit_ref, bias_ref,
    mixed_ref, state_ref, prob_ref, score_ref, mix_ref,
    gate_ref, carry_ref, band_ref, mix_band_ref, product_ref,
):
    width = mixed_ref.shape[1]
    tiles = mixed_ref.shape[0] // TILE
    scale = width ** -0.5
    lanes, place = lane_place()
    bias = bias_ref[...]

    def valid_of(tile):
        return (lanes + tile * TILE < length_ref[0]).astype(jnp.float32)

    def rows_of(tile):
        return pl.ds(pl.multiple_of(tile * TILE, TILE), TILE)

    def gather_writes(tile, none):
        logits = logit_ref[tile] + bias
        _, writes, inside, before, after, scans = gate_terms(logits, valid_of(tile), place)
        for index, (faded, rest) in enumerate(scans):
            gate_ref[tile, 4 + 2 * index] = faded
            gate_ref[tile, 5 + 2 * index] = rest * writes
        gate_ref[tile, 0] = writes
        gate_ref[tile, 1] = inside
        gate_ref[tile, 2] = jnp.exp(before)
        gate_ref[tile, 3] = jnp.exp(before + after)
        high, low = split_low(stacked(jnp.exp(after) * writes, lanes))
        rows = qkv_ref[rows_of(tile), width:]
        added = dot_nn(high, rows) + dot_nn(low, rows)
        state_ref[tile] = added
        return none

    lax.fori_loop(0, tiles, gather_writes, 0)

    carry_ref[...] = jnp.zeros_like(carry_ref)

    def run_states(tile, none):
        for part in range(2):
            span = pl.ds(part * BLOCK, BLOCK)
            fade = gate_ref[tile, 3, :, part * BLOCK : part * BLOCK + 1]
            carried = carry_ref[...]
            added = state_ref[tile, span, :]
            state_ref[tile, span, :] = carried
            carry_ref[...] = fade * carried + added
        return none

    lax.fori_loop(0, tiles, run_states, 0)

    masks = level_masks()

    def mix_pair(pair, none):
        both = [(slot, PAIR * pair + slot) for slot in range(PAIR)]
        queries, scores, probs, squares = {}, {}, {}, {}

        def faded_of(tile):
            return [gate_ref[tile, 4], gate_ref[tile, 6]]

        def near_of(tile):
            return [gate_ref[tile, 5], gate_ref[tile, 7]]

        for slot, tile in both:
            queries[slot] = qkv_ref[rows_of(tile), :width]
            squares[slot] = dot_nt(qkv_ref[rows_of(tile), width : 2 * width], queries[slot]) * scale
        for slot, tile in both:
            fill_products(product_ref, slot, gate_ref[tile, 0], gate_ref[tile, 1])
        for slot, tile in both:
            high, low = split_low(state_ref[tile, :, :width])
            carried = own_block(dot_nt(high, queries[slot]) + dot_nt(low, queries[slot]), lanes)
            scores[slot] = gate_ref[tile, 2] * carried * scale
        for slot, tile in both:
            take_band(squares[slot], band_ref, slot)
            scores[slot] = scores[slot] + level_total(
                near_of(tile), level_parts(squares[slot], masks), faded_of(tile)
            )
        for slot, tile in both:
            scores[slot] = lag_total(product_ref, slot, band_ref, scores[slot])
        for slot, tile in both:
            top = jnp.max(scores[slot], axis=0, keepdims=True)
            raised = jnp.exp(scores[slot] - top)
            probs[slot] = raised / jnp.sum(raised, axis=0, keepdims=True)
            score_ref[tile] = scores[slot]
            prob_ref[tile] = probs[slot]
        for slot, tile in both:
            lag_mix(product_ref, slot, mix_band_ref, probs[slot])
        for slot, tile in both:
            mixing = put_band(jnp.zeros((TILE, TILE), jnp.float32), mix_band_ref, slot)
            mixing = level_mix(mixing, near_of(tile), [probs[slot] * one for one in faded_of(tile)], masks)
            mixing = mixing.astype(jnp.bfloat16)
            mix_ref[tile] = mixing
            reach = stacked(probs[slot] * gate_ref[tile, 2], lanes).T.astype(jnp.bfloat16)
            result = dot_nn(mixing.T, qkv_ref[rows_of(tile), 2 * width :]) + dot_nn(
                reach, state_ref[tile, :, width:].astype(jnp.bfloat16)
            )
            rows = lax.broadcasted_iota(jnp.int32, (TILE, 1), 0) + tile * TILE
            mixed_ref[rows_of(tile), :] = jnp.where(rows < length_ref[0], result, 0.0).astype(jnp.bfloat16)
        return none

    lax.fori_loop(0, tiles // PAIR, mix_pair, 0)


def backward_kernel(
    length_ref, qkv_ref, logit_ref, bias_ref, back_ref, state_ref, prob_ref, score_ref, mix_ref,
    d_qkv_ref, d_bias_ref,
    adjoint_ref, gain_ref, key_band_ref, value_band_ref, band_ref, carry_ref, end_ref, cross_ref, product_ref,
):
    width = back_ref.shape[1]
    tiles = back_ref.shape[0] // TILE
    scale = width ** -0.5
    lanes, place = lane_place()
    bias = bias_ref[...]

    def valid_of(tile):
        return (lanes + tile * TILE < length_ref[0]).astype(jnp.float32)

    def rows_of(tile):
        return pl.ds(pl.multiple_of(tile * TILE, TILE), TILE)

    def back_of(tile):
        rows = lax.broadcasted_iota(jnp.int32, (TILE, 1), 0) + tile * TILE
        return jnp.where(rows < length_ref[0], back_ref[rows_of(tile), :], jnp.zeros((), back_ref.dtype))

    masks = level_masks()

    def slopes(pair, none):
        both = [(slot, PAIR * pair + slot) for slot in range(PAIR)]
        fades, powers, queries, keys, backs, gains, d_scores, faded, rests, near = ({} for _ in range(10))
        key_squares, value_squares = {}, {}
        for slot, tile in both:
            queries[slot] = qkv_ref[rows_of(tile), :width]
            keys[slot] = qkv_ref[rows_of(tile), width : 2 * width]
            backs[slot] = back_of(tile)
            key_squares[slot] = dot_nt(keys[slot], queries[slot]) * scale
            value_squares[slot] = dot_nt(qkv_ref[rows_of(tile), 2 * width :], backs[slot])
        for slot, tile in both:
            decay, writes, inside, before, after, scans = gate_terms(logit_ref[tile] + bias, valid_of(tile), place)
            faded[slot], rests[slot] = [one for one, _ in scans], [one for _, one in scans]
            near[slot] = [one * writes for one in rests[slot]]
            fades[slot] = jnp.exp(before)
            gain_ref[tile, 2] = decay
            gain_ref[tile, 3] = writes
            gain_ref[tile, 4] = jnp.exp(after)
            gain_ref[tile, 5] = jnp.exp(before + after)
            powers[slot] = fill_products(product_ref, slot, writes, inside)
        for slot, tile in both:
            high, low = split_low(state_ref[tile, :, width:])
            carried = own_block(dot_nt(high, backs[slot]) + dot_nt(low, backs[slot]), lanes)
            gains[slot] = fades[slot] * carried
        for slot, tile in both:
            take_band(key_squares[slot], key_band_ref, slot)
            take_band(value_squares[slot], value_band_ref, slot)
            gains[slot] = gains[slot] + level_total(
                near[slot], level_parts(value_squares[slot], masks), faded[slot]
            )
        for slot, tile in both:
            gains[slot] = lag_total(product_ref, slot, value_band_ref, gains[slot])
        for slot, tile in both:
            probs = prob_ref[tile]
            d_scores[slot] = probs * (gains[slot] - jnp.sum(probs * gains[slot], axis=0, keepdims=True))
            gain_ref[tile, 1] = d_scores[slot] * score_ref[tile] + probs * gains[slot]
        for slot, tile in both:
            lag_mix(product_ref, slot, band_ref, d_scores[slot])
        for slot, tile in both:
            probs = prob_ref[tile]

            def term_of(lag, slot=slot, probs=probs):
                row = slice(lag, lag + 1)
                return d_scores[slot] * key_band_ref[slot, row, :] + probs * value_band_ref[slot, row, :]

            lefts = [jnp.concatenate([d_scores[slot] * one, probs * one], axis=1) for one in faded[slot]]
            parts = [
                jnp.concatenate(
                    [jnp.where(mask, key_squares[slot], 0.0), jnp.where(mask, value_squares[slot], 0.0)], axis=1
                )
                for mask in masks
            ]
            gain_ref[tile, 0] = lag_back(powers[slot], term_of, 0, LAGS) + level_back(lefts, parts, rests[slot])
        for slot, tile in both:
            mixing = put_band(jnp.zeros((TILE, TILE), jnp.float32), band_ref, slot)
            mixing = level_mix(mixing, near[slot], [d_scores[slot] * one for one in faded[slot]], masks)
            mixing = (mixing * scale).astype(jnp.bfloat16)
            reach = stacked(d_scores[slot] * fades[slot] * scale, lanes)
            held = stacked(prob_ref[tile] * fades[slot], lanes).astype(jnp.bfloat16)
            d_qkv_ref[rows_of(tile), :width] = (
                dot_nn(mixing.T, keys[slot])
                + dot_nn(reach.T.astype(jnp.bfloat16), state_ref[tile, :, :width].astype(jnp.bfloat16))
            ).astype(jnp.bfloat16)
            adjoint_ref[tile, :, :width] = dot_nn(reach.astype(jnp.bfloat16), queries[slot])
            adjoint_ref[tile, :, width:] = dot_nn(held, backs[slot])
            d_qkv_ref[rows_of(tile), width : 2 * width] = dot_nn(mixing, queries[slot]).astype(jnp.bfloat16)
            d_qkv_ref[rows_of(tile), 2 * width : 3 * width] = dot_nn(mix_ref[tile], backs[slot]).astype(jnp.bfloat16)
        return none

    lax.fori_loop(0, tiles // PAIR, slopes, 0)

    carry_ref[...] = jnp.zeros_like(carry_ref)
    end_ref[...] = jnp.zeros_like(end_ref)

    def run_adjoints(count, none):
        tile = tiles - 1 - count
        for part in (1, 0):
            span = pl.ds(part * BLOCK, BLOCK)
            fade = gain_ref[tile, 5, :, part * BLOCK : part * BLOCK + 1]
            carried = carry_ref[...]
            added = adjoint_ref[tile, span, :]
            adjoint_ref[tile, span, :] = carried
            cross_ref[tile, span, :] = jnp.broadcast_to(
                jnp.sum(carried * end_ref[...], axis=1, keepdims=True), (BLOCK, TILE)
            )
            end_ref[...] = state_ref[tile, span, :]
            carry_ref[...] = fade * carried + added
        return none

    lax.fori_loop(0, tiles, run_adjoints, 0)

    d_bias_ref[...] = jnp.zeros_like(d_bias_ref)

    def finish(tile, none):
        key_rows = qkv_ref[rows_of(tile), width : 2 * width]
        value_rows = qkv_ref[rows_of(tile), 2 * width :]
        adjoint = adjoint_ref[tile]
        high, low = split_low(adjoint)
        rows = qkv_ref[rows_of(tile), width:]
        carried = own_block(dot_nt(high, rows) + dot_nt(low, rows), lanes)
        decay, writes, rest = gain_ref[tile, 2], gain_ref[tile, 3], gain_ref[tile, 4]
        d_writes = gain_ref[tile, 0] + rest * carried
        tail = stacked(rest * writes, lanes).T.astype(jnp.bfloat16)
        d_qkv_ref[rows_of(tile), width : 3 * width] = (
            d_qkv_ref[rows_of(tile), width : 3 * width].astype(jnp.float32) + dot_nn(tail, high)
        ).astype(jnp.bfloat16)
        cross = own_block(cross_ref[tile], lanes)
        d_decay = suffix_sum(gain_ref[tile, 1] - writes * d_writes, place) + cross - decay * d_writes
        logits = logit_ref[tile] + bias
        d_logit = valid_of(tile) * d_decay * jax.nn.sigmoid(-logits) * 0.125
        d_bias_ref[...] += jnp.broadcast_to(jnp.sum(d_logit, axis=1, keepdims=True), (BLOCK, TILE))
        d_qkv_ref[rows_of(tile), 3 * width :] = jnp.concatenate([d_logit, jnp.zeros_like(d_logit)], axis=0).T.astype(jnp.bfloat16)
        return none

    lax.fori_loop(0, tiles, finish, 0)


def mixer_forward(length, qkv, logits, bias):
    rows, width = qkv.shape[0], qkv.shape[1] // 3
    tiles = rows // TILE
    f32 = jnp.float32
    return pl.pallas_call(
        forward_kernel,
        out_shape=(
            jax.ShapeDtypeStruct((rows, width), jnp.bfloat16),
            jax.ShapeDtypeStruct((tiles, TILE, 2 * width), f32),
            jax.ShapeDtypeStruct((tiles, BLOCK, TILE), f32),
            jax.ShapeDtypeStruct((tiles, BLOCK, TILE), f32),
            jax.ShapeDtypeStruct((tiles, TILE, TILE), jnp.bfloat16),
        ),
        in_specs=[pl.BlockSpec(memory_space=pltpu.SMEM)] + [pl.BlockSpec(memory_space=pltpu.VMEM)] * 3,
        out_specs=[pl.BlockSpec(memory_space=pltpu.VMEM)] * 5,
        scratch_shapes=[
            pltpu.VMEM((tiles, 8, BLOCK, TILE), f32),
            pltpu.VMEM((BLOCK, 2 * width), f32),
            pltpu.VMEM((PAIR, LAGS, TILE), f32),
            pltpu.VMEM((PAIR, LAGS, TILE), f32),
            pltpu.VMEM((PAIR, LAGS, BLOCK, TILE), f32),
        ],
        compiler_params=pltpu.CompilerParams(vmem_limit_bytes=22 * MEBI),
        name="mixer_forward",
    )(length, qkv, logits, bias)


def mixer_backward(length, qkv, logits, bias, back, saved):
    rows, width = qkv.shape[0], qkv.shape[1] // 3
    tiles = rows // TILE
    f32 = jnp.float32
    return pl.pallas_call(
        backward_kernel,
        out_shape=(
            jax.ShapeDtypeStruct((rows, 3 * width + 2 * BLOCK), jnp.bfloat16),
            jax.ShapeDtypeStruct((BLOCK, TILE), f32),
        ),
        in_specs=[pl.BlockSpec(memory_space=pltpu.SMEM)] + [pl.BlockSpec(memory_space=pltpu.VMEM)] * 8,
        out_specs=[pl.BlockSpec(memory_space=pltpu.VMEM)] * 2,
        scratch_shapes=[
            pltpu.VMEM((tiles, TILE, 2 * width), f32),
            pltpu.VMEM((tiles, 6, BLOCK, TILE), f32),
            pltpu.VMEM((PAIR, LAGS, TILE), f32),
            pltpu.VMEM((PAIR, LAGS, TILE), f32),
            pltpu.VMEM((PAIR, LAGS, TILE), f32),
            pltpu.VMEM((BLOCK, 2 * width), f32),
            pltpu.VMEM((BLOCK, 2 * width), f32),
            pltpu.VMEM((tiles, TILE, TILE), f32),
            pltpu.VMEM((PAIR, LAGS, BLOCK, TILE), f32),
        ],
        compiler_params=pltpu.CompilerParams(vmem_limit_bytes=32 * MEBI),
        name="mixer_backward",
    )(length, qkv, logits, bias, back, *saved)


def to_low(values):
    return values.astype(jnp.bfloat16)


def to_wide(values):
    return values.astype(jnp.float32)


def dot_tn(left, right):
    return lax.dot_general(left, right, (((0,), (0,)), ((), ())), preferred_element_type=jnp.float32)


def tie(values, *earlier):
    return lax.optimization_barrier((values,) + earlier)[0]


def ring_order(size):
    return list(range(0, size, 2)) + list(range(size - 1 - size % 2, 0, -2))


def hop_pairs(order, hop):
    size = len(order)
    return [(order[i], order[(i + hop) % size]) for i in range(size)]


def ring_gather(shard, order):
    size = len(order)
    up, down = hop_pairs(order, 1), hop_pairs(order, -1)
    pieces = [shard] + [None] * (size - 1)
    from_low, from_high = shard, shard
    for step in range(1, (size + 1) // 2):
        from_low = lax.ppermute(from_low, DP, up)
        from_high = lax.ppermute(from_high, DP, down)
        pieces[size - step], pieces[step] = from_low, from_high
    if size % 2 == 0:
        half = shard.shape[0] // 2
        first = lax.ppermute(from_low[:half], DP, up)
        second = lax.ppermute(from_high[half:], DP, down)
        pieces[size // 2] = (first, second)
    return pieces


def ring_scatter(piece_of, order):
    size = len(order)
    up, down = hop_pairs(order, 1), hop_pairs(order, -1)
    half_count = (size - 1) // 2
    up_sum, down_sum = None, None
    if size % 2 == 0:
        farthest = piece_of(size // 2)
        half = farthest.shape[0] // 2 if not isinstance(farthest, tuple) else 0
        if half:
            farthest = (farthest[:half], farthest[half:])
        up_half = lax.ppermute(to_low(farthest[0]), DP, up)
        down_half = lax.ppermute(to_low(farthest[1]), DP, down)
        up_sum = jnp.concatenate([to_wide(up_half), jnp.zeros(up_half.shape, jnp.float32)], axis=0)
        down_sum = jnp.concatenate([jnp.zeros(down_half.shape, jnp.float32), to_wide(down_half)], axis=0)
    for step in range(half_count, 0, -1):
        up_piece, down_piece = to_wide(piece_of(step)), to_wide(piece_of(size - step))
        if up_sum is not None:
            up_piece, down_piece = up_piece + up_sum, down_piece + down_sum
        up_sum = to_wide(lax.ppermute(to_low(up_piece), DP, up))
        down_sum = to_wide(lax.ppermute(to_low(down_piece), DP, down))
    return piece_of(0), to_low(up_sum), to_low(down_sum)


def total_sum(values, axis):
    count = lax.axis_size(axis)
    step = 1
    while step < count:
        values = values + lax.ppermute(values, axis, [(i, i ^ step) for i in range(count)])
        step *= 2
    return values


def move_kernel(places_ref, source_ref, target_ref):
    target_ref[...] = source_ref[...]


def move_columns(matrix, places, inverse):
    size = places.shape[0]
    rows, columns = matrix.shape
    width = columns // size
    if width % 128:
        split = matrix.reshape(rows, size, width)
        if inverse:
            places = jnp.argsort(places)
        return jnp.take(split, places, axis=1).reshape(rows, columns)

    def plain(step, places_ref):
        return (0, step)

    def placed(step, places_ref):
        return (0, places_ref[step])

    return pl.pallas_call(
        move_kernel,
        out_shape=jax.ShapeDtypeStruct(matrix.shape, matrix.dtype),
        grid_spec=pltpu.PrefetchScalarGridSpec(
            num_scalar_prefetch=1,
            grid=(size,),
            in_specs=[pl.BlockSpec((rows, width), plain if inverse else placed)],
            out_specs=pl.BlockSpec((rows, width), placed if inverse else plain),
        ),
        compiler_params=pltpu.CompilerParams(vmem_limit_bytes=8 * MEBI),
        cost_estimate=pl.CostEstimate(flops=0, bytes_accessed=2 * matrix.size * matrix.dtype.itemsize, transcendentals=0),
    )(places, matrix)


ROWS = 128
WIDE = 256
MEBI = 1024 * 1024


def vmem_call(body, out_shape, operands, limit, scratch=(), scalars=1, anywhere=0, flops=0, moved=0):
    spaces = (
        [pl.BlockSpec(memory_space=pltpu.SMEM)] * scalars
        + [pl.BlockSpec(memory_space=pltpu.VMEM)] * (len(operands) - scalars - anywhere)
        + [pl.BlockSpec(memory_space=pl.ANY)] * anywhere
    )
    return pl.pallas_call(
        body,
        out_shape=out_shape,
        in_specs=spaces,
        out_specs=[pl.BlockSpec(memory_space=pltpu.VMEM)] * len(out_shape),
        scratch_shapes=list(scratch),
        compiler_params=pltpu.CompilerParams(vmem_limit_bytes=limit * MEBI),
        cost_estimate=pl.CostEstimate(flops=flops, bytes_accessed=moved, transcendentals=0),
    )(*operands)


def load_blocks(sources, target_ref, sems, blocks, low=0):
    groups = []
    for block in blocks:
        copies = []
        for first, span in block:
            start = 0
            for source in sources:
                rows = source.shape[0]
                index = sum(map(len, groups)) + len(copies)
                copies.append(
                    pltpu.make_async_copy(
                        source.at[:, pl.ds(low + first, span)],
                        target_ref.at[pl.ds(start, rows), pl.ds(first, span)],
                        sems.at[index],
                    )
                )
                start += rows
        groups.append(copies)
    for copies in groups:
        for copy in copies:
            copy.start()
    return groups


def finish(copies):
    for copy in copies:
        copy.wait()


def flat_pieces(pieces):
    flat = []
    for piece in pieces:
        flat += list(piece) if isinstance(piece, tuple) else [piece]
    return flat


def give_halves(block_ref, parity, parts, columns, kept_refs, sent_refs):
    rows = block_ref.shape[0] // parts // 2
    for part in range(parts):
        kept_refs[part][:, columns] = block_ref[pl.ds((2 * part + parity) * rows, rows), :].astype(jnp.bfloat16)
        sent_refs[part][:, columns] = block_ref[pl.ds((2 * part + 1 - parity) * rows, rows), :].astype(jnp.bfloat16)


def project_call(left, pieces, parity, parts, low, keep):
    rows, depth = left.shape
    flat = flat_pieces(pieces)
    count = len(flat)
    total = sum(piece.shape[0] for piece in flat)

    def body(parity_ref, left_ref, *refs):
        sources, outs = refs[:count], refs[count:]
        block_ref, sems = outs[-2:]
        weight_ref = outs[-3]
        finish(load_blocks(sources, weight_ref, sems, [[(0, depth)]], low)[0])
        parity = parity_ref[0]

        def one(step, none):
            columns = pl.ds(pl.multiple_of(step * WIDE, WIDE), WIDE)
            block_ref[...] = dot_nt(left_ref[...], weight_ref[columns, :])
            give_halves(block_ref, parity, parts, columns, outs[:parts], outs[parts : 2 * parts])
            return none

        lax.fori_loop(0, total // WIDE, one, 0)

    half = jax.ShapeDtypeStruct((rows // parts // 2, total), jnp.bfloat16)
    weight = (total, depth)
    outs = vmem_call(
        body,
        [half] * (2 * parts) + ([jax.ShapeDtypeStruct(weight, jnp.bfloat16)] if keep else []),
        (parity, left, *flat), 12 if keep else 22,
        scratch=([] if keep else [pltpu.VMEM(weight, jnp.bfloat16)])
        + [
            pltpu.VMEM((rows, WIDE), jnp.float32),
            pltpu.SemaphoreType.DMA((count,)),
        ],
        anywhere=count, flops=2 * rows * depth * total, moved=2 * (rows * depth + depth * total + rows * total),
    )
    return outs[:parts], outs[parts : 2 * parts], outs[2 * parts :]


def query_call(rows_low, factor, pieces, slots, columns_all):
    rows, depth = rows_low.shape
    flat = flat_pieces(pieces)
    count = len(flat)
    wide = columns_all - 2 * slots
    blocks = [[(wide, 2 * slots)]] + [[(start, 2 * WIDE)] for start in range(0, wide, 2 * WIDE)]

    def body(rows_ref, factor_ref, *refs):
        sources = refs[:count]
        qkv_ref, logit_ref, normed_ref, gain_ref, weight_ref, sems = refs[count:]
        groups = load_blocks(sources, weight_ref, sems, blocks)
        finish(groups[0])
        gain_ref[...] = weight_ref[:, wide:].astype(jnp.float32).T[slots : slots + 8]

        def norm_rows(step, none):
            span = pl.ds(pl.multiple_of(step * TILE, TILE), TILE)
            values = rows_ref[span, :].astype(jnp.float32)
            normed_ref[span, :] = (values * factor_ref[span, :] * gain_ref[0:1, :]).astype(jnp.bfloat16)
            return none

        lax.fori_loop(0, rows // TILE, norm_rows, 0)
        logits = dot_nn(normed_ref[...], weight_ref[:, wide:])
        for tile in range(rows // TILE):
            logit_ref[tile] = logits[tile * TILE : (tile + 1) * TILE, :].T[:slots]
        for copies in groups[1:]:
            finish(copies)

        def one(step, none):
            columns = pl.ds(pl.multiple_of(step * WIDE, WIDE), WIDE)
            qkv_ref[:, columns] = dot_nn(normed_ref[...], weight_ref[:, columns]).astype(jnp.bfloat16)
            return none

        lax.fori_loop(0, wide // WIDE, one, 0)

    return vmem_call(
        body,
        [
            jax.ShapeDtypeStruct((rows, wide), jnp.bfloat16),
            jax.ShapeDtypeStruct((rows // TILE, slots, TILE), jnp.float32),
            jax.ShapeDtypeStruct((rows, depth), jnp.bfloat16),
            jax.ShapeDtypeStruct((8, depth), jnp.float32),
        ],
        (rows_low, factor, *flat), 28,
        scratch=[pltpu.VMEM((depth, columns_all), jnp.bfloat16), pltpu.SemaphoreType.DMA((count * len(blocks),))],
        scalars=0, anywhere=count,
        flops=2 * rows * depth * columns_all, moved=2 * (rows + columns_all) * depth + 2 * rows * columns_all,
    )


def far_pieces(normed_ref, back_ref, hidden_ref, pair_ref, far_refs, share):
    half, middle = share // 2, normed_ref.shape[1] // share // 2
    columns = slice(middle * share, (middle + 1) * share)
    width = pair_ref.shape[1]
    pair = dot_tn(normed_ref[:, columns], pair_ref[...]).astype(jnp.bfloat16)
    down = dot_tn(back_ref[:, columns], hidden_ref[...]).astype(jnp.bfloat16)
    for part, far_ref in enumerate(far_refs):
        far_ref[:, :width] = pair[part * half : (part + 1) * half]
        far_ref[:, width:] = down[part * half : (part + 1) * half]


def act_columns(start, span, hidden, normed_ref, back_ref, weight_ref, hidden_ref, pair_ref):
    def columns(base):
        return pl.ds(start + base, span)

    gate_act = dot_nn(normed_ref[...], weight_ref[:, columns(0)])
    up_act = dot_nn(normed_ref[...], weight_ref[:, columns(hidden)])
    d_hidden = dot_nn(back_ref[...], weight_ref[:, columns(2 * hidden)])
    sigma = 1.0 / (1.0 + jnp.exp(-gate_act))
    gated = gate_act * sigma
    hidden_ref[:, columns(0)] = (gated * up_act).astype(jnp.bfloat16)
    pair_ref[:, columns(hidden)] = (d_hidden * gated).astype(jnp.bfloat16)
    pair_ref[:, columns(0)] = (d_hidden * up_act * (sigma * (1.0 + gate_act * (1.0 - sigma)))).astype(jnp.bfloat16)


def feed_call(normed, back, pieces, parity, earlier, parts):
    rows, depth = normed.shape
    flat = flat_pieces(pieces)
    count = len(flat)
    hidden = flat[0].shape[1] // 3
    given = 0 if earlier is None else 2
    blocks = [
        [(part * hidden, WIDE) for part in range(3)],
        [(part * hidden + WIDE, hidden - WIDE) for part in range(3)],
    ]

    def body(parity_ref, *refs):
        sources = refs[: count + 2 + given]
        outs = refs[count + 2 + given :]
        hidden_ref, pair_ref = outs[:2]
        far_refs = outs[2:4]
        total_refs = outs[4 : 6 if earlier is None else 6 + 2 * parts]
        outs = outs[4 + len(total_refs) :]
        weight_ref, normed_ref, back_ref, block_ref = outs[:4]
        sems = outs[-1]
        held = [
            pltpu.make_async_copy(sources[count], normed_ref, sems.at[6 * count]),
            pltpu.make_async_copy(sources[count + 1], back_ref, sems.at[6 * count + 1]),
        ]
        held[0].start()
        held[1].start()
        groups = load_blocks(sources[:count], weight_ref, sems, blocks)
        if given:
            sum_ref = outs[4]
            held += [
                pltpu.make_async_copy(sources[count + 2 + i], sum_ref.at[i], sems.at[6 * count + 2 + i]) for i in range(2)
            ]
            held[2].start()
            held[3].start()

        def act(start, span):
            act_columns(start, span, hidden, normed_ref, back_ref, weight_ref, hidden_ref, pair_ref)

        finish(held[:2])
        finish(groups[0])
        act(0, WIDE)
        for copies in groups[1:]:
            finish(copies)

        def act_wide(step, none):
            act(pl.multiple_of(step * WIDE, WIDE), WIDE)
            return none

        lax.fori_loop(1, hidden // WIDE, act_wide, 0)
        if hidden % WIDE:
            act(hidden // WIDE * WIDE, hidden % WIDE)
        far_pieces(normed_ref, back_ref, hidden_ref, pair_ref, far_refs, share)
        finish(held[2:])
        parity = parity_ref[0]

        def one(step, none):
            columns = pl.ds(pl.multiple_of(step * WIDE, WIDE), WIDE)
            d_block = dot_nt(pair_ref[...], weight_ref[columns, : 2 * hidden])
            y_block = dot_nt(hidden_ref[...], weight_ref[columns, 2 * hidden :])
            if not given:
                total_refs[0][:, columns] = d_block.astype(jnp.bfloat16)
                total_refs[1][:, columns] = y_block.astype(jnp.bfloat16)
            else:
                block_ref[...] = d_block + sum_ref[0, :, columns].astype(jnp.float32)
                give_halves(block_ref, parity, parts, columns, total_refs[:parts], total_refs[parts : 2 * parts])
                block_ref[...] = y_block + sum_ref[1, :, columns].astype(jnp.float32)
                give_halves(block_ref, parity, 1, columns, total_refs[2 * parts :][:1], total_refs[2 * parts + 1 :])
            return none

        lax.fori_loop(0, depth // WIDE, one, 0)

    low = jnp.bfloat16
    share = flat[0].shape[0]
    outs = [jax.ShapeDtypeStruct((rows, hidden), low), jax.ShapeDtypeStruct((rows, 2 * hidden), low)]
    outs += [jax.ShapeDtypeStruct((share // 2, 3 * hidden), low)] * 2
    if earlier is None:
        outs += [jax.ShapeDtypeStruct((rows, depth), low)] * 2
    else:
        outs += [jax.ShapeDtypeStruct((rows // parts // 2, depth), low)] * (2 * parts)
        outs += [jax.ShapeDtypeStruct((rows // 2, depth), low)] * 2
    scratch = [
        pltpu.VMEM((depth, 3 * hidden), low),
        pltpu.VMEM((rows, depth), low),
        pltpu.VMEM((rows, depth), low),
        pltpu.VMEM((rows, WIDE), jnp.float32),
    ]
    if given:
        scratch.append(pltpu.VMEM((2, rows, depth), low))
    scratch.append(pltpu.SemaphoreType.DMA((6 * count + 2 + given,)))
    return vmem_call(
        body, outs, (parity, *flat, normed, back, *(earlier or ())), 50,
        scratch=scratch, anywhere=count + 2 + given,
        flops=2 * rows * depth * hidden * 6, moved=2 * (3 * rows * depth + 3 * depth * hidden + 3 * rows * hidden),
    )


def act_call(normed, back, pieces):
    rows, depth = normed.shape
    flat = flat_pieces(pieces)
    count = len(flat)
    hidden = flat[0].shape[1] // 3
    blocks = [
        [(part * hidden, WIDE) for part in range(3)],
        [(part * hidden + WIDE, hidden - WIDE) for part in range(3)],
    ]

    def body(*refs):
        sources, (hidden_ref, pair_ref, weight_ref), far_refs = refs[:-8], refs[-8:-5], refs[-5:-3]
        normed_ref, back_ref, sems = refs[-3:]
        held = [
            pltpu.make_async_copy(sources[count], normed_ref, sems.at[6 * count]),
            pltpu.make_async_copy(sources[count + 1], back_ref, sems.at[6 * count + 1]),
        ]
        held[0].start()
        held[1].start()
        groups = load_blocks(sources[:count], weight_ref, sems, blocks)

        def act(start, span):
            act_columns(start, span, hidden, normed_ref, back_ref, weight_ref, hidden_ref, pair_ref)

        finish(held + groups[0])
        act(0, WIDE)
        finish(groups[1])

        def act_wide(step, none):
            act(pl.multiple_of(step * WIDE, WIDE), WIDE)
            return none

        lax.fori_loop(1, hidden // WIDE, act_wide, 0)
        if hidden % WIDE:
            act(hidden // WIDE * WIDE, hidden % WIDE)
        far_pieces(normed_ref, back_ref, hidden_ref, pair_ref, far_refs, share)

    low = jnp.bfloat16
    share = flat[0].shape[0]
    return vmem_call(
        body,
        [
            jax.ShapeDtypeStruct((rows, hidden), low),
            jax.ShapeDtypeStruct((rows, 2 * hidden), low),
            jax.ShapeDtypeStruct((depth, 3 * hidden), low),
        ]
        + [jax.ShapeDtypeStruct((share // 2, 3 * hidden), low)] * 2,
        (*flat, normed, back), 42,
        scratch=[
            pltpu.VMEM((rows, depth), low),
            pltpu.VMEM((rows, depth), low),
            pltpu.SemaphoreType.DMA((6 * count + 2,)),
        ],
        scalars=0, anywhere=count + 2,
        flops=2 * rows * depth * hidden * 3, moved=2 * (2 * rows * depth + 6 * depth * hidden + 3 * rows * hidden),
    )


def back_call(hidden_rows, pair_rows, weight, parity, earlier, parts):
    rows, hidden = hidden_rows.shape
    depth = weight.shape[0]

    def body(parity_ref, hidden_ref, pair_ref, weight_ref, d_ref, y_ref, *refs):
        outs, block_ref = refs[:-1], refs[-1]
        parity, whole = parity_ref[0], slice(0, WIDE)
        block_ref[...] = dot_nt(pair_ref[...], weight_ref[:, : 2 * hidden]) + d_ref[...].astype(jnp.float32)
        give_halves(block_ref, parity, parts, whole, outs[:parts], outs[parts : 2 * parts])
        block_ref[...] = dot_nt(hidden_ref[...], weight_ref[:, 2 * hidden :]) + y_ref[...].astype(jnp.float32)
        give_halves(block_ref, parity, 1, whole, outs[2 * parts : 2 * parts + 1], outs[2 * parts + 1 :])

    def still(step, parity_ref):
        return (0, 0)

    def across(step, parity_ref):
        return (0, step)

    def down(step, parity_ref):
        return (step, 0)

    heights = [rows // parts // 2] * (2 * parts) + [rows // 2] * 2
    return pl.pallas_call(
        body,
        out_shape=[jax.ShapeDtypeStruct((height, depth), jnp.bfloat16) for height in heights],
        grid_spec=pltpu.PrefetchScalarGridSpec(
            num_scalar_prefetch=1,
            grid=(depth // WIDE,),
            in_specs=[
                pl.BlockSpec((rows, hidden), still),
                pl.BlockSpec((rows, 2 * hidden), still),
                pl.BlockSpec((WIDE, 3 * hidden), down),
                pl.BlockSpec((rows, WIDE), across),
                pl.BlockSpec((rows, WIDE), across),
            ],
            out_specs=[pl.BlockSpec((height, WIDE), across) for height in heights],
            scratch_shapes=[pltpu.VMEM((rows, WIDE), jnp.float32)],
        ),
        compiler_params=pltpu.CompilerParams(vmem_limit_bytes=50 * MEBI),
        cost_estimate=pl.CostEstimate(
            flops=2 * rows * depth * hidden * 3, bytes_accessed=2 * (4 * rows * depth + 3 * depth * hidden), transcendentals=0
        ),
    )(parity, hidden_rows, pair_rows, weight, *earlier)


def sum_specs(parts, steps, rows, depth):
    share = steps // parts // 2

    def spec(index):
        return pl.BlockSpec((rows, depth), lambda step, scalars: (jnp.clip(step - index * share, 0, share - 1), 0))

    return [spec(index) for index in range(2 * parts)]


def place_row(parts, steps):
    share = steps // parts // 2

    def place(step, scalars):
        span = step // share
        part, other = span // 2, span % 2
        half = jnp.where(other == 0, scalars[0], 1 - scalars[0])
        return ((2 * part + half) * share + step % share, 0)

    return place


def pick_sum(step, share, refs):
    value = refs[0][...]
    for index, ref in enumerate(refs[1:]):
        value = jnp.where(step >= (index + 1) * share, ref[...], value)
    return value.astype(jnp.float32)


def row_call(body, scalars, parts, sums, whole, fixed, outs, narrow=(), limit=16):
    rows, depth = whole[0].shape
    steps = rows // ROWS
    place = place_row(parts, steps)
    block = pl.BlockSpec((ROWS, depth), place)
    ones = [pl.BlockSpec(array.shape, lambda step, scalars: (0, 0)) for array in fixed]
    moved = sum(a.size * a.dtype.itemsize for a in list(sums) + list(whole))
    moved += sum(rows * depth * jnp.dtype(kind).itemsize for kind in outs)
    return pl.pallas_call(
        body,
        out_shape=[jax.ShapeDtypeStruct((rows, depth), kind) for kind in outs]
        + [jax.ShapeDtypeStruct((rows, count), jnp.bfloat16) for count in narrow],
        grid_spec=pltpu.PrefetchScalarGridSpec(
            num_scalar_prefetch=1,
            grid=(steps,),
            in_specs=sum_specs(parts, steps, ROWS, depth) + [block] * len(whole) + ones,
            out_specs=[block] * len(outs) + [pl.BlockSpec((ROWS, count), place) for count in narrow],
        ),
        compiler_params=pltpu.CompilerParams(vmem_limit_bytes=limit * MEBI),
        cost_estimate=pl.CostEstimate(flops=10 * rows * depth, bytes_accessed=moved, transcendentals=0),
    )(scalars, *sums, *whole, *fixed)


def norm_factor(values):
    return lax.rsqrt(jnp.mean(values * values, axis=-1, keepdims=True) + epsilon)


def norm_call(scalars, sums, rows_in, gain):
    parts, steps = len(sums) // 2, rows_in.shape[0] // ROWS

    def body(scalar_ref, *refs):
        sum_refs = refs[: 2 * parts]
        rows_ref, gain_ref, resid_ref, normed_ref = refs[2 * parts :]
        total = pick_sum(pl.program_id(0), steps // parts // 2, sum_refs)
        resid = rows_ref[...].astype(jnp.float32) + total
        resid_ref[...] = resid.astype(jnp.bfloat16)
        normed_ref[...] = (resid * norm_factor(resid) * gain_ref[...]).astype(jnp.bfloat16)

    return row_call(body, scalars, parts, sums, [rows_in], [gain], [jnp.bfloat16, jnp.bfloat16])


def norm_back(total, values, gain):
    factor = norm_factor(values)
    hat = values * factor
    scaled = gain * total
    return factor * (scaled - hat * jnp.mean(scaled * hat, axis=-1, keepdims=True))


def norm_back_call(scalars, sums, resid, back, gain, full_out):
    parts, steps = len(sums) // 2, resid.shape[0] // ROWS

    def body(scalar_ref, *refs):
        sum_refs = refs[: 2 * parts]
        resid_ref, back_ref, gain_ref, out_ref, d_attn_ref, d_mixed_ref = refs[2 * parts :]
        total = pick_sum(pl.program_id(0), steps // parts // 2, sum_refs)
        slope = norm_back(total, resid_ref[...].astype(jnp.float32), gain_ref[...])
        d_attn = (back_ref[...].astype(jnp.float32) + slope).astype(jnp.bfloat16)
        d_attn_ref[...] = d_attn
        d_mixed_ref[...] = dot_nn(d_attn, out_ref[...]).astype(jnp.bfloat16)

    return row_call(body, scalars, parts, sums, [resid, back], [gain, full_out], [jnp.bfloat16], [full_out.shape[1]])


def store_placed(target_ref, values, scalar_ref, size):
    share = values.shape[1] // size
    if share % 128:
        target_ref[...] = values
        return
    for index in range(size):
        columns = pl.ds(pl.multiple_of(scalar_ref[1 + index] * share, 128), share)
        target_ref[:, columns] = values[:, index * share : (index + 1) * share]


def replaced(matrix, places):
    size = places.shape[0]
    share = matrix.shape[1] // size
    if share % 128 == 0:
        return matrix
    return jnp.take(matrix.reshape(-1, size, share), jnp.argsort(places), axis=1).reshape(matrix.shape)


def last_call(scalars, sums, d_resid, rows_in, gain, size):
    parts, steps = len(sums) // 2, rows_in.shape[0] // ROWS

    def body(scalar_ref, *refs):
        sum_refs = refs[: 2 * parts]
        d_resid_ref, rows_ref, gain_ref, out_ref = refs[2 * parts :]
        total = pick_sum(pl.program_id(0), steps // parts // 2, sum_refs)
        slope = norm_back(total, rows_ref[...].astype(jnp.float32), gain_ref[...])
        store_placed(out_ref, d_resid_ref[...].astype(jnp.float32) + slope, scalar_ref, size)

    (out,) = row_call(body, scalars, parts, sums, [d_resid, rows_in], [gain], [jnp.float32], limit=60)
    return replaced(out, scalars[1:])


def output_call(scalars, sums, resid, size):
    parts, steps = len(sums) // 2, resid.shape[0] // ROWS

    def body(scalar_ref, *refs):
        sum_refs = refs[: 2 * parts]
        resid_ref, out_ref = refs[2 * parts :]
        total = pick_sum(pl.program_id(0), steps // parts // 2, sum_refs)
        store_placed(out_ref, (resid_ref[...].astype(jnp.float32) + total).astype(jnp.bfloat16), scalar_ref, size)

    (out,) = row_call(body, scalars, parts, sums, [resid], [], [jnp.bfloat16])
    return replaced(out, scalars[1:])


def sum_refs_of(refs):
    total = refs[0][...].astype(jnp.float32)
    for ref in refs[1:]:
        total = total + ref[...].astype(jnp.float32)
    return total


def finish_feed(grads, w_gate, w_up, spans):
    share, count = w_gate.shape

    def body(*refs):
        grad_refs = refs[: len(grads)]
        gate_ref, up_ref, d_gate_ref, d_up_ref, d_down_ref, gain_ref = refs[len(grads) :]
        for index, (low, high) in enumerate(spans):
            span = high - low
            total = sum_refs_of(grad_refs[3 * index : 3 * index + 3])
            d_gate_ref[:, low:high] = total[:, :span]
            d_up_ref[:, low:high] = total[:, span : 2 * span]
            d_down_ref[low:high, :] = total[:, 2 * span :].T
        gain_ref[...] = jnp.sum(
            gate_ref[...].astype(jnp.float32) * d_gate_ref[...] + up_ref[...].astype(jnp.float32) * d_up_ref[...],
            axis=1, keepdims=True,
        )

    shapes = [(share, count), (share, count), (count, share), (share, 1)]
    return vmem_call(
        body, [jax.ShapeDtypeStruct(shape, jnp.float32) for shape in shapes],
        (*grads, w_gate, w_up), 24, scalars=0, moved=share * count * 36,
    )


def finish_mix(grads, mix_shard, width, slots):
    share = mix_shard.shape[0]
    used, start = 3 * width + slots, 3 * width + 2 * BLOCK

    def body(*refs):
        grad_refs = refs[: len(grads)]
        shard_ref, query_ref, key_ref, value_ref, slot_ref, out_ref, gain_ref = refs[len(grads) :]
        total = sum_refs_of(grad_refs)
        for index, ref in enumerate((query_ref, key_ref, value_ref)):
            ref[...] = total[:, index * width : (index + 1) * width]
        slot_ref[...] = total[:, 3 * width : used]
        out_ref[...] = total[:, start:].T
        gain_ref[...] = jnp.sum(shard_ref[:, :used].astype(jnp.float32) * total[:, :used], axis=1, keepdims=True)

    shapes = [(share, width)] * 3 + [(share, slots), (width, share), (share, 1)]
    return vmem_call(
        body, [jax.ShapeDtypeStruct(shape, jnp.float32) for shape in shapes],
        (*grads, mix_shard), 16, scalars=0, moved=share * start * 14,
    )


def exchange(kept, sent, held=()):
    heads = lax.axis_size(HEAD)
    near = [(i, i ^ 1) for i in range(heads)]
    far = [(i, i ^ 2) for i in range(heads)]
    sums, halves = [], []
    for own, given in zip(kept, sent):
        own = to_low(to_wide(own) + to_wide(lax.ppermute(given, HEAD, near)))
        halves.append(own)
        own = to_low(to_wide(own) + to_wide(tie(lax.ppermute(own, HEAD, far), *held)))
        sums += [own, lax.ppermute(own, HEAD, near)]
    return sums, halves


def layer(
    inputs,
    lengths,
    gain_attn,
    w_query,
    w_key,
    w_value,
    w_slot,
    gate_bias,
    w_out,
    gain_ffn,
    w_gate,
    w_up,
    w_down,
    cotangent,
):
    size = lax.axis_size(DP)
    order = ring_order(size)
    spots = [order.index(i) for i in range(size)]
    spot = jnp.array(spots, jnp.int32)[lax.axis_index(DP)]
    places = jnp.array(order + order, jnp.int32)[spot + jnp.arange(size, dtype=jnp.int32)]
    parity = jnp.bitwise_and(lax.axis_index(HEAD), 1).astype(jnp.int32)[None]
    scalars = jnp.concatenate([parity, places])
    share = gain_attn.shape[0]
    width, slots = w_query.shape[1], w_slot.shape[1]
    hidden_count = w_gate.shape[1]
    cut = (hidden_count // WIDE + 1) // 2 * WIDE
    spans = [(0, cut), (cut, hidden_count)]

    spare = jnp.zeros((share, 2 * BLOCK - slots - 2), w_slot.dtype)
    mix_shard = jnp.concatenate(
        [w_query, w_key, w_value, w_slot, gain_attn[:, None], gain_ffn[:, None], spare, w_out.T], axis=1
    )
    mix_count = 3 * width + 2 * BLOCK
    mix_pieces = ring_gather(mix_shard, order)
    down_rows = w_down.T
    feed_pieces = []
    for low, high in spans:
        shard = jnp.concatenate([w_gate[:, low:high], w_up[:, low:high], down_rows[:, low:high]], axis=1)
        feed_pieces.append(ring_gather(tie(shard, *flat_pieces([mix_pieces[size // 2]])), order))

    rows_low = move_columns(inputs, places, False)
    factor = norm_factor(to_wide(rows_low))
    back_low = move_columns(cotangent, places, False)
    rows_low, factor, _ = lax.optimization_barrier((rows_low, factor, back_low))

    qkv, logits, normed, gains = query_call(rows_low, factor, mix_pieces, slots, mix_count)
    gain_one, gain_two = gains[0:1], gains[1:2]
    bias = gate_bias[:, None]
    mixed, *saved = mixer_forward(lengths, qkv, logits, bias)
    kept, sent, (full_out,) = project_call(mixed, mix_pieces, parity, 2, mix_count, True)
    sums, _ = exchange(kept, sent)
    resid, normed_two = norm_call(scalars, sums, rows_low, gain_two)

    middle = size // 2

    def grads_of(pairs, far=None):
        span = slice(middle * share, (middle + 1) * share)
        far = far or to_low(jnp.concatenate([dot_tn(left[:, span], right) for left, right in pairs], axis=1))
        grads = [to_low(dot_tn(left, right)) for left, right in pairs]

        def piece_of(index):
            if index == middle:
                return far
            return jnp.concatenate([grad[index * share : (index + 1) * share] for grad in grads], axis=1)

        return piece_of

    partial, feed_grads = None, []
    for pieces in feed_pieces:
        if partial is None:
            hidden, pair, far_up, far_down, *partial = feed_call(normed_two, back_low, pieces, parity, None, 2)
        else:
            hidden, pair, weight, far_up, far_down = act_call(normed_two, back_low, pieces)
            partial = back_call(hidden, pair, weight, parity, partial, 2)
        piece_of = grads_of([(normed_two, pair), (back_low, hidden)], (far_up, far_down))
        feed_grads += ring_scatter(piece_of, order)

    sums, _ = exchange(partial[:2], partial[2:4])
    d_attn, d_mixed = norm_back_call(scalars, sums, resid, back_low, gain_two, full_out)
    d_all, d_bias = mixer_backward(lengths, qkv, logits, bias, d_mixed, saved)
    bias_sum = total_sum(d_bias[:, 0], DP)
    mix_grads = ring_scatter(grads_of([(normed, d_all), (d_attn, mixed)]), order)
    kept, sent, _ = project_call(d_all, mix_pieces, parity, 2, 0, False)
    sums, halves = exchange(kept, sent)
    early, _ = exchange([partial[4]], partial[5:], halves)
    output = output_call(scalars, early, resid, size)
    *feed_out, gain_sum_two = finish_feed(feed_grads, w_gate, w_up, spans)
    sums[0] = tie(sums[0], output)
    grad_inputs = last_call(scalars, sums, d_attn, rows_low, gain_one, size)
    *mix_out, gain_sum_one = finish_mix(mix_grads, mix_shard, width, slots)
    gain_sums = total_sum(jnp.stack([gain_sum_one[:, 0], gain_sum_two[:, 0]]), HEAD)

    return (
        output,
        grad_inputs,
        gain_sums[0] / to_wide(gain_attn),
        *mix_out[:4],
        bias_sum,
        mix_out[4],
        gain_sums[1] / to_wide(gain_ffn),
        *feed_out,
    )


def solution(mesh):
    in_specs = (
        P(DP, None),
        P(DP),
        P(DP),
        P(DP, HEAD),
        P(DP, HEAD),
        P(DP, HEAD),
        P(DP, HEAD),
        P(HEAD),
        P(HEAD, DP),
        P(DP),
        P(DP, HEAD),
        P(DP, HEAD),
        P(HEAD, DP),
        P(DP, None),
    )
    out_specs = (
        P(DP, None),
        P(DP, None),
        P(DP),
        P(DP, HEAD),
        P(DP, HEAD),
        P(DP, HEAD),
        P(DP, HEAD),
        P(HEAD),
        P(HEAD, DP),
        P(DP),
        P(DP, HEAD),
        P(DP, HEAD),
        P(HEAD, DP),
    )
    return jax.shard_map(layer, mesh=mesh, in_specs=in_specs, out_specs=out_specs, check_vma=False)
```
